32 devices in a mesh: section: 2 (over x), dp: 4 (over z), tensor: 4 (over y, core).
Axes of the slice: x: 2, y: 2, z: 4, core: 2. Of those that a mesh axis runs over, the one named last changes fastest.
Arguments:
- images: bfloat16 [4, 4, 577, 1024], P(None, 'dp', None, 'tensor'), may hold values from -6 to 6
- cotangent: bfloat16 [4, 4, 577, 1024], P(None, 'dp', None, 'tensor'), may hold values from -6 to 6
- ln1_gain: float32 [2, 1024], P('section', 'tensor'), may hold values from 0.5 to 1.5
- ln1_bias: float32 [2, 1024], P('section', 'tensor'), may hold values from -1.8 to 1.8
- qkv_weight: bfloat16 [2, 3, 1024, 1024], P('section', None, None, 'tensor'), may hold values from -6.25 to 6.25
- qv_bias: float32 [2, 2, 1024], P('section', None, 'tensor'), may hold values from -3 to 3
- out_weight: bfloat16 [2, 1024, 1024], P('section', 'tensor'), may hold values from -1 to 1
- out_bias: float32 [2, 1024], P('section', 'tensor'), may hold values from -3 to 3
- ln2_gain: float32 [2, 1024], P('section', 'tensor'), may hold values from 0.5 to 1.5
- ln2_bias: float32 [2, 1024], P('section', 'tensor'), may hold values from -1.8 to 1.8
- fc1_weight: bfloat16 [2, 1024, 4096], P('section', None, 'tensor'), may hold values from -0.1875 to 0.1875
- fc1_bias: float32 [2, 4096], P('section', 'tensor'), may hold values from -3 to 3
- fc2_weight: bfloat16 [2, 4096, 1024], P('section', 'tensor'), may hold values from -0.09375 to 0.09375
- fc2_bias: float32 [2, 1024], P('section', 'tensor'), may hold values from -3 to 3
Outputs:
- section_out: bfloat16 [2, 4, 4, 577, 1024], P('section', None, 'dp', None, 'tensor')
- input_grads: float32 [2, 4, 4, 577, 1024], P('section', None, 'dp', None, 'tensor')
- grad_ln1_gain: float32 [2, 1024], P('section', 'tensor')
- grad_ln1_bias: float32 [2, 1024], P('section', 'tensor')
- grad_qkv_weight: float32 [2, 3, 1024, 1024], P('section', None, None, 'tensor')
- grad_qv_bias: float32 [2, 2, 1024], P('section', None, 'tensor')
- grad_out_weight: float32 [2, 1024, 1024], P('section', 'tensor')
- grad_out_bias: float32 [2, 1024], P('section', 'tensor')
- grad_ln2_gain: float32 [2, 1024], P('section', 'tensor')
- grad_ln2_bias: float32 [2, 1024], P('section', 'tensor')
- grad_fc1_weight: float32 [2, 1024, 4096], P('section', None, 'tensor')
- grad_fc1_bias: float32 [2, 4096], P('section', 'tensor')
- grad_fc2_weight: float32 [2, 4096, 1024], P('section', 'tensor')
- grad_fc2_bias: float32 [2, 1024], P('section', 'tensor')
The draws below stay inside these ranges and needn't reach their ends.
All inputs are finite; a program needn't handle non-finite values.
Results may differ from the reference program's by a relative error of at most 0.02.
The reference program's roundings to bfloat16 on the way count: a program that leaves them out, or rounds other values in their place, can miss the bound.
Values may be sent and summed in bfloat16 or wider, within the bound.
A program may use at most 320 MiB of HBM per device.

```python
import jax
import jax.numpy as jnp
from jax import lax

D = 1024
HEADS = 16
FF = 4096
TOK = 577
MICRO = 4
HEAD_DIM = 64
IMAGES = 4
N_SECTION = 2


def draw_qkv_weight(key, part):
    base_draw = jnp.clip(jax.random.normal(key, (N_SECTION, 3, D, D), jnp.float32), -5.0, 5.0) * D ** (-0.5)
    return base_draw.astype(jnp.bfloat16)


def steps_of(rng, dims, shards, least, top_value):
    def one(position, parts):
        heights = jax.random.uniform(jax.random.fold_in(jax.random.fold_in(rng, 6), position), (parts,), jnp.float32, least / len(shards), top_value / len(shards))
        return jnp.repeat(jnp.exp(heights), dims[position] // parts).reshape((-1,) + (1,) * (len(dims) - position - 1))

    level = one(*shards[0])
    for cut in shards[1:]:
        level = level * one(*cut)
    return level


def scatter_about(rng, shape, scale, limit, pieces=(), kind=jnp.bfloat16):
    entries = scale * jax.random.normal(rng, shape, jnp.float32)
    if pieces:
        entries = entries * steps_of(rng, shape, pieces, -0.22, 0.18)
    return jnp.clip(entries, -limit, limit).astype(kind)


def setup_inputs(seed: int = 0) -> dict:
    key_of = jax.random.split(jax.random.key(seed), 15)
    images = scatter_about(key_of[0], (MICRO, IMAGES, TOK, D), 1.0, 6.0, ((1, 4), (3, 4)))
    cotangent = scatter_about(key_of[1], (MICRO, IMAGES, TOK, D), 1.0, 6.0, ((1, 4), (3, 4)))
    ln1_gain = jnp.clip(1.0 + 0.1 * jax.random.normal(key_of[2], (N_SECTION, D), jnp.float32), 0.5, 1.5)
    ln1_bias = scatter_about(key_of[3], (N_SECTION, D), 0.3, 1.8, ((0, 2), (1, 4)), jnp.float32)
    qkv_weight = draw_qkv_weight(jax.random.fold_in(key_of[14], 71), 0)
    qv_bias = scatter_about(key_of[5], (N_SECTION, 2, D), 0.5, 3.0, ((0, 2), (2, 4)), jnp.float32)
    out_weight = scatter_about(key_of[6], (N_SECTION, D, D), (max(1, D // (TOK // 24 + 1))) ** -0.5, 1.0, ((0, 2), (1, 4)))
    out_bias = scatter_about(key_of[7], (N_SECTION, D), 0.5, 3.0, ((0, 2), (1, 4)), jnp.float32)
    ln2_gain = jnp.clip(1.0 + 0.1 * jax.random.normal(key_of[8], (N_SECTION, D), jnp.float32), 0.5, 1.5)
    ln2_bias = scatter_about(key_of[9], (N_SECTION, D), 0.3, 1.8, ((0, 2), (1, 4)), jnp.float32)
    fc1_weight = scatter_about(key_of[10], (N_SECTION, D, FF), D ** -0.5, 0.1875, ((0, 2), (2, 4)))
    fc1_bias = scatter_about(key_of[11], (N_SECTION, FF), 0.5, 3.0, ((0, 2), (1, 4)), jnp.float32)
    fc2_weight = scatter_about(key_of[12], (N_SECTION, FF, D), FF ** -0.5, 0.09375, ((0, 2), (1, 4)))
    fc2_bias = scatter_about(key_of[13], (N_SECTION, D), 0.5, 3.0, ((0, 2), (1, 4)), jnp.float32)
    return {"images": images, "cotangent": cotangent, "ln1_gain": ln1_gain, "ln1_bias": ln1_bias, "qkv_weight": qkv_weight, "qv_bias": qv_bias, "out_weight": out_weight, "out_bias": out_bias, "ln2_gain": ln2_gain, "ln2_bias": ln2_bias, "fc1_weight": fc1_weight, "fc1_bias": fc1_bias, "fc2_weight": fc2_weight, "fc2_bias": fc2_bias}


NORM_EPSILON = 1e-06
ROOT_HALF = 0.7071067811865476
GAUSS_FACTOR = 0.3989422804014327

def gelu_exact(preact):
    return 0.5 * preact * (1.0 + jax.scipy.special.erf(preact * ROOT_HALF))

def gelu_slope(preact):
    return 0.5 * (1.0 + jax.scipy.special.erf(preact * ROOT_HALF)) + preact * jnp.exp(-0.5 * preact * preact) * GAUSS_FACTOR

def norm_forward(stream, norm_gain, norm_bias):
    row_mean = lax.optimization_barrier(jnp.mean(stream, axis=-1, keepdims=True))
    row_var = lax.optimization_barrier(jnp.mean(stream * stream, axis=-1, keepdims=True)) - row_mean * row_mean
    inv_std = lax.rsqrt(row_var + NORM_EPSILON)
    centred = (stream - row_mean) * inv_std
    return (centred, inv_std, (centred * norm_gain + norm_bias).astype(jnp.bfloat16))

def norm_backward(grad_normed, centred, inv_std, norm_gain):
    scaled = grad_normed * norm_gain
    return inv_std * (scaled - lax.optimization_barrier(jnp.mean(scaled, axis=-1, keepdims=True)) - centred * lax.optimization_barrier(jnp.mean(scaled * centred, axis=-1, keepdims=True)))

def heads_of(matrix):
    return matrix.astype(jnp.float32).reshape(TOK, HEADS, HEAD_DIM).transpose(1, 0, 2)

def merge_heads(stacked):
    return stacked.transpose(1, 0, 2).reshape(TOK, D)

def attention_scores(query, key_rows):
    return jnp.einsum('htd,hsd->hts', heads_of(query), heads_of(key_rows), precision=lax.Precision.HIGHEST) * HEAD_DIM ** (-0.5)

def layer_forward(layer_params, block_in):
    gain_one, bias_one, qkv_mats, qv_shift, out_mat, out_shift, gain_two, bias_two, expand_mat, expand_shift, reduce_mat, reduce_shift = layer_params
    stream = block_in.astype(jnp.float32)
    centred_one, inv_one, normed_one = norm_forward(stream, gain_one, bias_one)
    query = (jnp.dot(normed_one, qkv_mats[0], preferred_element_type=jnp.float32) + qv_shift[0]).astype(jnp.bfloat16)
    key_rows = jnp.dot(normed_one, qkv_mats[1], preferred_element_type=jnp.float32).astype(jnp.bfloat16)
    value_rows = (jnp.dot(normed_one, qkv_mats[2], preferred_element_type=jnp.float32) + qv_shift[1]).astype(jnp.bfloat16)
    scores = attention_scores(query, key_rows)
    log_total = jax.nn.logsumexp(scores, axis=-1, keepdims=True)
    probs_low = jnp.exp(scores - log_total).astype(jnp.bfloat16)
    attended = merge_heads(jnp.einsum('hts,hsd->htd', probs_low.astype(jnp.float32), heads_of(value_rows), precision=lax.Precision.HIGHEST)).astype(jnp.bfloat16)
    hidden = stream + (jnp.dot(attended, out_mat, preferred_element_type=jnp.float32) + out_shift)
    centred_two, inv_two, normed_two = norm_forward(hidden, gain_two, bias_two)
    preact = jnp.dot(normed_two, expand_mat, preferred_element_type=jnp.float32) + expand_shift
    activated = gelu_exact(preact).astype(jnp.bfloat16)
    output = hidden + (jnp.dot(activated, reduce_mat, preferred_element_type=jnp.float32) + reduce_shift)
    kept_state = (centred_one, inv_one, normed_one, query, key_rows, value_rows, log_total, attended, centred_two, inv_two, normed_two, preact, activated)
    return (output.astype(jnp.bfloat16), kept_state)

def layer_backward(layer_params, kept_state, grad_out):
    gain_one, bias_one, qkv_mats, qv_shift, out_mat, out_shift, gain_two, bias_two, expand_mat, expand_shift, reduce_mat, reduce_shift = layer_params
    centred_one, inv_one, normed_one, query, key_rows, value_rows, log_total, attended, centred_two, inv_two, normed_two, preact, activated = kept_state
    grad_out_low = grad_out.astype(jnp.bfloat16)
    grad_reduce_shift = lax.optimization_barrier(jnp.sum(grad_out, axis=0))
    grad_reduce_mat = jnp.dot(activated.T, grad_out_low, preferred_element_type=jnp.float32)
    grad_preact = jnp.dot(grad_out_low, reduce_mat.T, preferred_element_type=jnp.float32) * gelu_slope(preact)
    grad_expand_shift = lax.optimization_barrier(jnp.sum(grad_preact, axis=0))
    preact_low = grad_preact.astype(jnp.bfloat16)
    grad_expand_mat = jnp.dot(normed_two.T, preact_low, preferred_element_type=jnp.float32)
    grad_normed_two = jnp.dot(preact_low, expand_mat.T, preferred_element_type=jnp.float32)
    grad_gain_two = lax.optimization_barrier(jnp.sum(grad_normed_two * centred_two, axis=0))
    grad_bias_two = lax.optimization_barrier(jnp.sum(grad_normed_two, axis=0))
    grad_hidden = grad_out + norm_backward(grad_normed_two, centred_two, inv_two, gain_two)
    grad_out_shift = lax.optimization_barrier(jnp.sum(grad_hidden, axis=0))
    hidden_low = grad_hidden.astype(jnp.bfloat16)
    grad_out_mat = jnp.dot(attended.T, hidden_low, preferred_element_type=jnp.float32)
    grad_attended = jnp.dot(hidden_low, out_mat.T, preferred_element_type=jnp.float32).astype(jnp.bfloat16)
    scores = attention_scores(query, key_rows)
    probability = jnp.exp(scores - log_total)
    probs_back = lax.optimization_barrier(probability.astype(jnp.bfloat16)).astype(jnp.float32)
    grad_heads = heads_of(grad_attended)
    grad_value = merge_heads(jnp.einsum('hts,htd->hsd', probs_back, grad_heads, precision=lax.Precision.HIGHEST))
    grad_prob = jnp.einsum('htd,hsd->hts', grad_heads, heads_of(value_rows), precision=lax.Precision.HIGHEST)
    grad_scores = probability * (grad_prob - lax.optimization_barrier(jnp.sum(probability * grad_prob, axis=-1, keepdims=True))) * HEAD_DIM ** (-0.5)
    scores_back = lax.optimization_barrier(grad_scores.astype(jnp.bfloat16)).astype(jnp.float32)
    grad_query = merge_heads(jnp.einsum('hts,hsd->htd', scores_back, heads_of(key_rows), precision=lax.Precision.HIGHEST))
    grad_key = merge_heads(jnp.einsum('hts,htd->hsd', scores_back, heads_of(query), precision=lax.Precision.HIGHEST))
    grad_qv_shift = jnp.stack([lax.optimization_barrier(jnp.sum(grad_query, axis=0)), lax.optimization_barrier(jnp.sum(grad_value, axis=0))])
    low_grads = [grad_query.astype(jnp.bfloat16), grad_key.astype(jnp.bfloat16), grad_value.astype(jnp.bfloat16)]
    grad_qkv_mats = jnp.stack([jnp.dot(normed_one.T, piece_grad, preferred_element_type=jnp.float32) for piece_grad in low_grads])
    grad_normed_one = jnp.dot(low_grads[0], qkv_mats[0].T, preferred_element_type=jnp.float32)
    grad_normed_one = grad_normed_one + jnp.dot(low_grads[1], qkv_mats[1].T, preferred_element_type=jnp.float32)
    grad_normed_one = grad_normed_one + jnp.dot(low_grads[2], qkv_mats[2].T, preferred_element_type=jnp.float32)
    grad_gain_one = lax.optimization_barrier(jnp.sum(grad_normed_one * centred_one, axis=0))
    grad_bias_one = lax.optimization_barrier(jnp.sum(grad_normed_one, axis=0))
    grad_input = grad_hidden + norm_backward(grad_normed_one, centred_one, inv_one, gain_one)
    grads = (grad_gain_one, grad_bias_one, grad_qkv_mats, grad_qv_shift, grad_out_mat, grad_out_shift, grad_gain_two, grad_bias_two, grad_expand_mat, grad_expand_shift, grad_reduce_mat, grad_reduce_shift)
    return (grad_input, grads)

def reference(images, cotangent, ln1_gain, ln1_bias, qkv_weight, qv_bias, out_weight, out_bias, ln2_gain, ln2_bias, fc1_weight, fc1_bias, fc2_weight, fc2_bias):
    stacks = (ln1_gain, ln1_bias, qkv_weight, qv_bias, out_weight, out_bias, ln2_gain, ln2_bias, fc1_weight, fc1_bias, fc2_weight, fc2_bias)
    lower_params = tuple((stacked[0] for stacked in stacks))
    upper_params = tuple((stacked[1] for stacked in stacks))
    flat_in = images.reshape(MICRO * IMAGES, TOK, D)
    flat_cot = cotangent.reshape(MICRO * IMAGES, TOK, D)
    zero_grads = tuple((jnp.zeros(stacked.shape[1:], jnp.float32) for stacked in stacks))

    def visit_image(carry, pair):
        image_in, image_cot = pair
        out_lower, kept_lower = layer_forward(lower_params, image_in)
        out_upper, kept_upper = layer_forward(upper_params, out_lower)
        grad_upper, grads_upper = layer_backward(upper_params, kept_upper, image_cot.astype(jnp.float32))
        passed_down = lax.optimization_barrier(grad_upper.astype(jnp.bfloat16)).astype(jnp.float32)
        grad_lower, grads_lower = layer_backward(lower_params, kept_lower, passed_down)
        sums_lower = jax.tree.map(jnp.add, carry[0], grads_lower)
        sums_upper = jax.tree.map(jnp.add, carry[1], grads_upper)
        return ((sums_lower, sums_upper), (out_lower, out_upper, grad_lower, grad_upper))
    (sums_lower, sums_upper), (out_lower, out_upper, grad_lower, grad_upper) = lax.scan(visit_image, (zero_grads, zero_grads), (flat_in, flat_cot))
    section_out = jnp.stack([out_lower, out_upper]).reshape(2, MICRO, IMAGES, TOK, D)
    input_grads = jnp.stack([grad_lower, grad_upper]).reshape(2, MICRO, IMAGES, TOK, D)
    grads = [jnp.stack([sums_lower[index], sums_upper[index]]) for index in range(12)]
    return (section_out, input_grads, grads[0], grads[1], grads[2], grads[3], grads[4], grads[5], grads[6], grads[7], grads[8], grads[9], grads[10], grads[11])
```

```python
import functools
import types

import jax
import jax.numpy as jnp
from jax import lax
from jax.experimental import pallas as pl
from jax.experimental.pallas import tpu as pltpu
from jax.sharding import PartitionSpec as P

BF16, F32 = jnp.bfloat16, jnp.float32
HEAD_DIM = 64
EPSILON = 1e-06
ROOT_HALF = 0.7071067811865476
GAUSS_FACTOR = 0.3989422804014327
MASKED = -1e30
STEP = 32
ANY = pl.BlockSpec(memory_space=pl.ANY)
VMEM_BYTES = 67043328

LN1_GAIN, LN1_BIAS, Q_BIAS, V_BIAS, OUT_BIAS, LN2_GAIN, LN2_BIAS, FC2_BIAS, FC1_BIAS = range(9)
VECTOR_ROWS = 16


def flip(place, bit):
    return place + bit - 2 * bit * lax.rem(lax.div(place, bit), 2)


def partner(place, slot):
    bit = 1
    while bit <= slot:
        if slot & bit:
            place = flip(place, bit)
        bit *= 2
    return place


def sizes_of(images, fc1_weight, tensor):
    micro, _, tok, width = images.shape
    dm = types.SimpleNamespace()
    dm.T, dm.W, dm.micro, dm.tok = tensor, width, micro, tok
    dm.D = width * tensor
    dm.FL = fc1_weight.shape[2]
    dm.RP = -(-tok // STEP) * STEP
    dm.RL = -(-tok // 128) * 128
    dm.C = min(512, dm.FL)
    dm.NC = dm.FL // dm.C
    dm.order = [
        (2 * p + half, c) for p in range(tensor // 2) for c in range(dm.NC) for half in range(2)
    ]
    dm.NI = len(dm.order)
    dm.NCH = 2 + 2 * dm.NC
    return dm


def full_vector(dm, vectors, row):
    return jnp.concatenate([vectors[j, row : row + 1, :] for j in range(dm.T)], axis=1)


def norm_rows(rows, width):
    mean = jnp.sum(rows, axis=1, keepdims=True) * (1.0 / width)
    var = jnp.sum(rows * rows, axis=1, keepdims=True) * (1.0 / width) - mean * mean
    inv = lax.rsqrt(var + EPSILON)
    return (rows - mean) * inv, inv


def block_rows(dm, ref, rows):
    return jnp.concatenate([ref[j, rows, :] for j in range(dm.T)], axis=1)


def dot_last(left, right):
    return lax.dot_general(left, right, (((1,), (1,)), ((), ())), preferred_element_type=F32)


def dot_plain(left, right):
    return lax.dot_general(left, right, (((1,), (0,)), ((), ())), preferred_element_type=F32)


def half_masks(rows):
    lane = lax.broadcasted_iota(jnp.int32, (rows, 128), 1)
    return [lane < HEAD_DIM, lane >= HEAD_DIM]


def chunk_refs(dm, index, qkv, out, up, down):
    if index == 0:
        return qkv
    if index == 1:
        return out
    c = (index - 2) // 2
    if index % 2 == 0:
        return up.at[:, pl.ds(c * dm.C, dm.C)]
    return down.at[pl.ds(c * dm.C, dm.C), :]


def meet(dm, section, tensor):
    barrier = pltpu.get_barrier_semaphore()
    for slot in range(1, dm.T):
        pl.semaphore_signal(barrier, inc=1, device_id={"tensor": partner(tensor, slot)})
    pl.semaphore_signal(barrier, inc=1, device_id={"section": 1 - section})
    pl.semaphore_wait(barrier, dm.T)


def forward_kernel(
    dm,
    xin, spin, wqkv, wout, wup, wdown,
    gqkv, gout, gup, gdown, xc, xkeep, qkeep, kkeep, vkeep, okeep, hkeep, akeep, spkeep, result,
    xarr, n1, wq, wob, w1b, w2b, ab, gb, acc, n2, yb, b1r, spb, q, k, v, o,
    wsend, wrecv, xsend, xrecv, psend, precv, osend, orecv, ssem, lsem, lw, la,
):
    section, tensor = lax.axis_index("section"), lax.axis_index("tensor")
    T, W, D, RP, RL, C, NI = dm.T, dm.W, dm.D, dm.RP, dm.RL, dm.C, dm.NI
    lower, upper = section == 0, section == 1
    own = (wqkv, wout, wup, wdown)

    def slot_refs(slot):
        return (gqkv.at[slot], gout.at[slot], gup.at[slot], gdown.at[slot])

    def weight_copy(slot, index):
        relay = slot > 1 and slot % 2 == 1
        source = chunk_refs(dm, index, *(slot_refs(slot - 1) if relay else own))
        return pltpu.make_async_remote_copy(
            src_ref=source,
            dst_ref=chunk_refs(dm, index, *slot_refs(slot)),
            send_sem=wsend.at[slot, index],
            recv_sem=wrecv.at[slot, index],
            device_id={"tensor": flip(tensor, 1) if relay else partner(tensor, slot)},
        )

    def input_copy(slot):
        return pltpu.make_async_remote_copy(
            src_ref=xin.at[lax.rem(partner(tensor, slot), dm.micro)],
            dst_ref=xc.at[tensor],
            send_sem=xsend.at[slot],
            recv_sem=xrecv.at[slot],
            device_id={"tensor": partner(tensor, slot)},
        )

    def vector_copy(slot):
        return pltpu.make_async_remote_copy(
            src_ref=spin,
            dst_ref=spb.at[tensor],
            send_sem=psend.at[slot],
            recv_sem=precv.at[slot],
            device_id={"tensor": partner(tensor, slot)},
        )

    def output_copy(slot):
        return pltpu.make_async_remote_copy(
            src_ref=yb.at[partner(tensor, slot)],
            dst_ref=result.at[tensor],
            send_sem=osend.at[slot],
            recv_sem=orecv.at[slot],
            device_id={"tensor": partner(tensor, slot)},
        )

    stream_copy = pltpu.make_async_remote_copy(
        src_ref=yb,
        dst_ref=xarr,
        send_sem=ssem.at[0],
        recv_sem=ssem.at[1],
        device_id={"section": 1 - section},
    )

    meet(dm, section, tensor)
    for slot in range(1, T):
        vector_copy(slot).start()
        input_copy(slot).start()
    own_vec = pltpu.make_async_copy(spin, spb.at[tensor], lsem.at[0])
    own_vec.start()
    own_in = pltpu.make_async_copy(xin.at[lax.rem(tensor, dm.micro)], xc.at[tensor], lsem.at[1])
    own_in.start()
    direct = [slot for slot in range(1, T) if slot == 1 or slot % 2 == 0]
    for index in range(dm.NCH):
        for slot in direct:
            weight_copy(slot, index).start()

    def relay(slot, index):
        weight_copy(slot, index).wait_recv()
        weight_copy(slot + 1, index).start()

    own_vec.wait()
    own_in.wait()
    for slot in range(1, T):
        vector_copy(slot).wait_recv()
        input_copy(slot).wait_recv()

    @pl.when(upper)
    def _():
        for index in range(dm.NCH):
            for slot in range(2, T, 2):
                relay(slot, index)
        stream_copy.wait_recv()

    @pl.when(lower)
    def _():
        load = pltpu.make_async_copy(xc, xarr, lsem.at[0])
        load.start()
        load.wait()

    def arrive(slot, index):
        if slot == 0:
            return
        if slot % 2 == 0:

            @pl.when(lower)
            def _():
                relay(slot, index)

        else:
            weight_copy(slot, index).wait_recv()

    def source_of(slot, index):
        return chunk_refs(dm, index, *(own if slot == 0 else slot_refs(slot)))

    keep_x = pltpu.make_async_copy(xarr, xkeep, lsem.at[1])
    keep_x.start()
    keep_p = pltpu.make_async_copy(spb, spkeep, lsem.at[2])
    keep_p.start()

    gain, bias = full_vector(dm, spb, LN1_GAIN), full_vector(dm, spb, LN1_BIAS)

    def first_norm(r, _):
        rows = pl.ds(pl.multiple_of(r * STEP, STEP), STEP)
        hat, _inv = norm_rows(block_rows(dm, xarr, rows).astype(F32), D)
        n1[rows, :] = (hat * gain + bias).astype(BF16)
        return 0

    lax.fori_loop(0, RP // STEP, first_norm, 0)

    for index, (slot, c) in enumerate(dm.order):
        shard = spb[partner(tensor, slot)]
        per = C // W
        first = FC1_BIAS + c * per
        b1r[index] = jnp.concatenate([shard[first + i : first + i + 1, :] for i in range(per)], axis=1)

    pad = jnp.zeros((RL - RP, W), BF16)
    for slot in range(T):
        for ref in (q, k, v):
            ref[slot, pl.ds(RP, RL - RP), :] = pad

    def load_qkv(slot, parity):
        return pltpu.make_async_copy(source_of(slot, 0), wq.at[parity], lw.at[parity])

    def fetch_qkv(which):
        for slot in range(T):

            @pl.when(which == slot)
            def _():
                arrive(slot, 0)
                load_qkv(slot, slot % 2).start()

    masks = half_masks(128)
    lane = lax.broadcasted_iota(jnp.int32, (1, RL), 1)
    key_bias = jnp.where(lane < dm.tok, 0.0, MASKED).astype(F32)

    fetch_qkv(0)

    def heads(slot, _):
        parity = lax.rem(slot, 2)
        pltpu.make_async_copy(gqkv.at[0], wq.at[parity], lw.at[parity]).wait()
        early = jnp.logical_or(upper, slot < 1)

        @pl.when(jnp.logical_and(early, slot + 1 < T))
        def _():
            fetch_qkv(slot + 1)

        shard = spb[partner_dynamic(dm, tensor, slot)]
        rows = pl.ds(0, RP)
        q[slot, rows, :] = (dot_plain(n1[...], wq[parity, 0]) + shard[Q_BIAS : Q_BIAS + 1]).astype(BF16)
        k[slot, rows, :] = dot_plain(n1[...], wq[parity, 1]).astype(BF16)
        v[slot, rows, :] = (dot_plain(n1[...], wq[parity, 2]) + shard[V_BIAS : V_BIAS + 1]).astype(BF16)

        for pair in range(W // 128):
            lanes = slice(pair * 128, pair * 128 + 128)

            def block(b, _):
                rows = pl.ds(pl.multiple_of(b * 128, 128), 128)
                query = q[slot, rows, lanes] * jnp.asarray(HEAD_DIM**-0.5, BF16)
                parts = []
                for mask in masks:
                    s = dot_last(jnp.where(mask, query, jnp.zeros_like(query)), k[slot, :, lanes]) + key_bias
                    e = jnp.exp(s - jnp.max(s, axis=1, keepdims=True))
                    p = (e * (1.0 / jnp.sum(e, axis=1, keepdims=True))).astype(BF16)
                    parts.append(dot_plain(p, v[slot, :, lanes]))
                o[slot, rows, lanes] = jnp.where(masks[0], parts[0], parts[1]).astype(BF16)
                return 0

            lax.fori_loop(0, RL // 128, block, 0, unroll=True)

        @pl.when(jnp.logical_and(jnp.logical_not(early), slot + 1 < T))
        def _():
            fetch_qkv(slot + 1)

        return 0

    lax.fori_loop(0, T, heads, 0)

    keeps = []
    for number, (source, target) in enumerate(((q, qkeep), (k, kkeep), (v, vkeep), (o, okeep))):
        keeps.append(pltpu.make_async_copy(source, target, la.at[2 + number]))
        keeps[-1].start()

    loads = []
    for slot in range(T):
        arrive(slot, 1)
        loads.append(
            pltpu.make_async_copy(source_of(slot, 1), wob.at[pl.ds(slot * W, W)], lw.at[2 + slot])
        )
        loads[-1].start()

    def arrive_ff(index):
        slot, c = dm.order[index]
        arrive(slot, 2 + 2 * c)
        arrive(slot, 3 + 2 * c)

    def load_ff(index, parity):
        slot, c = dm.order[index]
        return [
            pltpu.make_async_copy(source_of(slot, 2 + 2 * c), w1b.at[parity], lsem.at[3 + parity]),
            pltpu.make_async_copy(source_of(slot, 3 + 2 * c), w2b.at[parity], lsem.at[5 + parity]),
        ]

    def fetch_ff(which):
        for index in range(NI):

            @pl.when(which == index)
            def _():
                arrive_ff(index)
                for load in load_ff(index, index % 2):
                    load.start()

    fetch_ff(0)
    for load in loads:
        load.wait()
    attended = jnp.concatenate([o[slot, pl.ds(0, RP), :] for slot in range(T)], axis=1)
    for n in range(D // 256):
        acc[:, pl.ds(n * 256, 256)] = dot_plain(attended, wob[:, pl.ds(n * 256, 256)])

    out_bias = full_vector(dm, spb, OUT_BIAS)
    gain2, bias2 = full_vector(dm, spb, LN2_GAIN), full_vector(dm, spb, LN2_BIAS)
    down_bias = full_vector(dm, spb, FC2_BIAS)

    def second_norm(r, _):
        rows = pl.ds(pl.multiple_of(r * STEP, STEP), STEP)
        hidden = block_rows(dm, xarr, rows).astype(F32) + (acc[rows, :] + out_bias)
        hat, _inv = norm_rows(hidden, D)
        n2[rows, :] = (hat * gain2 + bias2).astype(BF16)
        acc[rows, :] = hidden
        return 0

    lax.fori_loop(0, RP // STEP, second_norm, 0)
    keep_h = pltpu.make_async_copy(acc, hkeep, lsem.at[0])
    keep_h.start()
    keep_h.wait()

    def keep_a(index, parity):
        return pltpu.make_async_copy(ab.at[parity], akeep.at[index], la.at[parity])

    def feed(index, _):
        parity = lax.rem(index, 2)
        for load in load_ff(0, parity):
            load.wait()
        early = jnp.logical_or(upper, index + 1 < 2 * dm.NC)

        @pl.when(jnp.logical_and(early, index + 1 < NI))
        def _():
            fetch_ff(index + 1)

        @pl.when(index >= 2)
        def _():
            keep_a(index - 2, parity).wait()

        ab[parity] = dot_plain(n2[...], w1b[parity])
        shift = b1r[index]

        def bend(r, _):
            rows = pl.ds(pl.multiple_of(r * STEP, STEP), STEP)
            a = ab[parity, rows, :] + shift
            ab[parity, rows, :] = a
            gb[rows, :] = (0.5 * a * (1.0 + lax.erf(a * ROOT_HALF))).astype(BF16)
            return 0

        lax.fori_loop(0, RP // STEP, bend, 0)
        keep_a(index, parity).start()
        for n in range(D // 256):
            cols = pl.ds(n * 256, 256)
            acc[:, cols] += dot_plain(gb[...], w2b[parity, :, cols])

        @pl.when(jnp.logical_and(jnp.logical_not(early), index + 1 < NI))
        def _():
            fetch_ff(index + 1)

        return 0

    lax.fori_loop(0, NI, feed, 0)

    def close(r, _):
        rows = pl.ds(pl.multiple_of(r * STEP, STEP), STEP)
        y = (acc[rows, :] + down_bias).astype(BF16)
        for j in range(T):
            yb[j, rows, :] = y[:, j * W : (j + 1) * W]
        return 0

    lax.fori_loop(0, RP // STEP, close, 0)

    @pl.when(lower)
    def _():
        stream_copy.start()

    for slot in range(1, T):
        output_copy(slot).start()
    own_out = pltpu.make_async_copy(yb.at[tensor], result.at[tensor], lsem.at[0])
    own_out.start()
    own_out.wait()
    keep_x.wait()
    keep_p.wait()
    for keep in keeps:
        keep.wait()
    for index in (NI - 2, NI - 1):
        keep_a(index, index % 2).wait()
    for slot in range(1, T):
        output_copy(slot).wait()
        vector_copy(slot).wait_send()
        input_copy(slot).wait_send()
        for index in range(dm.NCH):
            weight_copy(slot, index).wait_send()

    @pl.when(lower)
    def _():
        stream_copy.wait_send()


def partner_dynamic(dm, place, slot):
    bit = 1
    while bit < dm.T:
        take = lax.rem(lax.div(slot, bit), 2)
        place = place + take * (bit - 2 * bit * lax.rem(lax.div(place, bit), 2))
        bit *= 2
    return place


def forward_call(dm, xin, vectors, wqkv, wout, wup, wdown):
    T, W, D, RP, RL, C, NI, FL = dm.T, dm.W, dm.D, dm.RP, dm.RL, dm.C, dm.NI, dm.FL
    sds = jax.ShapeDtypeStruct
    outs = (
        sds((T, 3, D, W), BF16), sds((T, W, D), BF16), sds((T, D, FL), BF16), sds((T, FL, D), BF16),
        sds((T, RP, W), BF16), sds((T, RP, W), BF16),
        sds((T, RL, W), BF16), sds((T, RL, W), BF16), sds((T, RL, W), BF16), sds((T, RL, W), BF16),
        sds((RP, D), F32), sds((NI, RP, C), F32), sds((T, VECTOR_ROWS, W), F32), sds((T, RP, W), BF16),
    )
    dma = pltpu.SemaphoreType.DMA
    scratch = [
        pltpu.VMEM((T, RP, W), BF16), pltpu.VMEM((RP, D), BF16), pltpu.VMEM((2, 3, D, W), BF16),
        pltpu.VMEM((D, D), BF16), pltpu.VMEM((2, D, C), BF16), pltpu.VMEM((2, C, D), BF16),
        pltpu.VMEM((2, RP, C), F32), pltpu.VMEM((RP, C), BF16), pltpu.VMEM((RP, D), F32),
        pltpu.VMEM((RP, D), BF16), pltpu.VMEM((T, RP, W), BF16), pltpu.VMEM((NI, 1, C), F32),
        pltpu.VMEM((T, VECTOR_ROWS, W), F32),
        pltpu.VMEM((T, RL, W), BF16), pltpu.VMEM((T, RL, W), BF16), pltpu.VMEM((T, RL, W), BF16), pltpu.VMEM((T, RL, W), BF16),
        dma((T, dm.NCH)), dma((T, dm.NCH)), dma((T,)), dma((T,)), dma((T,)), dma((T,)), dma((T,)), dma((T,)),
        dma((2,)), dma((8,)), dma((2 + T,)), dma((6,)),
    ]
    return pl.pallas_call(
        functools.partial(forward_kernel, dm),
        out_shape=outs,
        in_specs=[ANY] * 6,
        out_specs=[ANY] * len(outs),
        scratch_shapes=scratch,
        name="layer_forward",
        compiler_params=pltpu.CompilerParams(
            collective_id=0, has_side_effects=True, vmem_limit_bytes=VMEM_BYTES
        ),
    )(xin, vectors, wqkv, wout, wup, wdown)


def packed_vectors(dm, ln1_gain, ln1_bias, qv_bias, out_bias, ln2_gain, ln2_bias, fc1_bias, fc2_bias):
    rows = [ln1_gain, ln1_bias, qv_bias[0], out_bias, ln2_gain, ln2_bias, fc2_bias, fc1_bias]
    flat = jnp.concatenate([row.reshape(-1, dm.W) for row in rows], axis=0)
    return jnp.pad(flat, ((0, VECTOR_ROWS - flat.shape[0]), (0, 0)))


def padded_rows(dm, array):
    return jnp.pad(array, ((0, 0), (0, dm.RP - dm.tok), (0, 0)))


def dot_rows(left, right):
    return lax.dot_general(left, right, (((0,), (0,)), ((), ())), preferred_element_type=F32)


def fold(rows):
    total = rows[0:8, :]
    for first in range(8, rows.shape[0], 8):
        total = total + rows[first : first + 8, :]
    return total


def norm_rows_back(grad, hat, inv, gain, width):
    scaled = grad * gain
    mean = jnp.sum(scaled, axis=1, keepdims=True) * (1.0 / width)
    along = jnp.sum(scaled * hat, axis=1, keepdims=True) * (1.0 / width)
    return inv * (scaled - mean - hat * along)


def backward_kernel(
    dm,
    xc, xkeep, qkeep, kkeep, vkeep, okeep, hkeep, akeep, spkeep,
    wqkv, wout, wup, wdown, gqkv, gout, gup, gdown,
    dqkv, dout, dup, ddown, result, flat_sums, head_sums, up_sums,
    arr, dyb, acc, dh, hh, dhb, gs, das, n1t, n2t, nb, q, k, v, o, do, dq, dk, dv, xx,
    w1b, w2b, ab, dgb, wob, wq, s1, s2, yb, spb, fs, hs, us, dva, dka,
    ssem, osend, orecv, lsem, lw, lq, lg,
):
    section, tensor = lax.axis_index("section"), lax.axis_index("tensor")
    T, W, D, RP, RL, C, NI = dm.T, dm.W, dm.D, dm.RP, dm.RL, dm.C, dm.NI
    lower, upper = section == 0, section == 1
    own = (wqkv, wout, wup, wdown)
    real = pl.ds(0, RP)

    def source_of(slot, index):
        if slot == 0:
            return chunk_refs(dm, index, *own)
        return chunk_refs(dm, index, gqkv.at[slot], gout.at[slot], gup.at[slot], gdown.at[slot])

    stream_copy = pltpu.make_async_remote_copy(
        src_ref=arr,
        dst_ref=arr,
        send_sem=ssem.at[0],
        recv_sem=ssem.at[1],
        device_id={"section": 1 - section},
    )

    def output_copy(slot):
        return pltpu.make_async_remote_copy(
            src_ref=yb.at[partner(tensor, slot)],
            dst_ref=result.at[tensor],
            send_sem=osend.at[slot],
            recv_sem=orecv.at[slot],
            device_id={"tensor": partner(tensor, slot)},
        )

    def load_ff(index, parity):
        slot, c = dm.order[index]
        return [
            pltpu.make_async_copy(source_of(slot, 2 + 2 * c), w1b.at[parity], lw.at[parity]),
            pltpu.make_async_copy(source_of(slot, 3 + 2 * c), w2b.at[parity], lw.at[2 + parity]),
            pltpu.make_async_copy(akeep.at[index], ab.at[parity], lw.at[4 + parity]),
        ]

    def fetch_ff(which):
        for index in range(NI):

            @pl.when(which == index)
            def _():
                for load in load_ff(index, index % 2):
                    load.start()

    fetch_ff(0)
    loads = [
        pltpu.make_async_copy(source, target, lsem.at[number])
        for number, (source, target) in enumerate(
            ((spkeep, spb), (hkeep, hh), (qkeep, q), (kkeep, k), (vkeep, v), (okeep, o), (xkeep, xx))
        )
    ]
    for load in loads:
        load.start()
    out_loads = [
        pltpu.make_async_copy(source_of(slot, 1), wob.at[pl.ds(slot * W, W)], lq.at[2 + slot])
        for slot in range(T)
    ]
    for load in out_loads:
        load.start()

    meet(dm, section, tensor)

    @pl.when(upper)
    def _():
        load = pltpu.make_async_copy(xc, arr, lsem.at[7])
        load.start()
        load.wait()

    tail_rows = pl.ds(RP, RL - RP)
    blank = jnp.zeros((RL - RP, D), BF16)
    dyb[tail_rows, :] = blank
    dhb[tail_rows, :] = blank
    nb[tail_rows, :] = blank
    for index in range(NI):
        gs[index, tail_rows, :] = blank[:, :C]
        das[index, tail_rows, :] = blank[:, :C]
    for slot in range(T):
        do[slot, tail_rows, :] = blank[:, :W]
    acc[...] = jnp.zeros_like(acc)
    fs[...] = jnp.zeros_like(fs)
    hs[...] = jnp.zeros_like(hs)

    @pl.when(lower)
    def _():
        stream_copy.wait_recv()

    def spread(r, _):
        rows = pl.ds(pl.multiple_of(r * STEP, STEP), STEP)
        dyb[rows, :] = block_rows(dm, arr, rows)
        return 0

    lax.fori_loop(0, RP // STEP, spread, 0)

    def feed_back(index, _):
        parity = lax.rem(index, 2)
        for load in load_ff(0, parity):
            load.wait()

        @pl.when(index + 1 < NI)
        def _():
            fetch_ff(index + 1)

        dgb[...] = dot_last(dyb[real, :], w2b[parity])

        def bend(r, total):
            rows = pl.ds(pl.multiple_of(r * STEP, STEP), STEP)
            a = ab[parity, rows, :]
            cdf = 0.5 * (1.0 + lax.erf(a * ROOT_HALF))
            gs[index, rows, :] = (a * cdf).astype(BF16)
            da = dgb[rows, :] * (cdf + a * jnp.exp(-0.5 * a * a) * GAUSS_FACTOR)
            das[index, rows, :] = da.astype(BF16)
            return total + fold(da)

        total = lax.fori_loop(0, RP // STEP, bend, jnp.zeros((8, C), F32))
        us[index] = jnp.sum(total, axis=0, keepdims=True)
        for n in range(D // 256):
            cols = pl.ds(n * 256, 256)
            acc[:, cols] += dot_last(das[index, real, :], w1b[parity, cols, :])
        return 0

    lax.fori_loop(0, NI, feed_back, 0)

    for load in loads:
        load.wait()
    for load in out_loads:
        load.wait()
    gain2, bias2 = full_vector(dm, spb, LN2_GAIN), full_vector(dm, spb, LN2_BIAS)

    def second_norm(r, _):
        rows = pl.ds(pl.multiple_of(r * STEP, STEP), STEP)
        hat, inv = norm_rows(hh[rows, :], D)
        grad = acc[rows, :]
        dy = dyb[rows, :].astype(F32)
        fs[0] += fold(grad * hat)
        fs[1] += fold(grad)
        whole = dy + norm_rows_back(grad, hat, inv, gain2, D)
        dh[rows, :] = whole
        dhb[rows, :] = whole.astype(BF16)
        fs[2] += fold(whole)
        fs[3] += fold(dy)
        nb[rows, :] = (hat * gain2 + bias2).astype(BF16)
        return 0

    lax.fori_loop(0, RP // STEP, second_norm, 0)

    def turn(target):
        for n in range(D // 256):
            cols = pl.ds(n * 256, 256)
            target[cols, :] = nb[:, cols].T

    turn(n2t)

    def put_ff(index, parity):
        slot, c = dm.order[index]
        return [
            pltpu.make_async_copy(s1.at[parity], dup.at[slot, :, pl.ds(c * C, C)], lg.at[parity]),
            pltpu.make_async_copy(s2.at[parity], ddown.at[slot, pl.ds(c * C, C), :], lg.at[2 + parity]),
        ]

    def feed_weights():
        def one(index, _):
            parity = lax.rem(index, 2)

            @pl.when(index >= 2)
            def _():
                for put in put_ff(0, parity):
                    put.wait()

            for n in range(D // 256):
                cols = pl.ds(n * 256, 256)
                s1[parity, cols, :] = dot_plain(n2t[cols, :], das[index]).astype(BF16)
            for n in range(C // 256):
                cols = pl.ds(n * 256, 256)
                s2[parity, cols, :] = dot_rows(gs[index, :, cols], dyb[...]).astype(BF16)
            for j in range(NI):

                @pl.when(index == j)
                def _():
                    for put in put_ff(j, j % 2):
                        put.start()

            return 0

        lax.fori_loop(0, NI, one, 0)
        for parity in range(2):
            for put in put_ff(0, parity):
                put.wait()

    @pl.when(lower)
    def _():
        feed_weights()

    for slot in range(T):
        do[slot, real, :] = dot_last(dhb[real, :], wob[pl.ds(slot * W, W), :]).astype(BF16)

    mask_full = half_masks(RL)
    row = lax.broadcasted_iota(jnp.int32, (RL, 1), 0)
    key_bias = jnp.where(row < dm.tok, 0.0, MASKED).astype(F32)
    scale = HEAD_DIM**-0.5
    blocks = [(first, min(256, RL - first)) for first in range(0, RL, 256)]

    def heads(slot, _):
        for pair in range(W // 128):
            lanes = slice(pair * 128, pair * 128 + 128)
            keys, values = k[slot, :, lanes], v[slot, :, lanes]
            for number, (first, size) in enumerate(blocks):
                rows = slice(first, first + size)
                query, grad = q[slot, rows, lanes], do[slot, rows, lanes]
                dq_block = jnp.zeros((size, 128), F32)
                dk_block, dv_block = jnp.zeros((RL, 128), F32), jnp.zeros((RL, 128), F32)
                for half in range(2):
                    mask = mask_full[half][:size]
                    query_h = jnp.where(mask, query, jnp.zeros_like(query))
                    grad_h = jnp.where(mask, grad, jnp.zeros_like(grad))
                    keys_h = jnp.where(mask_full[half], keys, jnp.zeros_like(keys))
                    s = dot_last(keys, query_h * jnp.asarray(scale, BF16)) + key_bias
                    e = jnp.exp(s - jnp.max(s, axis=0, keepdims=True))
                    p = e * (1.0 / jnp.sum(e, axis=0, keepdims=True))
                    dp = dot_last(values, grad_h)
                    delta = jnp.sum(p * dp, axis=0, keepdims=True)
                    ds = (p * (dp - delta) * scale).astype(BF16)
                    dv_block = dv_block + dot_plain(p.astype(BF16), grad_h)
                    dk_block = dk_block + dot_plain(ds, query_h)
                    dq_block = dq_block + dot_rows(ds, keys_h)
                dq[slot, rows, lanes] = dq_block.astype(BF16)
                hs[slot, 0, :, lanes] += fold(dq_block)
                if number == 0:
                    dka[...] = dk_block
                    dva[...] = dv_block
                else:
                    dka[...] += dk_block
                    dva[...] += dv_block
            dk[slot, :, lanes] = dka[...].astype(BF16)
            total = dva[...]
            dv[slot, :, lanes] = total.astype(BF16)
            hs[slot, 1, :, lanes] += fold(total)
        return 0

    lax.fori_loop(0, T, heads, 0)

    def load_qkv(slot, parity):
        return pltpu.make_async_copy(source_of(slot, 0), wq.at[parity], lq.at[parity])

    load_qkv(0, 0).start()
    for slot in range(T):
        load_qkv(slot, slot % 2).wait()
        if slot + 1 < T:
            load_qkv(slot + 1, (slot + 1) % 2).start()
        for n in range(D // 256):
            cols = pl.ds(n * 256, 256)
            part = dot_last(dq[slot, real, :], wq[slot % 2, 0, cols, :])
            part = part + dot_last(dk[slot, real, :], wq[slot % 2, 1, cols, :])
            part = part + dot_last(dv[slot, real, :], wq[slot % 2, 2, cols, :])
            if slot == 0:
                acc[:, cols] = part
            else:
                acc[:, cols] += part

    gain1, bias1 = full_vector(dm, spb, LN1_GAIN), full_vector(dm, spb, LN1_BIAS)

    def first_norm(r, _):
        rows = pl.ds(pl.multiple_of(r * STEP, STEP), STEP)
        hat, inv = norm_rows(block_rows(dm, xx, rows).astype(F32), D)
        grad = acc[rows, :]
        fs[4] += fold(grad * hat)
        fs[5] += fold(grad)
        whole = dh[rows, :] + norm_rows_back(grad, hat, inv, gain1, D)
        nb[rows, :] = (hat * gain1 + bias1).astype(BF16)
        low = whole.astype(BF16)
        for j in range(T):
            yb[j, rows, :] = whole[:, j * W : (j + 1) * W]
            xx[j, rows, :] = low[:, j * W : (j + 1) * W]
        return 0

    lax.fori_loop(0, RP // STEP, first_norm, 0)

    down_copy = pltpu.make_async_remote_copy(
        src_ref=xx,
        dst_ref=arr,
        send_sem=ssem.at[0],
        recv_sem=ssem.at[1],
        device_id={"section": 1 - section},
    )

    @pl.when(upper)
    def _():
        down_copy.start()

    for slot in range(1, T):
        output_copy(slot).start()
    own_out = pltpu.make_async_copy(yb.at[tensor], result.at[tensor], lsem.at[0])
    own_out.start()
    turn(n1t)

    def put_qkv(slot, parity):
        return [
            pltpu.make_async_copy(s1.at[parity, :, pl.ds(0, W)], dqkv.at[slot, 0], lg.at[4 + parity]),
            pltpu.make_async_copy(s1.at[parity, :, pl.ds(C // 2, W)], dqkv.at[slot, 1], lg.at[6 + parity]),
        ]

    for slot in range(T):
        number = 0
        s2[slot % 2, pl.ds(0, W), :] = dot_rows(o[slot], dhb[...]).astype(BF16)
        put_out = pltpu.make_async_copy(s2.at[slot % 2, pl.ds(0, W), :], dout.at[slot], lg.at[4])
        put_out.start()
        for source in (dq, dk, dv):
            for n in range(D // 256):
                cols = pl.ds(n * 256, 256)
                s1[number % 2, cols, pl.ds(0, W)] = dot_plain(n1t[cols, :], source[slot]).astype(BF16)
            put = pltpu.make_async_copy(s1.at[number % 2, :, pl.ds(0, W)], dqkv.at[slot, number], lg.at[number % 2])
            put.start()
            put.wait()
            number += 1
        put_out.wait()

    @pl.when(upper)
    def _():
        feed_weights()

    keeps = []
    for number, (source, target) in enumerate(((fs, flat_sums), (hs, head_sums), (us, up_sums))):
        keeps.append(pltpu.make_async_copy(source, target, lsem.at[1 + number]))
        keeps[-1].start()
    for keep in keeps:
        keep.wait()
    own_out.wait()
    for slot in range(1, T):
        output_copy(slot).wait()

    @pl.when(upper)
    def _():
        down_copy.wait_send()


def backward_call(dm, kept, own):
    T, W, D, RP, RL, C, NI, FL = dm.T, dm.W, dm.D, dm.RP, dm.RL, dm.C, dm.NI, dm.FL
    sds = jax.ShapeDtypeStruct
    gathered, rest = kept[:4], kept[4:13]
    outs = (
        sds((T, 3, D, W), BF16), sds((T, W, D), BF16), sds((T, D, FL), BF16), sds((T, FL, D), BF16),
        sds((T, RP, W), F32), sds((6, 8, D), F32), sds((T, 2, 8, W), F32), sds((NI, 1, C), F32),
    )
    dma = pltpu.SemaphoreType.DMA
    heads = pltpu.VMEM((T, RL, W), BF16)
    scratch = [
        pltpu.VMEM((T, RP, W), BF16), pltpu.VMEM((RL, D), BF16), pltpu.VMEM((RP, D), F32), pltpu.VMEM((RP, D), F32),
        pltpu.VMEM((RP, D), F32), pltpu.VMEM((RL, D), BF16), pltpu.VMEM((NI, RL, C), BF16), pltpu.VMEM((NI, RL, C), BF16),
        pltpu.VMEM((D, RL), BF16), pltpu.VMEM((D, RL), BF16), pltpu.VMEM((RL, D), BF16),
        heads, heads, heads, heads, heads, heads, heads, heads, pltpu.VMEM((T, RP, W), BF16),
        pltpu.VMEM((2, D, C), BF16), pltpu.VMEM((2, C, D), BF16), pltpu.VMEM((2, RP, C), F32), pltpu.VMEM((RP, C), F32),
        pltpu.VMEM((D, D), BF16), pltpu.VMEM((2, 3, D, W), BF16), pltpu.VMEM((2, D, C), BF16), pltpu.VMEM((2, C, D), BF16),
        pltpu.VMEM((T, RP, W), F32), pltpu.VMEM((T, VECTOR_ROWS, W), F32),
        pltpu.VMEM((6, 8, D), F32), pltpu.VMEM((T, 2, 8, W), F32), pltpu.VMEM((NI, 1, C), F32),
        pltpu.VMEM((RL, 128), F32), pltpu.VMEM((RL, 128), F32),
        dma((2,)), dma((T,)), dma((T,)), dma((8,)), dma((6,)), dma((2 + T,)), dma((8,)),
    ]
    return pl.pallas_call(
        functools.partial(backward_kernel, dm),
        out_shape=outs,
        in_specs=[ANY] * 17,
        out_specs=[ANY] * len(outs),
        scratch_shapes=scratch,
        name="layer_backward",
        compiler_params=pltpu.CompilerParams(
            collective_id=1, has_side_effects=True, vmem_limit_bytes=VMEM_BYTES
        ),
    )(*rest, *own, *gathered)


def shards(
    images, cotangent, ln1_gain, ln1_bias, qkv_weight, qv_bias, out_weight, out_bias,
    ln2_gain, ln2_bias, fc1_weight, fc1_bias, fc2_weight, fc2_bias,
):
    dm = sizes_of(images, fc1_weight, lax.axis_size("tensor"))
    T, W, D = dm.T, dm.W, dm.D
    section, tensor = lax.axis_index("section"), lax.axis_index("tensor")
    xin = padded_rows(dm, jnp.where(section == 0, images[:, 0], cotangent[:, 0]))
    vectors = packed_vectors(
        dm, ln1_gain[0], ln1_bias[0], qv_bias, out_bias[0], ln2_gain[0], ln2_bias[0], fc1_bias[0], fc2_bias[0]
    )
    own = (qkv_weight[0], out_weight[0], fc1_weight[0], fc2_weight[0])
    kept = forward_call(dm, xin, vectors, *own)
    section_out = kept[13][: dm.micro, : dm.tok][None, :, None]
    dqkv, dout, dup, ddown, result, flat_sums, head_sums, up_sums = backward_call(dm, kept, own)
    input_grads = result[: dm.micro, : dm.tok][None, :, None]

    def reduced(parts):
        if T > dm.micro:
            parts = jnp.where(tensor < dm.micro, parts, jnp.zeros_like(parts))
        bit = 1
        while bit < T:
            keep = [slot for slot in range(parts.shape[0]) if slot % 2 == 0]
            give = [slot for slot in range(parts.shape[0]) if slot % 2 == 1]
            pairs = [(source, source ^ bit) for source in range(T)]
            sent = lax.ppermute(parts[jnp.array(give)], "tensor", pairs)
            parts = parts[jnp.array(keep)].astype(F32) + sent.astype(F32)
            if parts.shape[0] > 1 or True:
                parts = parts.astype(BF16)
            bit *= 2
        return lax.psum(parts[0], "dp").astype(F32)

    absolute = jnp.sum(flat_sums, axis=1).reshape(6, T, W)
    by_slot = jnp.sum(head_sums, axis=2)
    up_rows = [None] * T
    for index, (slot, c) in enumerate(dm.order):
        up_rows[slot] = (up_rows[slot] or []) + [up_sums[index].reshape(-1, W)]
    by_slot = jnp.concatenate([by_slot, jnp.stack([jnp.concatenate(rows, axis=0) for rows in up_rows])], axis=1)
    places = jnp.stack([partner(tensor, slot) for slot in range(T)])
    relative = jnp.zeros_like(by_slot).at[places].set(by_slot)
    small = jnp.concatenate([absolute.transpose(1, 0, 2), relative], axis=1)
    if T > dm.micro:
        small = jnp.where(tensor < dm.micro, small, jnp.zeros_like(small))
    small = lax.psum(small, ("tensor", "dp"))
    small = lax.dynamic_index_in_dim(small, tensor, 0, keepdims=False)
    g2, b2, ob, db, g1, b1 = (small[i][None] for i in range(6))
    qv = small[6:8][None]
    ub = small[8:].reshape(1, -1)
    return (
        section_out, input_grads, g1, b1, reduced(dqkv)[None], qv, reduced(dout)[None], ob, g2, b2,
        reduced(dup)[None], ub, reduced(ddown)[None], db,
    )


def solution(mesh):
    vector = P("section", "tensor")
    rows = P(None, "dp", None, "tensor")
    placed_rows = P("section", None, "dp", None, "tensor")
    qkv, qv = P("section", None, None, "tensor"), P("section", None, "tensor")
    by_row, by_column = P("section", "tensor", None), P("section", None, "tensor")
    return jax.shard_map(
        shards,
        mesh=mesh,
        in_specs=(rows, rows, vector, vector, qkv, qv, by_row, vector, vector, vector, by_column, vector, by_row, vector),
        out_specs=(
            placed_rows, placed_rows, vector, vector, qkv, qv, by_row, vector, vector, vector,
            by_column, vector, by_row, vector,
        ),
        check_vma=False,
    )
```

```python
import functools
import types

import jax
import jax.numpy as jnp
from jax import lax
from jax.experimental import pallas as pl
from jax.experimental.pallas import tpu as pltpu
from jax.sharding import PartitionSpec as P

BF16, F32 = jnp.bfloat16, jnp.float32
HEAD_DIM = 64
EPSILON = 1e-06
ROOT_HALF = 0.7071067811865476
GAUSS_FACTOR = 0.3989422804014327
MASKED = -1e30
STEP = 32
ANY = pl.BlockSpec(memory_space=pl.ANY)
VMEM_BYTES = 67043328

LN1_GAIN, LN1_BIAS, Q_BIAS, V_BIAS, OUT_BIAS, LN2_GAIN, LN2_BIAS, FC2_BIAS, FC1_BIAS = range(9)
VECTOR_ROWS = 16


def flip(place, bit):
    return place + bit - 2 * bit * lax.rem(lax.div(place, bit), 2)


def partner(place, slot):
    bit = 1
    while bit <= slot:
        if slot & bit:
            place = flip(place, bit)
        bit *= 2
    return place


def sizes_of(images, fc1_weight, tensor):
    micro, _, tok, width = images.shape
    dm = types.SimpleNamespace()
    dm.T, dm.W, dm.micro, dm.tok = tensor, width, micro, tok
    dm.D = width * tensor
    dm.FL = fc1_weight.shape[2]
    dm.RP = -(-tok // STEP) * STEP
    dm.RL = -(-tok // 128) * 128
    dm.C = min(512, dm.FL)
    dm.NC = dm.FL // dm.C
    dm.order = [
        (2 * p + half, c) for p in range(tensor // 2) for c in range(dm.NC) for half in range(2)
    ]
    dm.NI = len(dm.order)
    dm.NCH = 2 + 2 * dm.NC
    return dm


def full_vector(dm, vectors, row):
    return jnp.concatenate([vectors[j, row : row + 1, :] for j in range(dm.T)], axis=1)


def norm_rows(rows, width):
    mean = jnp.sum(rows, axis=1, keepdims=True) * (1.0 / width)
    var = jnp.sum(rows * rows, axis=1, keepdims=True) * (1.0 / width) - mean * mean
    inv = lax.rsqrt(var + EPSILON)
    return (rows - mean) * inv, inv


def block_rows(dm, ref, rows):
    return jnp.concatenate([ref[j, rows, :] for j in range(dm.T)], axis=1)


def dot_last(left, right):
    return lax.dot_general(left, right, (((1,), (1,)), ((), ())), preferred_element_type=F32)


def dot_plain(left, right):
    return lax.dot_general(left, right, (((1,), (0,)), ((), ())), preferred_element_type=F32)


def half_masks(rows):
    lane = lax.broadcasted_iota(jnp.int32, (rows, 128), 1)
    return [lane < HEAD_DIM, lane >= HEAD_DIM]


def chunk_refs(dm, index, qkv, out, up, down):
    if index == 0:
        return qkv
    if index == 1:
        return out
    c = (index - 2) // 2
    if index % 2 == 0:
        return up.at[:, pl.ds(c * dm.C, dm.C)]
    return down.at[pl.ds(c * dm.C, dm.C), :]


def meet(dm, section, tensor):
    barrier = pltpu.get_barrier_semaphore()
    for slot in range(1, dm.T):
        pl.semaphore_signal(barrier, inc=1, device_id={"tensor": partner(tensor, slot)})
    pl.semaphore_signal(barrier, inc=1, device_id={"section": 1 - section})
    pl.semaphore_wait(barrier, dm.T)


def forward_kernel(
    dm,
    xin, spin, wqkv, wout, wup, wdown,
    gqkv, gout, gup, gdown, xc, xkeep, qkeep, kkeep, vkeep, okeep, hkeep, akeep, spkeep, result,
    xarr, n1, wq, wob, w1b, w2b, ab, gb, acc, n2, yb, b1r, spb, q, k, v, o,
    wsend, wrecv, xsend, xrecv, psend, precv, osend, orecv, ssem, lsem, lw, la,
):
    section, tensor = lax.axis_index("section"), lax.axis_index("tensor")
    T, W, D, RP, RL, C, NI = dm.T, dm.W, dm.D, dm.RP, dm.RL, dm.C, dm.NI
    lower, upper = section == 0, section == 1
    own = (wqkv, wout, wup, wdown)

    def slot_refs(slot):
        return (gqkv.at[slot], gout.at[slot], gup.at[slot], gdown.at[slot])

    def weight_copy(slot, index):
        relay = slot > 1 and slot % 2 == 1
        source = chunk_refs(dm, index, *(slot_refs(slot - 1) if relay else own))
        return pltpu.make_async_remote_copy(
            src_ref=source,
            dst_ref=chunk_refs(dm, index, *slot_refs(slot)),
            send_sem=wsend.at[slot, index],
            recv_sem=wrecv.at[slot, index],
            device_id={"tensor": flip(tensor, 1) if relay else partner(tensor, slot)},
        )

    def input_copy(slot):
        return pltpu.make_async_remote_copy(
            src_ref=xin.at[lax.rem(partner(tensor, slot), dm.micro)],
            dst_ref=xc.at[tensor],
            send_sem=xsend.at[slot],
            recv_sem=xrecv.at[slot],
            device_id={"tensor": partner(tensor, slot)},
        )

    def vector_copy(slot):
        return pltpu.make_async_remote_copy(
            src_ref=spin,
            dst_ref=spb.at[tensor],
            send_sem=psend.at[slot],
            recv_sem=precv.at[slot],
            device_id={"tensor": partner(tensor, slot)},
        )

    def output_copy(slot):
        return pltpu.make_async_remote_copy(
            src_ref=yb.at[partner(tensor, slot)],
            dst_ref=result.at[tensor],
            send_sem=osend.at[slot],
            recv_sem=orecv.at[slot],
            device_id={"tensor": partner(tensor, slot)},
        )

    stream_copy = pltpu.make_async_remote_copy(
        src_ref=yb,
        dst_ref=xarr,
        send_sem=ssem.at[0],
        recv_sem=ssem.at[1],
        device_id={"section": 1 - section},
    )

    meet(dm, section, tensor)
    for slot in range(1, T):
        vector_copy(slot).start()
        input_copy(slot).start()
    own_vec = pltpu.make_async_copy(spin, spb.at[tensor], lsem.at[0])
    own_vec.start()
    own_in = pltpu.make_async_copy(xin.at[lax.rem(tensor, dm.micro)], xc.at[tensor], lsem.at[1])
    own_in.start()
    direct = [slot for slot in range(1, T) if slot == 1 or slot % 2 == 0]
    for index in range(dm.NCH):
        for slot in direct:
            weight_copy(slot, index).start()

    def relay(slot, index):
        weight_copy(slot, index).wait_recv()
        weight_copy(slot + 1, index).start()

    own_vec.wait()
    own_in.wait()
    for slot in range(1, T):
        vector_copy(slot).wait_recv()
        input_copy(slot).wait_recv()

    @pl.when(upper)
    def _():
        for index in range(dm.NCH):
            for slot in range(2, T, 2):
                relay(slot, index)
        stream_copy.wait_recv()

    @pl.when(lower)
    def _():
        load = pltpu.make_async_copy(xc, xarr, lsem.at[0])
        load.start()
        load.wait()

    def arrive(slot, index):
        if slot == 0:
            return
        if slot % 2 == 0:

            @pl.when(lower)
            def _():
                relay(slot, index)

        else:
            weight_copy(slot, index).wait_recv()

    def source_of(slot, index):
        return chunk_refs(dm, index, *(own if slot == 0 else slot_refs(slot)))

    keep_x = pltpu.make_async_copy(xarr, xkeep, lsem.at[1])
    keep_x.start()
    keep_p = pltpu.make_async_copy(spb, spkeep, lsem.at[2])
    keep_p.start()

    gain, bias = full_vector(dm, spb, LN1_GAIN), full_vector(dm, spb, LN1_BIAS)

    def first_norm(r, _):
        rows = pl.ds(pl.multiple_of(r * STEP, STEP), STEP)
        hat, _inv = norm_rows(block_rows(dm, xarr, rows).astype(F32), D)
        n1[rows, :] = (hat * gain + bias).astype(BF16)
        return 0

    lax.fori_loop(0, RP // STEP, first_norm, 0)

    for index, (slot, c) in enumerate(dm.order):
        shard = spb[partner(tensor, slot)]
        per = C // W
        first = FC1_BIAS + c * per
        b1r[index] = jnp.concatenate([shard[first + i : first + i + 1, :] for i in range(per)], axis=1)

    pad = jnp.zeros((RL - RP, W), BF16)
    for slot in range(T):
        for ref in (q, k, v):
            ref[slot, pl.ds(RP, RL - RP), :] = pad

    def load_qkv(slot, parity):
        return pltpu.make_async_copy(source_of(slot, 0), wq.at[parity], lw.at[parity])

    def fetch_qkv(which):
        for slot in range(T):

            @pl.when(which == slot)
            def _():
                arrive(slot, 0)
                load_qkv(slot, slot % 2).start()

    masks = half_masks(128)
    lane = lax.broadcasted_iota(jnp.int32, (1, RL), 1)
    key_bias = jnp.where(lane < dm.tok, 0.0, MASKED).astype(F32)

    fetch_qkv(0)

    def heads(slot, _):
        parity = lax.rem(slot, 2)
        pltpu.make_async_copy(gqkv.at[0], wq.at[parity], lw.at[parity]).wait()
        early = jnp.logical_or(upper, slot < 1)

        @pl.when(jnp.logical_and(early, slot + 1 < T))
        def _():
            fetch_qkv(slot + 1)

        shard = spb[partner_dynamic(dm, tensor, slot)]
        rows = pl.ds(0, RP)
        q[slot, rows, :] = (dot_plain(n1[...], wq[parity, 0]) + shard[Q_BIAS : Q_BIAS + 1]).astype(BF16)
        k[slot, rows, :] = dot_plain(n1[...], wq[parity, 1]).astype(BF16)
        v[slot, rows, :] = (dot_plain(n1[...], wq[parity, 2]) + shard[V_BIAS : V_BIAS + 1]).astype(BF16)

        for pair in range(W // 128):
            lanes = slice(pair * 128, pair * 128 + 128)

            def block(b, _):
                rows = pl.ds(pl.multiple_of(b * 128, 128), 128)
                query = q[slot, rows, lanes] * jnp.asarray(HEAD_DIM**-0.5, BF16)
                parts = []
                for mask in masks:
                    s = dot_last(jnp.where(mask, query, jnp.zeros_like(query)), k[slot, :, lanes]) + key_bias
                    e = jnp.exp(s - jnp.max(s, axis=1, keepdims=True))
                    p = (e * (1.0 / jnp.sum(e, axis=1, keepdims=True))).astype(BF16)
                    parts.append(dot_plain(p, v[slot, :, lanes]))
                o[slot, rows, lanes] = jnp.where(masks[0], parts[0], parts[1]).astype(BF16)
                return 0

            lax.fori_loop(0, RL // 128, block, 0, unroll=True)

        @pl.when(jnp.logical_and(jnp.logical_not(early), slot + 1 < T))
        def _():
            fetch_qkv(slot + 1)

        return 0

    lax.fori_loop(0, T, heads, 0)

    keeps = []
    for number, (source, target) in enumerate(((q, qkeep), (k, kkeep), (v, vkeep), (o, okeep))):
        keeps.append(pltpu.make_async_copy(source, target, la.at[2 + number]))
        keeps[-1].start()

    loads = []
    for slot in range(T):
        arrive(slot, 1)
        loads.append(
            pltpu.make_async_copy(source_of(slot, 1), wob.at[pl.ds(slot * W, W)], lw.at[2 + slot])
        )
        loads[-1].start()

    def arrive_ff(index):
        slot, c = dm.order[index]
        arrive(slot, 2 + 2 * c)
        arrive(slot, 3 + 2 * c)

    def load_ff(index, parity):
        slot, c = dm.order[index]
        return [
            pltpu.make_async_copy(source_of(slot, 2 + 2 * c), w1b.at[parity], lsem.at[3 + parity]),
            pltpu.make_async_copy(source_of(slot, 3 + 2 * c), w2b.at[parity], lsem.at[5 + parity]),
        ]

    def fetch_ff(which):
        for index in range(NI):

            @pl.when(which == index)
            def _():
                arrive_ff(index)
                for load in load_ff(index, index % 2):
                    load.start()

    fetch_ff(0)
    for load in loads:
        load.wait()
    attended = jnp.concatenate([o[slot, pl.ds(0, RP), :] for slot in range(T)], axis=1)
    for n in range(D // 256):
        acc[:, pl.ds(n * 256, 256)] = dot_plain(attended, wob[:, pl.ds(n * 256, 256)])

    out_bias = full_vector(dm, spb, OUT_BIAS)
    gain2, bias2 = full_vector(dm, spb, LN2_GAIN), full_vector(dm, spb, LN2_BIAS)
    down_bias = full_vector(dm, spb, FC2_BIAS)

    def second_norm(r, _):
        rows = pl.ds(pl.multiple_of(r * STEP, STEP), STEP)
        hidden = block_rows(dm, xarr, rows).astype(F32) + (acc[rows, :] + out_bias)
        hat, _inv = norm_rows(hidden, D)
        n2[rows, :] = (hat * gain2 + bias2).astype(BF16)
        acc[rows, :] = hidden
        return 0

    lax.fori_loop(0, RP // STEP, second_norm, 0)
    keep_h = pltpu.make_async_copy(acc, hkeep, lsem.at[0])
    keep_h.start()
    keep_h.wait()

    def keep_a(index, parity):
        return pltpu.make_async_copy(ab.at[parity], akeep.at[index], la.at[parity])

    def feed(index, _):
        parity = lax.rem(index, 2)
        for load in load_ff(0, parity):
            load.wait()
        early = jnp.logical_or(upper, index + 1 < 2 * dm.NC)

        @pl.when(jnp.logical_and(early, index + 1 < NI))
        def _():
            fetch_ff(index + 1)

        @pl.when(index >= 2)
        def _():
            keep_a(index - 2, parity).wait()

        ab[parity] = dot_plain(n2[...], w1b[parity])
        shift = b1r[index]

        def bend(r, _):
            rows = pl.ds(pl.multiple_of(r * STEP, STEP), STEP)
            a = ab[parity, rows, :] + shift
            ab[parity, rows, :] = a
            gb[rows, :] = (0.5 * a * (1.0 + lax.erf(a * ROOT_HALF))).astype(BF16)
            return 0

        lax.fori_loop(0, RP // STEP, bend, 0)
        keep_a(index, parity).start()
        for n in range(D // 256):
            cols = pl.ds(n * 256, 256)
            acc[:, cols] += dot_plain(gb[...], w2b[parity, :, cols])

        @pl.when(jnp.logical_and(jnp.logical_not(early), index + 1 < NI))
        def _():
            fetch_ff(index + 1)

        return 0

    lax.fori_loop(0, NI, feed, 0)

    def close(r, _):
        rows = pl.ds(pl.multiple_of(r * STEP, STEP), STEP)
        y = (acc[rows, :] + down_bias).astype(BF16)
        for j in range(T):
            yb[j, rows, :] = y[:, j * W : (j + 1) * W]
        return 0

    lax.fori_loop(0, RP // STEP, close, 0)

    @pl.when(lower)
    def _():
        stream_copy.start()

    for slot in range(1, T):
        output_copy(slot).start()
    own_out = pltpu.make_async_copy(yb.at[tensor], result.at[tensor], lsem.at[0])
    own_out.start()
    own_out.wait()
    keep_x.wait()
    keep_p.wait()
    for keep in keeps:
        keep.wait()
    for index in (NI - 2, NI - 1):
        keep_a(index, index % 2).wait()
    for slot in range(1, T):
        output_copy(slot).wait()
        vector_copy(slot).wait_send()
        input_copy(slot).wait_send()
        for index in range(dm.NCH):
            weight_copy(slot, index).wait_send()

    @pl.when(lower)
    def _():
        stream_copy.wait_send()


def partner_dynamic(dm, place, slot):
    bit = 1
    while bit < dm.T:
        take = lax.rem(lax.div(slot, bit), 2)
        place = place + take * (bit - 2 * bit * lax.rem(lax.div(place, bit), 2))
        bit *= 2
    return place


def forward_call(dm, xin, vectors, wqkv, wout, wup, wdown):
    T, W, D, RP, RL, C, NI, FL = dm.T, dm.W, dm.D, dm.RP, dm.RL, dm.C, dm.NI, dm.FL
    sds = jax.ShapeDtypeStruct
    outs = (
        sds((T, 3, D, W), BF16), sds((T, W, D), BF16), sds((T, D, FL), BF16), sds((T, FL, D), BF16),
        sds((T, RP, W), BF16), sds((T, RP, W), BF16),
        sds((T, RL, W), BF16), sds((T, RL, W), BF16), sds((T, RL, W), BF16), sds((T, RL, W), BF16),
        sds((RP, D), F32), sds((NI, RP, C), F32), sds((T, VECTOR_ROWS, W), F32), sds((T, RP, W), BF16),
    )
    dma = pltpu.SemaphoreType.DMA
    scratch = [
        pltpu.VMEM((T, RP, W), BF16), pltpu.VMEM((RP, D), BF16), pltpu.VMEM((2, 3, D, W), BF16),
        pltpu.VMEM((D, D), BF16), pltpu.VMEM((2, D, C), BF16), pltpu.VMEM((2, C, D), BF16),
        pltpu.VMEM((2, RP, C), F32), pltpu.VMEM((RP, C), BF16), pltpu.VMEM((RP, D), F32),
        pltpu.VMEM((RP, D), BF16), pltpu.VMEM((T, RP, W), BF16), pltpu.VMEM((NI, 1, C), F32),
        pltpu.VMEM((T, VECTOR_ROWS, W), F32),
        pltpu.VMEM((T, RL, W), BF16), pltpu.VMEM((T, RL, W), BF16), pltpu.VMEM((T, RL, W), BF16), pltpu.VMEM((T, RL, W), BF16),
        dma((T, dm.NCH)), dma((T, dm.NCH)), dma((T,)), dma((T,)), dma((T,)), dma((T,)), dma((T,)), dma((T,)),
        dma((2,)), dma((8,)), dma((2 + T,)), dma((6,)),
    ]
    return pl.pallas_call(
        functools.partial(forward_kernel, dm),
        out_shape=outs,
        in_specs=[ANY] * 6,
        out_specs=[ANY] * len(outs),
        scratch_shapes=scratch,
        name="layer_forward",
        compiler_params=pltpu.CompilerParams(
            collective_id=0, has_side_effects=True, vmem_limit_bytes=VMEM_BYTES
        ),
    )(xin, vectors, wqkv, wout, wup, wdown)


def packed_vectors(dm, ln1_gain, ln1_bias, qv_bias, out_bias, ln2_gain, ln2_bias, fc1_bias, fc2_bias):
    rows = [ln1_gain, ln1_bias, qv_bias[0], out_bias, ln2_gain, ln2_bias, fc2_bias, fc1_bias]
    flat = jnp.concatenate([row.reshape(-1, dm.W) for row in rows], axis=0)
    return jnp.pad(flat, ((0, VECTOR_ROWS - flat.shape[0]), (0, 0)))


def padded_rows(dm, array):
    return jnp.pad(array, ((0, 0), (0, dm.RP - dm.tok), (0, 0)))


def dot_rows(left, right):
    return lax.dot_general(left, right, (((0,), (0,)), ((), ())), preferred_element_type=F32)


def fold(rows):
    total = rows[0:8, :]
    for first in range(8, rows.shape[0], 8):
        total = total + rows[first : first + 8, :]
    return total


def norm_rows_back(grad, hat, inv, gain, width):
    scaled = grad * gain
    mean = jnp.sum(scaled, axis=1, keepdims=True) * (1.0 / width)
    along = jnp.sum(scaled * hat, axis=1, keepdims=True) * (1.0 / width)
    return inv * (scaled - mean - hat * along)


def backward_kernel(
    dm,
    xc, xkeep, qkeep, kkeep, vkeep, okeep, hkeep, akeep, spkeep,
    wqkv, wout, wup, wdown, gqkv, gout, gup, gdown,
    dqkv, dout, dup, ddown, result, flat_sums, head_sums, up_sums,
    arr, dyb, acc, dh, hh, dhb, gs, das, n1t, n2t, nb, q, k, v, o, do, dq, dk, dv, xx,
    w1b, w2b, ab, dgb, wob, wq, s1, s2, yb, spb, fs, hs, us, dva, dka,
    ssem, osend, orecv, lsem, lw, lq, lg,
):
    section, tensor = lax.axis_index("section"), lax.axis_index("tensor")
    T, W, D, RP, RL, C, NI = dm.T, dm.W, dm.D, dm.RP, dm.RL, dm.C, dm.NI
    lower, upper = section == 0, section == 1
    own = (wqkv, wout, wup, wdown)
    real = pl.ds(0, RP)

    def source_of(slot, index):
        if slot == 0:
            return chunk_refs(dm, index, *own)
        return chunk_refs(dm, index, gqkv.at[slot], gout.at[slot], gup.at[slot], gdown.at[slot])

    stream_copy = pltpu.make_async_remote_copy(
        src_ref=arr,
        dst_ref=arr,
        send_sem=ssem.at[0],
        recv_sem=ssem.at[1],
        device_id={"section": 1 - section},
    )

    def output_copy(slot):
        return pltpu.make_async_remote_copy(
            src_ref=yb.at[partner(tensor, slot)],
            dst_ref=result.at[tensor],
            send_sem=osend.at[slot],
            recv_sem=orecv.at[slot],
            device_id={"tensor": partner(tensor, slot)},
        )

    def load_ff(index, parity):
        slot, c = dm.order[index]
        return [
            pltpu.make_async_copy(source_of(slot, 2 + 2 * c), w1b.at[parity], lw.at[parity]),
            pltpu.make_async_copy(source_of(slot, 3 + 2 * c), w2b.at[parity], lw.at[2 + parity]),
            pltpu.make_async_copy(akeep.at[index], ab.at[parity], lw.at[4 + parity]),
        ]

    def fetch_ff(which):
        for index in range(NI):

            @pl.when(which == index)
            def _():
                for load in load_ff(index, index % 2):
                    load.start()

    fetch_ff(0)
    loads = [
        pltpu.make_async_copy(source, target, lsem.at[number])
        for number, (source, target) in enumerate(
            ((spkeep, spb), (hkeep, hh), (qkeep, q), (kkeep, k), (vkeep, v), (okeep, o), (xkeep, xx))
        )
    ]
    for load in loads:
        load.start()
    out_loads = [
        pltpu.make_async_copy(source_of(slot, 1), wob.at[pl.ds(slot * W, W)], lq.at[2 + slot])
        for slot in range(T)
    ]
    for load in out_loads:
        load.start()

    meet(dm, section, tensor)

    @pl.when(upper)
    def _():
        load = pltpu.make_async_copy(xc, arr, lsem.at[7])
        load.start()
        load.wait()

    tail_rows = pl.ds(RP, RL - RP)
    blank = jnp.zeros((RL - RP, D), BF16)
    dyb[tail_rows, :] = blank
    dhb[tail_rows, :] = blank
    nb[tail_rows, :] = blank
    for index in range(NI):
        gs[index, tail_rows, :] = blank[:, :C]
        das[index, tail_rows, :] = blank[:, :C]
    for slot in range(T):
        do[slot, tail_rows, :] = blank[:, :W]
    acc[...] = jnp.zeros_like(acc)
    fs[...] = jnp.zeros_like(fs)
    hs[...] = jnp.zeros_like(hs)

    @pl.when(lower)
    def _():
        stream_copy.wait_recv()

    def spread(r, _):
        rows = pl.ds(pl.multiple_of(r * STEP, STEP), STEP)
        incoming = block_rows(dm, arr, rows)
        if T > dm.micro:
            incoming = jnp.where(tensor < dm.micro, incoming, jnp.zeros_like(incoming))
        dyb[rows, :] = incoming
        return 0

    lax.fori_loop(0, RP // STEP, spread, 0)

    def feed_back(index, _):
        parity = lax.rem(index, 2)
        for load in load_ff(0, parity):
            load.wait()

        @pl.when(index + 1 < NI)
        def _():
            fetch_ff(index + 1)

        dgb[...] = dot_last(dyb[real, :], w2b[parity])

        def bend(r, total):
            rows = pl.ds(pl.multiple_of(r * STEP, STEP), STEP)
            a = ab[parity, rows, :]
            cdf = 0.5 * (1.0 + lax.erf(a * ROOT_HALF))
            gs[index, rows, :] = (a * cdf).astype(BF16)
            da = dgb[rows, :] * (cdf + a * jnp.exp(-0.5 * a * a) * GAUSS_FACTOR)
            das[index, rows, :] = da.astype(BF16)
            return total + fold(da)

        total = lax.fori_loop(0, RP // STEP, bend, jnp.zeros((8, C), F32))
        us[index] = jnp.sum(total, axis=0, keepdims=True)
        for n in range(D // 256):
            cols = pl.ds(n * 256, 256)
            acc[:, cols] += dot_last(das[index, real, :], w1b[parity, cols, :])
        return 0

    lax.fori_loop(0, NI, feed_back, 0)

    for load in loads:
        load.wait()
    for load in out_loads:
        load.wait()
    gain2, bias2 = full_vector(dm, spb, LN2_GAIN), full_vector(dm, spb, LN2_BIAS)

    def second_norm(r, _):
        rows = pl.ds(pl.multiple_of(r * STEP, STEP), STEP)
        hat, inv = norm_rows(hh[rows, :], D)
        grad = acc[rows, :]
        dy = dyb[rows, :].astype(F32)
        fs[0] += fold(grad * hat)
        fs[1] += fold(grad)
        whole = dy + norm_rows_back(grad, hat, inv, gain2, D)
        dh[rows, :] = whole
        dhb[rows, :] = whole.astype(BF16)
        fs[2] += fold(whole)
        fs[3] += fold(dy)
        nb[rows, :] = (hat * gain2 + bias2).astype(BF16)
        return 0

    lax.fori_loop(0, RP // STEP, second_norm, 0)

    def turn(target):
        for n in range(D // 256):
            cols = pl.ds(n * 256, 256)
            target[cols, :] = nb[:, cols].T

    turn(n2t)

    def put_ff(index, parity):
        slot, c = dm.order[index]
        return [
            pltpu.make_async_copy(s1.at[parity], dup.at[slot, :, pl.ds(c * C, C)], lg.at[parity]),
            pltpu.make_async_copy(s2.at[parity], ddown.at[slot, pl.ds(c * C, C), :], lg.at[2 + parity]),
        ]

    def feed_weights():
        def one(index, _):
            parity = lax.rem(index, 2)

            @pl.when(index >= 2)
            def _():
                for put in put_ff(0, parity):
                    put.wait()

            for n in range(D // 256):
                cols = pl.ds(n * 256, 256)
                s1[parity, cols, :] = dot_plain(n2t[cols, :], das[index]).astype(BF16)
            for n in range(C // 256):
                cols = pl.ds(n * 256, 256)
                s2[parity, cols, :] = dot_rows(gs[index, :, cols], dyb[...]).astype(BF16)
            for j in range(NI):

                @pl.when(index == j)
                def _():
                    for put in put_ff(j, j % 2):
                        put.start()

            return 0

        lax.fori_loop(0, NI, one, 0)
        for parity in range(2):
            for put in put_ff(0, parity):
                put.wait()

    @pl.when(lower)
    def _():
        feed_weights()

    for slot in range(T):
        do[slot, real, :] = dot_last(dhb[real, :], wob[pl.ds(slot * W, W), :]).astype(BF16)

    mask_full = half_masks(RL)
    row = lax.broadcasted_iota(jnp.int32, (RL, 1), 0)
    key_bias = jnp.where(row < dm.tok, 0.0, MASKED).astype(F32)
    scale = HEAD_DIM**-0.5
    blocks = [(first, min(256, RL - first)) for first in range(0, RL, 256)]

    def heads(slot, _):
        for pair in range(W // 128):
            lanes = slice(pair * 128, pair * 128 + 128)
            keys, values = k[slot, :, lanes], v[slot, :, lanes]
            for number, (first, size) in enumerate(blocks):
                rows = slice(first, first + size)
                query, grad = q[slot, rows, lanes], do[slot, rows, lanes]
                dq_block = jnp.zeros((size, 128), F32)
                dk_block, dv_block = jnp.zeros((RL, 128), F32), jnp.zeros((RL, 128), F32)
                for half in range(2):
                    mask = mask_full[half][:size]
                    query_h = jnp.where(mask, query, jnp.zeros_like(query))
                    grad_h = jnp.where(mask, grad, jnp.zeros_like(grad))
                    keys_h = jnp.where(mask_full[half], keys, jnp.zeros_like(keys))
                    s = dot_last(keys, query_h * jnp.asarray(scale, BF16)) + key_bias
                    e = jnp.exp(s - jnp.max(s, axis=0, keepdims=True))
                    p = e * (1.0 / jnp.sum(e, axis=0, keepdims=True))
                    dp = dot_last(values, grad_h)
                    delta = jnp.sum(p * dp, axis=0, keepdims=True)
                    ds = (p * (dp - delta) * scale).astype(BF16)
                    dv_block = dv_block + dot_plain(p.astype(BF16), grad_h)
                    dk_block = dk_block + dot_plain(ds, query_h)
                    dq_block = dq_block + dot_rows(ds, keys_h)
                dq[slot, rows, lanes] = dq_block.astype(BF16)
                hs[slot, 0, :, lanes] += fold(dq_block)
                if number == 0:
                    dka[...] = dk_block
                    dva[...] = dv_block
                else:
                    dka[...] += dk_block
                    dva[...] += dv_block
            dk[slot, :, lanes] = dka[...].astype(BF16)
            total = dva[...]
            dv[slot, :, lanes] = total.astype(BF16)
            hs[slot, 1, :, lanes] += fold(total)
        return 0

    lax.fori_loop(0, T, heads, 0)

    def load_qkv(slot, parity):
        return pltpu.make_async_copy(source_of(slot, 0), wq.at[parity], lq.at[parity])

    load_qkv(0, 0).start()
    for slot in range(T):
        load_qkv(slot, slot % 2).wait()
        if slot + 1 < T:
            load_qkv(slot + 1, (slot + 1) % 2).start()
        for n in range(D // 256):
            cols = pl.ds(n * 256, 256)
            part = dot_last(dq[slot, real, :], wq[slot % 2, 0, cols, :])
            part = part + dot_last(dk[slot, real, :], wq[slot % 2, 1, cols, :])
            part = part + dot_last(dv[slot, real, :], wq[slot % 2, 2, cols, :])
            if slot == 0:
                acc[:, cols] = part
            else:
                acc[:, cols] += part

    gain1, bias1 = full_vector(dm, spb, LN1_GAIN), full_vector(dm, spb, LN1_BIAS)

    def first_norm(r, _):
        rows = pl.ds(pl.multiple_of(r * STEP, STEP), STEP)
        hat, inv = norm_rows(block_rows(dm, xx, rows).astype(F32), D)
        grad = acc[rows, :]
        fs[4] += fold(grad * hat)
        fs[5] += fold(grad)
        whole = dh[rows, :] + norm_rows_back(grad, hat, inv, gain1, D)
        nb[rows, :] = (hat * gain1 + bias1).astype(BF16)
        low = whole.astype(BF16)
        for j in range(T):
            yb[j, rows, :] = whole[:, j * W : (j + 1) * W]
            xx[j, rows, :] = low[:, j * W : (j + 1) * W]
        return 0

    lax.fori_loop(0, RP // STEP, first_norm, 0)

    down_copy = pltpu.make_async_remote_copy(
        src_ref=xx,
        dst_ref=arr,
        send_sem=ssem.at[0],
        recv_sem=ssem.at[1],
        device_id={"section": 1 - section},
    )

    @pl.when(upper)
    def _():
        down_copy.start()

    for slot in range(1, T):
        output_copy(slot).start()
    own_out = pltpu.make_async_copy(yb.at[tensor], result.at[tensor], lsem.at[0])
    own_out.start()
    turn(n1t)

    def put_qkv(slot, parity):
        return [
            pltpu.make_async_copy(s1.at[parity, :, pl.ds(0, W)], dqkv.at[slot, 0], lg.at[4 + parity]),
            pltpu.make_async_copy(s1.at[parity, :, pl.ds(C // 2, W)], dqkv.at[slot, 1], lg.at[6 + parity]),
        ]

    for slot in range(T):
        number = 0
        s2[slot % 2, pl.ds(0, W), :] = dot_rows(o[slot], dhb[...]).astype(BF16)
        put_out = pltpu.make_async_copy(s2.at[slot % 2, pl.ds(0, W), :], dout.at[slot], lg.at[4])
        put_out.start()
        for source in (dq, dk, dv):
            for n in range(D // 256):
                cols = pl.ds(n * 256, 256)
                s1[number % 2, cols, pl.ds(0, W)] = dot_plain(n1t[cols, :], source[slot]).astype(BF16)
            put = pltpu.make_async_copy(s1.at[number % 2, :, pl.ds(0, W)], dqkv.at[slot, number], lg.at[number % 2])
            put.start()
            put.wait()
            number += 1
        put_out.wait()

    @pl.when(upper)
    def _():
        feed_weights()

    keeps = []
    for number, (source, target) in enumerate(((fs, flat_sums), (hs, head_sums), (us, up_sums))):
        keeps.append(pltpu.make_async_copy(source, target, lsem.at[1 + number]))
        keeps[-1].start()
    for keep in keeps:
        keep.wait()
    own_out.wait()
    for slot in range(1, T):
        output_copy(slot).wait()

    @pl.when(upper)
    def _():
        down_copy.wait_send()


def backward_call(dm, kept, own):
    T, W, D, RP, RL, C, NI, FL = dm.T, dm.W, dm.D, dm.RP, dm.RL, dm.C, dm.NI, dm.FL
    sds = jax.ShapeDtypeStruct
    gathered, rest = kept[:4], kept[4:13]
    outs = (
        sds((T, 3, D, W), BF16), sds((T, W, D), BF16), sds((T, D, FL), BF16), sds((T, FL, D), BF16),
        sds((T, RP, W), F32), sds((6, 8, D), F32), sds((T, 2, 8, W), F32), sds((NI, 1, C), F32),
    )
    dma = pltpu.SemaphoreType.DMA
    heads = pltpu.VMEM((T, RL, W), BF16)
    scratch = [
        pltpu.VMEM((T, RP, W), BF16), pltpu.VMEM((RL, D), BF16), pltpu.VMEM((RP, D), F32), pltpu.VMEM((RP, D), F32),
        pltpu.VMEM((RP, D), F32), pltpu.VMEM((RL, D), BF16), pltpu.VMEM((NI, RL, C), BF16), pltpu.VMEM((NI, RL, C), BF16),
        pltpu.VMEM((D, RL), BF16), pltpu.VMEM((D, RL), BF16), pltpu.VMEM((RL, D), BF16),
        heads, heads, heads, heads, heads, heads, heads, heads, pltpu.VMEM((T, RP, W), BF16),
        pltpu.VMEM((2, D, C), BF16), pltpu.VMEM((2, C, D), BF16), pltpu.VMEM((2, RP, C), F32), pltpu.VMEM((RP, C), F32),
        pltpu.VMEM((D, D), BF16), pltpu.VMEM((2, 3, D, W), BF16), pltpu.VMEM((2, D, C), BF16), pltpu.VMEM((2, C, D), BF16),
        pltpu.VMEM((T, RP, W), F32), pltpu.VMEM((T, VECTOR_ROWS, W), F32),
        pltpu.VMEM((6, 8, D), F32), pltpu.VMEM((T, 2, 8, W), F32), pltpu.VMEM((NI, 1, C), F32),
        pltpu.VMEM((RL, 128), F32), pltpu.VMEM((RL, 128), F32),
        dma((2,)), dma((T,)), dma((T,)), dma((8,)), dma((6,)), dma((2 + T,)), dma((8,)),
    ]
    return pl.pallas_call(
        functools.partial(backward_kernel, dm),
        out_shape=outs,
        in_specs=[ANY] * 17,
        out_specs=[ANY] * len(outs),
        scratch_shapes=scratch,
        name="layer_backward",
        compiler_params=pltpu.CompilerParams(
            collective_id=1, has_side_effects=True, vmem_limit_bytes=VMEM_BYTES
        ),
    )(*rest, *own, *gathered)


def piece_list(dm):
    down, up, out, qkv = [], [], [], []
    for first in range(0, dm.FL, 128):
        down.append((3, first, 128))
    for first in range(0, dm.D, 128):
        up.append((2, first, 128))
    for first in range(0, dm.W, 128):
        out.append((1, first, 128))
    for first in range(0, 3 * dm.D, 512):
        qkv.append((0, first, 512))
    return down + up + out + qkv


def reduce_kernel(
    dm,
    dqkv, dout, dup, ddown, flat_sums, head_sums, up_sums,
    rqkv, rout, rup, rdown, rsmall,
    *scratch,
):
    section, dp, tensor = lax.axis_index("section"), lax.axis_index("dp"), lax.axis_index("tensor")
    T, W, D, FL, NI, C = dm.T, dm.W, dm.D, dm.FL, dm.NI, dm.C
    line = lax.axis_size("dp")
    stages = dm.stages
    scratch = list(scratch)
    mine = [scratch.pop(0) for _ in range(4)]
    land = [[scratch.pop(0) for _ in range(4)] for _ in range(stages)]
    inward = [scratch.pop(0) for _ in range(4)]
    outward = [scratch.pop(0) for _ in range(4)]
    parts, gathered, small_in, small_out, small_own = [scratch.pop(0) for _ in range(5)]
    lsend, lrecv, isend, irecv, osend, orecv, msem, wsem, gsend, grecv, vsem = scratch
    partial = (dqkv, dout, dup, ddown)
    reduced = (rqkv, rout, rup, rdown)
    pieces = piece_list(dm)
    NP = len(pieces)

    half = line // 2
    left = dp < half
    outer = jnp.logical_or(dp == 0, dp == line - 1)
    middle = jnp.logical_or(dp == half - 1, dp == half)
    toward = jnp.where(left, 1, -1)
    inner_dp = dp + toward
    outer_dp = lax.rem(dp - toward + line, line)

    barrier = pltpu.get_barrier_semaphore()
    for slot in range(1, T):
        pl.semaphore_signal(barrier, inc=1, device_id={"tensor": partner(tensor, slot)})
    pl.semaphore_signal(barrier, inc=1, device_id={"dp": lax.rem(dp + 1, line)})
    pl.semaphore_signal(barrier, inc=1, device_id={"dp": lax.rem(dp + line - 1, line)})
    pl.semaphore_wait(barrier, T + 1)

    def at(ref, piece, *lead):
        kind, first, rows = pieces[piece]
        return ref[kind].at[(*lead, pl.ds(first, rows), slice(None))]

    def lowest(slot):
        stage = 0
        while slot % 2 == 0:
            slot //= 2
            stage += 1
        return stage

    def fold_copy(piece, slot):
        stage = lowest(slot)
        bit = 1 << stage
        source = at(partial, piece, slot) if stage == 0 else at(land[stage - 1], piece, slot >> stage)
        return pltpu.make_async_remote_copy(
            src_ref=source,
            dst_ref=at(land[stage], piece, (slot - bit) >> (stage + 1)),
            send_sem=lsend.at[piece, slot],
            recv_sem=lrecv.at[piece, slot],
            device_id={"tensor": flip(tensor, bit)},
        )

    def inward_copy(piece, source):
        return pltpu.make_async_remote_copy(
            src_ref=source,
            dst_ref=at(inward, piece),
            send_sem=isend.at[piece],
            recv_sem=irecv.at[piece],
            device_id={"dp": inner_dp},
        )

    def meet_copy(piece, source):
        return pltpu.make_async_remote_copy(
            src_ref=source,
            dst_ref=at(outward, piece),
            send_sem=isend.at[piece],
            recv_sem=orecv.at[piece],
            device_id={"dp": inner_dp},
        )

    def outward_copy(piece):
        return pltpu.make_async_remote_copy(
            src_ref=at(outward, piece),
            dst_ref=at(outward, piece),
            send_sem=osend.at[piece],
            recv_sem=orecv.at[piece],
            device_id={"dp": outer_dp},
        )

    def load(piece, slot):
        return pltpu.make_async_copy(at(partial, piece, slot), at(mine, piece, slot // 2), msem.at[piece, slot // 2])

    def store(piece):
        return pltpu.make_async_copy(at(outward, piece), at(reduced, piece), wsem.at[piece])

    for j in range(T):
        for row in range(6):
            parts[j, row : row + 1, :] = jnp.sum(flat_sums[row, :, j * W : (j + 1) * W], axis=0, keepdims=True)
        parts[j, 8 + FL // W : VECTOR_ROWS, :] = jnp.zeros((VECTOR_ROWS - 8 - FL // W, W), F32)
    per = C // W
    for slot in range(T):
        place = partner(tensor, slot)
        for row in range(2):
            parts[place, 6 + row : 7 + row, :] = jnp.sum(head_sums[slot, row], axis=0, keepdims=True)
        for index, (owner, c) in enumerate(dm.order):
            if owner == slot:
                for i in range(per):
                    row = 8 + c * per + i
                    parts[place, row : row + 1, :] = up_sums[index, :, i * W : (i + 1) * W]

    def small_copy(slot):
        return pltpu.make_async_remote_copy(
            src_ref=parts.at[partner(tensor, slot)],
            dst_ref=gathered.at[slot],
            send_sem=gsend.at[slot],
            recv_sem=grecv.at[slot],
            device_id={"tensor": partner(tensor, slot)},
        )

    def small_line(number, source, target, place):
        return pltpu.make_async_remote_copy(
            src_ref=source,
            dst_ref=target,
            send_sem=vsem.at[number],
            recv_sem=vsem.at[number + 1],
            device_id={"dp": place},
        )

    for piece in range(NP):
        for slot in range(1, T, 2):
            fold_copy(piece, slot).start()
        for slot in range(0, T, 2):
            load(piece, slot).start()
    for slot in range(1, T):
        small_copy(slot).start()

    def rows_of(piece):
        kind, first, rows = pieces[piece]
        width = (W, D, FL, D)[kind]
        step = max(16, min(rows, 32768 // width))
        return kind, first, rows // step, step

    def add_into(piece, target, sources):
        kind, first, count, step = rows_of(piece)

        def one(r, _):
            rows = pl.ds(pl.multiple_of(first + r * step, 16), step)
            total = target[0][kind][(*target[1], rows, slice(None))].astype(F32)
            for ref, lead in sources:
                total = total + ref[kind][(*lead, rows, slice(None))].astype(F32)
            target[0][kind][(*target[1], rows, slice(None))] = total.astype(BF16)
            return 0

        lax.fori_loop(0, count, one, 0)

    def pass_on(piece, stage):
        bit = 1 << stage
        for slot in range(bit, T, 2 * bit):
            for before in range(stage):
                fold_copy(piece, slot + (1 << before)).wait_recv()
            load(piece, slot).wait()
            add_into(
                piece,
                (land[stage - 1], (slot >> stage,)),
                [(mine, (slot // 2,))] + [(land[b], (slot >> (b + 1),)) for b in range(stage - 1)],
            )
            fold_copy(piece, slot).start()

    def own_sum(piece):
        for stage in range(stages):
            fold_copy(piece, 1 << stage).wait_recv()
        load(piece, 0).wait()
        add_into(piece, (land[stages - 1], (0,)), [(mine, (0,))] + [(land[b], (0,)) for b in range(stages - 1)])

        @pl.when(outer)
        def _():
            inward_copy(piece, at(land[stages - 1], piece, 0)).start()

    def gather_in(piece):
        @pl.when(jnp.logical_not(outer))
        def _():
            inward_copy(piece, at(inward, piece)).wait_recv()
            add_into(piece, (inward, ()), [(land[stages - 1], (0,))])

            @pl.when(middle)
            def _():
                meet_copy(piece, at(inward, piece)).start()

            @pl.when(jnp.logical_not(middle))
            def _():
                inward_copy(piece, at(inward, piece)).start()

    def spread_middle(piece):
        @pl.when(middle)
        def _():
            meet_copy(piece, at(inward, piece)).wait_recv()
            add_into(piece, (outward, ()), [(inward, ())])
            outward_copy(piece).start()
            store(piece).start()

    def spread_out(piece):
        @pl.when(jnp.logical_not(middle))
        def _():
            outward_copy(piece).wait_recv()

            @pl.when(jnp.logical_not(outer))
            def _():
                outward_copy(piece).start()

            store(piece).start()

    def small_chain():
        for slot in range(1, T):
            small_copy(slot).wait_recv()
        total = parts[tensor]
        for slot in range(1, T):
            total = total + gathered[slot]
        small_own[...] = total

        @pl.when(outer)
        def _():
            small_line(0, small_own, small_in, inner_dp).start()

        @pl.when(jnp.logical_not(outer))
        def _():
            small_line(0, small_own, small_in, inner_dp).wait_recv()
            small_in[...] = small_in[...] + small_own[...]

            @pl.when(jnp.logical_not(middle))
            def _():
                small_line(0, small_in, small_in, inner_dp).start()

        @pl.when(middle)
        def _():
            meeting = small_line(2, small_in, small_out, inner_dp)
            meeting.start()
            meeting.wait_recv()
            small_out[...] = small_out[...] + small_in[...]
            small_line(4, small_out, small_out, outer_dp).start()

        @pl.when(jnp.logical_not(middle))
        def _():
            small_line(4, small_out, small_out, outer_dp).wait_recv()

            @pl.when(jnp.logical_not(outer))
            def _():
                small_line(4, small_out, small_out, outer_dp).start()

        rsmall[...] = small_out[...]

    def run(action, piece, *rest):
        if 0 <= piece < NP:
            action(piece, *rest)

    ahead = 1
    depth = stages - 1
    for stage in range(1, stages):
        for piece in range(ahead + (depth - stage)):
            run(pass_on, piece, stage)
    for step in range(NP + 4):
        for stage in range(1, stages):
            run(pass_on, step + ahead + (depth - stage), stage)
        run(own_sum, step)
        run(gather_in, step - 1)
        run(spread_middle, step - 2)
        run(spread_out, step - 3)
        if step == NP:
            small_chain()

    for piece in range(NP):
        store(piece).wait()
        for slot in range(1, T):
            fold_copy(piece, slot).wait_send()

        @pl.when(jnp.logical_not(middle))
        def _():
            inward_copy(piece, at(inward, piece)).wait_send()

        @pl.when(middle)
        def _():
            meet_copy(piece, at(inward, piece)).wait_send()

        @pl.when(jnp.logical_not(outer))
        def _():
            outward_copy(piece).wait_send()

    for slot in range(1, T):
        small_copy(slot).wait_send()

    @pl.when(jnp.logical_not(middle))
    def _():
        small_line(0, small_in, small_in, inner_dp).wait_send()

    @pl.when(middle)
    def _():
        small_line(2, small_in, small_out, inner_dp).wait_send()

    @pl.when(jnp.logical_not(outer))
    def _():
        small_line(4, small_out, small_out, outer_dp).wait_send()


def reduce_call(dm, partial, sums):
    T, W, D, FL = dm.T, dm.W, dm.D, dm.FL
    dm.stages = T.bit_length() - 1
    sds = jax.ShapeDtypeStruct
    dims = ((3 * D, W), (W, D), (D, FL), (FL, D))
    partial = (partial[0].reshape(T, 3 * D, W),) + tuple(partial[1:])
    outs = tuple(sds(d, BF16) for d in dims) + (sds((VECTOR_ROWS, W), F32),)
    NP = len(piece_list(dm))
    dma = pltpu.SemaphoreType.DMA
    scratch = [pltpu.VMEM((T // 2, *d), BF16) for d in dims]
    for stage in range(dm.stages):
        scratch += [pltpu.VMEM((T >> (stage + 1), *d), BF16) for d in dims]
    scratch += [pltpu.VMEM(d, BF16) for d in dims] * 2
    scratch += [pltpu.VMEM((T, VECTOR_ROWS, W), F32)] * 2 + [pltpu.VMEM((VECTOR_ROWS, W), F32)] * 3
    scratch += [
        dma((NP, T)), dma((NP, T)), dma((NP,)), dma((NP,)), dma((NP,)), dma((NP,)),
        dma((NP, T // 2)), dma((NP,)), dma((T,)), dma((T,)), dma((6,)),
    ]
    whole = pl.BlockSpec(memory_space=pltpu.VMEM)
    return pl.pallas_call(
        functools.partial(reduce_kernel, dm),
        out_shape=outs,
        in_specs=[ANY] * 4 + [whole] * 3,
        out_specs=[ANY] * 4 + [whole],
        scratch_shapes=scratch,
        name="grad_reduce",
        compiler_params=pltpu.CompilerParams(
            collective_id=2, has_side_effects=True, vmem_limit_bytes=VMEM_BYTES
        ),
    )(*partial, *sums)


def shards(
    images, cotangent, ln1_gain, ln1_bias, qkv_weight, qv_bias, out_weight, out_bias,
    ln2_gain, ln2_bias, fc1_weight, fc1_bias, fc2_weight, fc2_bias,
):
    dm = sizes_of(images, fc1_weight, lax.axis_size("tensor"))
    T, W, D = dm.T, dm.W, dm.D
    section, tensor = lax.axis_index("section"), lax.axis_index("tensor")
    xin = padded_rows(dm, jnp.where(section == 0, images[:, 0], cotangent[:, 0]))
    vectors = packed_vectors(
        dm, ln1_gain[0], ln1_bias[0], qv_bias, out_bias[0], ln2_gain[0], ln2_bias[0], fc1_bias[0], fc2_bias[0]
    )
    own = (qkv_weight[0], out_weight[0], fc1_weight[0], fc2_weight[0])
    kept = forward_call(dm, xin, vectors, *own)
    section_out = kept[13][: dm.micro, : dm.tok][None, :, None]
    dqkv, dout, dup, ddown, result, flat_sums, head_sums, up_sums = backward_call(dm, kept, own)
    input_grads = result[: dm.micro, : dm.tok][None, :, None]

    rqkv, rout, rup, rdown, small = reduce_call(dm, (dqkv, dout, dup, ddown), (flat_sums, head_sums, up_sums))
    g2, b2, ob, db, g1, b1 = (small[i][None] for i in range(6))
    qv = small[6:8][None]
    ub = small[8 : 8 + dm.FL // W].reshape(1, -1)
    wide = lambda array: array.astype(F32)[None]
    return (
        section_out, input_grads, g1, b1, wide(rqkv.reshape(3, D, W)), qv, wide(rout), ob, g2, b2,
        wide(rup), ub, wide(rdown), db,
    )


def solution(mesh):
    vector = P("section", "tensor")
    rows = P(None, "dp", None, "tensor")
    placed_rows = P("section", None, "dp", None, "tensor")
    qkv, qv = P("section", None, None, "tensor"), P("section", None, "tensor")
    by_row, by_column = P("section", "tensor", None), P("section", None, "tensor")
    return jax.shard_map(
        shards,
        mesh=mesh,
        in_specs=(rows, rows, vector, vector, qkv, qv, by_row, vector, vector, vector, by_column, vector, by_row, vector),
        out_specs=(
            placed_rows, placed_rows, vector, vector, qkv, qv, by_row, vector, vector, vector,
            by_column, vector, by_row, vector,
        ),
        check_vma=False,
    )
```

```python
import functools
import types

import jax
import jax.numpy as jnp
from jax import lax
from jax.experimental import pallas as pl
from jax.experimental.pallas import tpu as pltpu
from jax.sharding import PartitionSpec as P

BF16, F32 = jnp.bfloat16, jnp.float32
HEAD_DIM = 64
EPSILON = 1e-06
ROOT_HALF = 0.7071067811865476
GAUSS_FACTOR = 0.3989422804014327
MASKED = -1e30
STEP = 32
ANY = pl.BlockSpec(memory_space=pl.ANY)
VMEM_BYTES = 67043328

LN1_GAIN, LN1_BIAS, Q_BIAS, V_BIAS, OUT_BIAS, LN2_GAIN, LN2_BIAS, FC2_BIAS, FC1_BIAS = range(9)
VECTOR_ROWS = 16


def flip(place, bit):
    return place + bit - 2 * bit * lax.rem(lax.div(place, bit), 2)


def partner(place, slot):
    bit = 1
    while bit <= slot:
        if slot & bit:
            place = flip(place, bit)
        bit *= 2
    return place


def sizes_of(images, fc1_weight, tensor):
    micro, _, tok, width = images.shape
    dm = types.SimpleNamespace()
    dm.T, dm.W, dm.micro, dm.tok = tensor, width, micro, tok
    dm.D = width * tensor
    dm.FL = fc1_weight.shape[2]
    dm.RP = -(-tok // STEP) * STEP
    dm.RL = -(-tok // 128) * 128
    dm.KR = -(-tok // 16) * 16
    dm.HS = width // HEAD_DIM
    dm.C = min(512, dm.FL)
    dm.NC = dm.FL // dm.C
    dm.order = [
        (2 * p + half, c) for p in range(tensor // 2) for c in range(dm.NC) for half in range(2)
    ]
    dm.NI = len(dm.order)
    dm.NCH = 2 + 2 * dm.NC
    return dm


def full_vector(dm, vectors, row):
    return jnp.concatenate([vectors[j, row : row + 1, :] for j in range(dm.T)], axis=1)


def norm_rows(rows, width):
    mean = jnp.sum(rows, axis=1, keepdims=True) * (1.0 / width)
    var = jnp.sum(rows * rows, axis=1, keepdims=True) * (1.0 / width) - mean * mean
    inv = lax.rsqrt(var + EPSILON)
    return (rows - mean) * inv, inv


def block_rows(dm, ref, rows):
    return jnp.concatenate([ref[j, rows, :] for j in range(dm.T)], axis=1)


def dot_last(left, right):
    return lax.dot_general(left, right, (((1,), (1,)), ((), ())), preferred_element_type=F32)


def dot_plain(left, right):
    return lax.dot_general(left, right, (((1,), (0,)), ((), ())), preferred_element_type=F32)


def add_masked(dm, scores):
    cut = dm.tok // 8 * 8
    if cut == dm.KR:
        return scores
    row = lax.broadcasted_iota(jnp.int32, (dm.KR - cut, 1), 0) + cut
    bias = jnp.where(row < dm.tok, 0.0, MASKED).astype(F32)
    return jnp.concatenate([scores[:cut], scores[cut:] + bias], axis=0)


def half_masks(rows):
    lane = lax.broadcasted_iota(jnp.int32, (rows, 128), 1)
    return [lane < HEAD_DIM, lane >= HEAD_DIM]


def chunk_refs(dm, index, qkv, out, up, down):
    if index == 0:
        return qkv
    if index == 1:
        return out
    c = (index - 2) // 2
    if index % 2 == 0:
        return up.at[:, pl.ds(c * dm.C, dm.C)]
    return down.at[pl.ds(c * dm.C, dm.C), :]


def meet(dm, section, tensor):
    barrier = pltpu.get_barrier_semaphore()
    for slot in range(1, dm.T):
        pl.semaphore_signal(barrier, inc=1, device_id={"tensor": partner(tensor, slot)})
    pl.semaphore_signal(barrier, inc=1, device_id={"section": 1 - section})
    pl.semaphore_wait(barrier, dm.T)


def forward_kernel(
    dm,
    xin, spin, wqkv, wout, wup, wdown,
    gqkv, gout, gup, gdown, xc, xkeep, qkeep, kkeep, vkeep, okeep, lkeep, hkeep, akeep, spkeep, ykeep,
    xarr, n1, wq, wob, w1b, w2b, ab, gb, acc, n2, yb, b1r, spb, q, k, v, o, lse,
    wsend, wrecv, xsend, xrecv, psend, precv, ssem, lsem, lw, la,
):
    section, tensor = lax.axis_index("section"), lax.axis_index("tensor")
    T, W, D, RP, RL, C, NI = dm.T, dm.W, dm.D, dm.RP, dm.RL, dm.C, dm.NI
    lower, upper = section == 0, section == 1
    own = (wqkv, wout, wup, wdown)

    def slot_refs(slot):
        return (gqkv.at[slot], gout.at[slot], gup.at[slot], gdown.at[slot])

    def weight_copy(slot, index):
        relay = slot > 1 and slot % 2 == 1
        source = chunk_refs(dm, index, *(slot_refs(slot - 1) if relay else own))
        return pltpu.make_async_remote_copy(
            src_ref=source,
            dst_ref=chunk_refs(dm, index, *slot_refs(slot)),
            send_sem=wsend.at[slot, index],
            recv_sem=wrecv.at[slot, index],
            device_id={"tensor": flip(tensor, 1) if relay else partner(tensor, slot)},
        )

    def input_copy(slot):
        return pltpu.make_async_remote_copy(
            src_ref=xin.at[lax.rem(partner(tensor, slot), dm.micro)],
            dst_ref=xc.at[tensor],
            send_sem=xsend.at[slot],
            recv_sem=xrecv.at[slot],
            device_id={"tensor": partner(tensor, slot)},
        )

    def vector_copy(slot):
        return pltpu.make_async_remote_copy(
            src_ref=spin,
            dst_ref=spb.at[tensor],
            send_sem=psend.at[slot],
            recv_sem=precv.at[slot],
            device_id={"tensor": partner(tensor, slot)},
        )

    stream_copy = pltpu.make_async_remote_copy(
        src_ref=yb,
        dst_ref=xarr,
        send_sem=ssem.at[0],
        recv_sem=ssem.at[1],
        device_id={"section": 1 - section},
    )

    meet(dm, section, tensor)
    for slot in range(1, T):
        vector_copy(slot).start()
        input_copy(slot).start()
    own_vec = pltpu.make_async_copy(spin, spb.at[tensor], lsem.at[0])
    own_vec.start()
    own_in = pltpu.make_async_copy(xin.at[lax.rem(tensor, dm.micro)], xc.at[tensor], lsem.at[1])
    own_in.start()
    direct = [slot for slot in range(1, T) if slot == 1 or slot % 2 == 0]
    for index in range(dm.NCH):
        for slot in direct:
            weight_copy(slot, index).start()

    def relay(slot, index):
        weight_copy(slot, index).wait_recv()
        weight_copy(slot + 1, index).start()

    own_vec.wait()
    own_in.wait()
    for slot in range(1, T):
        vector_copy(slot).wait_recv()
        input_copy(slot).wait_recv()

    @pl.when(upper)
    def _():
        for index in range(dm.NCH):
            for slot in range(2, T, 2):
                relay(slot, index)
        stream_copy.wait_recv()

    @pl.when(lower)
    def _():
        load = pltpu.make_async_copy(xc, xarr, lsem.at[0])
        load.start()
        load.wait()

    def arrive(slot, index):
        if slot == 0:
            return
        if slot % 2 == 0:

            @pl.when(lower)
            def _():
                relay(slot, index)

        else:
            weight_copy(slot, index).wait_recv()

    def source_of(slot, index):
        return chunk_refs(dm, index, *(own if slot == 0 else slot_refs(slot)))

    keep_x = pltpu.make_async_copy(xarr, xkeep, lsem.at[1])
    keep_x.start()
    keep_p = pltpu.make_async_copy(spb, spkeep, lsem.at[2])
    keep_p.start()

    gain, bias = full_vector(dm, spb, LN1_GAIN), full_vector(dm, spb, LN1_BIAS)

    def first_norm(r, _):
        rows = pl.ds(pl.multiple_of(r * STEP, STEP), STEP)
        hat, _inv = norm_rows(block_rows(dm, xarr, rows).astype(F32), D)
        n1[rows, :] = (hat * gain + bias).astype(BF16)
        return 0

    lax.fori_loop(0, RP // STEP, first_norm, 0)

    for index, (slot, c) in enumerate(dm.order):
        shard = spb[partner(tensor, slot)]
        per = C // W
        first = FC1_BIAS + c * per
        b1r[index] = jnp.concatenate([shard[first + i : first + i + 1, :] for i in range(per)], axis=1)

    pad = jnp.zeros((RL - RP, W), BF16)
    for slot in range(T):
        for ref in (q, k, v):
            ref[slot, pl.ds(RP, RL - RP), :] = pad

    def load_qkv(slot, parity):
        return pltpu.make_async_copy(source_of(slot, 0), wq.at[parity], lw.at[parity])

    def fetch_qkv(which):
        for slot in range(T):

            @pl.when(which == slot)
            def _():
                arrive(slot, 0)
                load_qkv(slot, slot % 2).start()

    masks = half_masks(RL)

    fetch_qkv(0)

    def heads(slot, _):
        parity = lax.rem(slot, 2)
        pltpu.make_async_copy(gqkv.at[0], wq.at[parity], lw.at[parity]).wait()
        early = jnp.logical_or(upper, slot < 1)

        @pl.when(jnp.logical_and(early, slot + 1 < T))
        def _():
            fetch_qkv(slot + 1)

        shard = spb[partner_dynamic(dm, tensor, slot)]
        rows = pl.ds(0, RP)
        q[slot, rows, :] = (dot_plain(n1[...], wq[parity, 0]) + shard[Q_BIAS : Q_BIAS + 1]).astype(BF16)
        k[slot, rows, :] = dot_plain(n1[...], wq[parity, 1]).astype(BF16)
        v[slot, rows, :] = (dot_plain(n1[...], wq[parity, 2]) + shard[V_BIAS : V_BIAS + 1]).astype(BF16)

        for pair in range(W // 128):
            lanes = slice(pair * 128, pair * 128 + 128)

            keys, values = k[slot, pl.ds(0, dm.KR), lanes], v[slot, pl.ds(0, dm.KR), lanes]
            query = q[slot, :, lanes] * jnp.asarray(HEAD_DIM**-0.5, BF16)
            total = None
            for half in range(2):
                query_h = jnp.where(masks[half], query, jnp.zeros_like(query))
                values_h = jnp.where(masks[half][: dm.KR], values, jnp.zeros_like(values))
                scores = add_masked(dm, dot_last(keys, query_h))
                most = jnp.max(scores, axis=0, keepdims=True)
                e = jnp.exp(scores - most)
                norm = jnp.sum(e, axis=0, keepdims=True)
                lse[slot, pl.ds(2 * pair + half, 1), :] = most + jnp.log(norm)
                part = dot_rows((e * (1.0 / norm)).astype(BF16), values_h)
                total = part if total is None else total + part
            o[slot, :, lanes] = total.astype(BF16)

        @pl.when(jnp.logical_and(jnp.logical_not(early), slot + 1 < T))
        def _():
            fetch_qkv(slot + 1)

        return 0

    lax.fori_loop(0, T, heads, 0)

    keeps = []
    for number, (source, target) in enumerate(((q, qkeep), (k, kkeep), (v, vkeep), (o, okeep), (lse, lkeep))):
        keeps.append(pltpu.make_async_copy(source, target, la.at[2 + number]))
        keeps[-1].start()

    loads = []
    for slot in range(T):
        arrive(slot, 1)
        loads.append(
            pltpu.make_async_copy(source_of(slot, 1), wob.at[pl.ds(slot * W, W)], lw.at[2 + slot])
        )
        loads[-1].start()

    def arrive_ff(index):
        slot, c = dm.order[index]
        arrive(slot, 2 + 2 * c)
        arrive(slot, 3 + 2 * c)

    def load_ff(index, parity):
        slot, c = dm.order[index]
        return [
            pltpu.make_async_copy(source_of(slot, 2 + 2 * c), w1b.at[parity], lsem.at[3 + parity]),
            pltpu.make_async_copy(source_of(slot, 3 + 2 * c), w2b.at[parity], lsem.at[5 + parity]),
        ]

    def fetch_ff(which):
        for index in range(NI):

            @pl.when(which == index)
            def _():
                arrive_ff(index)
                for load in load_ff(index, index % 2):
                    load.start()

    fetch_ff(0)
    for load in loads:
        load.wait()
    attended = jnp.concatenate([o[slot, pl.ds(0, RP), :] for slot in range(T)], axis=1)
    for n in range(D // 256):
        acc[:, pl.ds(n * 256, 256)] = dot_plain(attended, wob[:, pl.ds(n * 256, 256)])

    out_bias = full_vector(dm, spb, OUT_BIAS)
    gain2, bias2 = full_vector(dm, spb, LN2_GAIN), full_vector(dm, spb, LN2_BIAS)
    down_bias = full_vector(dm, spb, FC2_BIAS)

    def second_norm(r, _):
        rows = pl.ds(pl.multiple_of(r * STEP, STEP), STEP)
        hidden = block_rows(dm, xarr, rows).astype(F32) + (acc[rows, :] + out_bias)
        hat, _inv = norm_rows(hidden, D)
        n2[rows, :] = (hat * gain2 + bias2).astype(BF16)
        acc[rows, :] = hidden
        return 0

    lax.fori_loop(0, RP // STEP, second_norm, 0)
    keep_h = pltpu.make_async_copy(acc, hkeep, lsem.at[0])
    keep_h.start()
    keep_h.wait()

    def keep_a(index, parity):
        return pltpu.make_async_copy(ab.at[parity], akeep.at[index], la.at[parity])

    def feed(index, _):
        parity = lax.rem(index, 2)
        for load in load_ff(0, parity):
            load.wait()
        early = jnp.logical_or(upper, index + 1 < 2 * dm.NC)

        @pl.when(jnp.logical_and(early, index + 1 < NI))
        def _():
            fetch_ff(index + 1)

        @pl.when(index >= 2)
        def _():
            keep_a(index - 2, parity).wait()

        a = dot_plain(n2[...], w1b[parity]) + b1r[index]
        ab[parity] = a
        gb[...] = (0.5 * a * (1.0 + lax.erf(a * ROOT_HALF))).astype(BF16)
        keep_a(index, parity).start()
        for n in range(D // 256):
            cols = pl.ds(n * 256, 256)
            acc[:, cols] += dot_plain(gb[...], w2b[parity, :, cols])

        @pl.when(jnp.logical_and(jnp.logical_not(early), index + 1 < NI))
        def _():
            fetch_ff(index + 1)

        return 0

    lax.fori_loop(0, NI, feed, 0)

    def close(r, _):
        rows = pl.ds(pl.multiple_of(r * STEP, STEP), STEP)
        y = (acc[rows, :] + down_bias).astype(BF16)
        for j in range(T):
            yb[j, rows, :] = y[:, j * W : (j + 1) * W]
        return 0

    lax.fori_loop(0, RP // STEP, close, 0)

    @pl.when(lower)
    def _():
        stream_copy.start()

    keep_y = pltpu.make_async_copy(yb, ykeep, lsem.at[0])
    keep_y.start()
    keep_y.wait()
    keep_x.wait()
    keep_p.wait()
    for keep in keeps:
        keep.wait()
    for index in (NI - 2, NI - 1):
        keep_a(index, index % 2).wait()
    for slot in range(1, T):
        vector_copy(slot).wait_send()
        input_copy(slot).wait_send()
        for index in range(dm.NCH):
            weight_copy(slot, index).wait_send()

    @pl.when(lower)
    def _():
        stream_copy.wait_send()


def partner_dynamic(dm, place, slot):
    bit = 1
    while bit < dm.T:
        take = lax.rem(lax.div(slot, bit), 2)
        place = place + take * (bit - 2 * bit * lax.rem(lax.div(place, bit), 2))
        bit *= 2
    return place


def forward_call(dm, xin, vectors, wqkv, wout, wup, wdown):
    T, W, D, RP, RL, C, NI, FL = dm.T, dm.W, dm.D, dm.RP, dm.RL, dm.C, dm.NI, dm.FL
    sds = jax.ShapeDtypeStruct
    outs = (
        sds((T, 3, D, W), BF16), sds((T, W, D), BF16), sds((T, D, FL), BF16), sds((T, FL, D), BF16),
        sds((T, RP, W), BF16), sds((T, RP, W), BF16),
        sds((T, RL, W), BF16), sds((T, RL, W), BF16), sds((T, RL, W), BF16), sds((T, RL, W), BF16),
        sds((T, dm.HS, RL), F32), sds((RP, D), F32), sds((NI, RP, C), F32), sds((T, VECTOR_ROWS, W), F32), sds((T, RP, W), BF16),
    )
    dma = pltpu.SemaphoreType.DMA
    scratch = [
        pltpu.VMEM((T, RP, W), BF16), pltpu.VMEM((RP, D), BF16), pltpu.VMEM((2, 3, D, W), BF16),
        pltpu.VMEM((D, D), BF16), pltpu.VMEM((2, D, C), BF16), pltpu.VMEM((2, C, D), BF16),
        pltpu.VMEM((2, RP, C), F32), pltpu.VMEM((RP, C), BF16), pltpu.VMEM((RP, D), F32),
        pltpu.VMEM((RP, D), BF16), pltpu.VMEM((T, RP, W), BF16), pltpu.VMEM((NI, 1, C), F32),
        pltpu.VMEM((T, VECTOR_ROWS, W), F32),
        pltpu.VMEM((T, RL, W), BF16), pltpu.VMEM((T, RL, W), BF16), pltpu.VMEM((T, RL, W), BF16), pltpu.VMEM((T, RL, W), BF16),
        pltpu.VMEM((T, dm.HS, RL), F32),
        dma((T, dm.NCH)), dma((T, dm.NCH)), dma((T,)), dma((T,)), dma((T,)), dma((T,)),
        dma((2,)), dma((8,)), dma((2 + T,)), dma((7,)),
    ]
    return pl.pallas_call(
        functools.partial(forward_kernel, dm),
        out_shape=outs,
        in_specs=[ANY] * 6,
        out_specs=[ANY] * len(outs),
        scratch_shapes=scratch,
        name="layer_forward",
        compiler_params=pltpu.CompilerParams(
            collective_id=0, has_side_effects=True, vmem_limit_bytes=VMEM_BYTES
        ),
    )(xin, vectors, wqkv, wout, wup, wdown)


def packed_vectors(dm, ln1_gain, ln1_bias, qv_bias, out_bias, ln2_gain, ln2_bias, fc1_bias, fc2_bias):
    rows = [ln1_gain, ln1_bias, qv_bias[0], out_bias, ln2_gain, ln2_bias, fc2_bias, fc1_bias]
    flat = jnp.concatenate([row.reshape(-1, dm.W) for row in rows], axis=0)
    return jnp.pad(flat, ((0, VECTOR_ROWS - flat.shape[0]), (0, 0)))


def padded_rows(dm, array):
    return jnp.pad(array, ((0, 0), (0, dm.RP - dm.tok), (0, 0)))


def dot_rows(left, right):
    return lax.dot_general(left, right, (((0,), (0,)), ((), ())), preferred_element_type=F32)


def fold(rows):
    total = rows[0:8, :]
    for first in range(8, rows.shape[0], 8):
        total = total + rows[first : first + 8, :]
    return total


def norm_rows_back(grad, hat, inv, gain, width):
    scaled = grad * gain
    mean = jnp.sum(scaled, axis=1, keepdims=True) * (1.0 / width)
    along = jnp.sum(scaled * hat, axis=1, keepdims=True) * (1.0 / width)
    return inv * (scaled - mean - hat * along)


def backward_kernel(
    dm,
    xc, xkeep, qkeep, kkeep, vkeep, okeep, lkeep, hkeep, akeep, spkeep, ykeep,
    wqkv, wout, wup, wdown, gqkv, gout, gup, gdown,
    dqkv, dout, dup, ddown, result, dxkeep, flat_sums, head_sums, up_sums,
    arr, dyb, acc, dh, hh, dhb, gs, das, n1t, n2t, nb, q, k, v, o, do, dq, dk, dv, xx,
    w1b, w2b, ab, wob, wq, s1, s2, yb, spb, fs, hs, us, lse,
    ssem, osend, orecv, lsem, lw, lq, lg,
):
    section, tensor = lax.axis_index("section"), lax.axis_index("tensor")
    T, W, D, RP, RL, C, NI = dm.T, dm.W, dm.D, dm.RP, dm.RL, dm.C, dm.NI
    lower, upper = section == 0, section == 1
    own = (wqkv, wout, wup, wdown)
    real = pl.ds(0, RP)

    def source_of(slot, index):
        if slot == 0:
            return chunk_refs(dm, index, *own)
        return chunk_refs(dm, index, gqkv.at[slot], gout.at[slot], gup.at[slot], gdown.at[slot])

    stream_copy = pltpu.make_async_remote_copy(
        src_ref=arr,
        dst_ref=arr,
        send_sem=ssem.at[0],
        recv_sem=ssem.at[1],
        device_id={"section": 1 - section},
    )

    def output_copy(slot):
        return pltpu.make_async_remote_copy(
            src_ref=ykeep.at[partner(tensor, slot)],
            dst_ref=result.at[tensor],
            send_sem=osend.at[slot],
            recv_sem=orecv.at[slot],
            device_id={"tensor": partner(tensor, slot)},
        )

    def load_ff(index, parity):
        slot, c = dm.order[index]
        return [
            pltpu.make_async_copy(source_of(slot, 2 + 2 * c), w1b.at[parity], lw.at[parity]),
            pltpu.make_async_copy(source_of(slot, 3 + 2 * c), w2b.at[parity], lw.at[2 + parity]),
            pltpu.make_async_copy(akeep.at[index], ab.at[parity], lw.at[4 + parity]),
        ]

    def fetch_ff(which):
        for index in range(NI):

            @pl.when(which == index)
            def _():
                for load in load_ff(index, index % 2):
                    load.start()

    fetch_ff(0)
    loads = [
        pltpu.make_async_copy(source, target, lsem.at[number])
        for number, (source, target) in enumerate(
            ((spkeep, spb), (hkeep, hh), (qkeep, q), (kkeep, k), (vkeep, v), (okeep, o), (xkeep, xx), (lkeep, lse))
        )
    ]
    for load in loads:
        load.start()
    out_loads = [
        pltpu.make_async_copy(source_of(slot, 1), wob.at[pl.ds(slot * W, W)], lq.at[2 + slot])
        for slot in range(T)
    ]
    for load in out_loads:
        load.start()

    meet(dm, section, tensor)
    for slot in range(1, T):
        output_copy(slot).start()
    own_out = pltpu.make_async_copy(ykeep.at[tensor], result.at[tensor], lsem.at[8])
    own_out.start()

    @pl.when(upper)
    def _():
        load = pltpu.make_async_copy(xc, arr, lsem.at[9])
        load.start()
        load.wait()

    tail_rows = pl.ds(RP, RL - RP)
    blank = jnp.zeros((RL - RP, D), BF16)
    dyb[tail_rows, :] = blank
    dhb[tail_rows, :] = blank
    nb[tail_rows, :] = blank
    for index in range(NI):
        gs[index, tail_rows, :] = blank[:, :C]
        das[index, tail_rows, :] = blank[:, :C]
    for slot in range(T):
        do[slot, tail_rows, :] = blank[:, :W]
        if dm.KR < RL:
            for ref in (dk, dv):
                ref[slot, pl.ds(dm.KR, RL - dm.KR), :] = jnp.zeros((RL - dm.KR, W), BF16)
    acc[...] = jnp.zeros_like(acc)
    fs[...] = jnp.zeros_like(fs)
    hs[...] = jnp.zeros_like(hs)

    @pl.when(lower)
    def _():
        stream_copy.wait_recv()

    def spread(r, _):
        rows = pl.ds(pl.multiple_of(r * STEP, STEP), STEP)
        incoming = block_rows(dm, arr, rows)
        if T > dm.micro:
            incoming = jnp.where(tensor < dm.micro, incoming, jnp.zeros_like(incoming))
        dyb[rows, :] = incoming
        return 0

    lax.fori_loop(0, RP // STEP, spread, 0)

    def feed_back(index, _):
        parity = lax.rem(index, 2)
        for load in load_ff(0, parity):
            load.wait()

        @pl.when(index + 1 < NI)
        def _():
            fetch_ff(index + 1)

        for first in range(0, C, 256):
            cols = pl.ds(first, 256)
            a = ab[parity, :, cols]
            cdf = 0.5 * (1.0 + lax.erf(a * ROOT_HALF))
            gs[index, real, cols] = (a * cdf).astype(BF16)
            slope = cdf + a * jnp.exp(-0.5 * a * a) * GAUSS_FACTOR
            da = dot_last(dyb[real, :], w2b[parity, cols, :]) * slope
            das[index, real, cols] = da.astype(BF16)
            us[index, :, cols] = jnp.sum(fold(da), axis=0, keepdims=True)
        for n in range(D // 256):
            cols = pl.ds(n * 256, 256)
            acc[:, cols] += dot_last(das[index, real, :], w1b[parity, cols, :])
        return 0

    lax.fori_loop(0, NI, feed_back, 0)

    for load in loads:
        load.wait()
    for load in out_loads:
        load.wait()
    gain2, bias2 = full_vector(dm, spb, LN2_GAIN), full_vector(dm, spb, LN2_BIAS)

    def second_norm(r, _):
        rows = pl.ds(pl.multiple_of(r * STEP, STEP), STEP)
        hat, inv = norm_rows(hh[rows, :], D)
        grad = acc[rows, :]
        dy = dyb[rows, :].astype(F32)
        fs[0] += fold(grad * hat)
        fs[1] += fold(grad)
        whole = dy + norm_rows_back(grad, hat, inv, gain2, D)
        dh[rows, :] = whole
        dhb[rows, :] = whole.astype(BF16)
        fs[2] += fold(whole)
        fs[3] += fold(dy)
        nb[rows, :] = (hat * gain2 + bias2).astype(BF16)
        return 0

    lax.fori_loop(0, RP // STEP, second_norm, 0)

    def turn(target):
        for n in range(D // 256):
            cols = pl.ds(n * 256, 256)
            target[cols, :] = nb[:, cols].T

    turn(n2t)

    def put_ff(index, parity):
        slot, c = dm.order[index]
        return [
            pltpu.make_async_copy(s1.at[parity], dup.at[slot, :, pl.ds(c * C, C)], lg.at[parity]),
            pltpu.make_async_copy(s2.at[parity], ddown.at[slot, pl.ds(c * C, C), :], lg.at[2 + parity]),
        ]

    def feed_weights():
        def one(index, _):
            parity = lax.rem(index, 2)

            @pl.when(index >= 2)
            def _():
                for put in put_ff(0, parity):
                    put.wait()

            for n in range(D // 256):
                cols = pl.ds(n * 256, 256)
                s1[parity, cols, :] = dot_plain(n2t[cols, :], das[index])
            for n in range(C // 256):
                cols = pl.ds(n * 256, 256)
                s2[parity, cols, :] = dot_rows(gs[index, :, cols], dyb[...])
            for j in range(NI):

                @pl.when(index == j)
                def _():
                    for put in put_ff(j, j % 2):
                        put.start()

            return 0

        lax.fori_loop(0, NI, one, 0)
        for parity in range(2):
            for put in put_ff(0, parity):
                put.wait()

    @pl.when(lower)
    def _():
        feed_weights()

    for slot in range(T):
        do[slot, real, :] = dot_last(dhb[real, :], wob[pl.ds(slot * W, W), :]).astype(BF16)

    masks = half_masks(RL)
    scale = jnp.asarray(HEAD_DIM**-0.5, BF16)
    real_keys = pl.ds(0, dm.KR)

    def heads(slot, _):
        for pair in range(W // 128):
            lanes = slice(pair * 128, pair * 128 + 128)
            keys, values = k[slot, real_keys, lanes], v[slot, real_keys, lanes]
            query, grad = q[slot, :, lanes] * scale, do[slot, :, lanes]
            scaled_keys = keys * scale
            sums = None
            for half in range(2):
                mask = masks[half]
                query_h = jnp.where(mask, query, jnp.zeros_like(query))
                grad_h = jnp.where(mask, grad, jnp.zeros_like(grad))
                keys_h = jnp.where(mask[: dm.KR], scaled_keys, jnp.zeros_like(keys))
                scores = add_masked(dm, dot_last(keys, query_h))
                p = jnp.exp(scores - lse[slot, pl.ds(2 * pair + half, 1), :])
                dp = dot_last(values, grad_h)
                delta = jnp.sum(p * dp, axis=0, keepdims=True)
                ds = (p * (dp - delta)).astype(BF16)
                terms = (dot_rows(ds, keys_h), dot_plain(ds, query_h), dot_plain(p.astype(BF16), grad_h))
                sums = terms if sums is None else tuple(x + y for x, y in zip(sums, terms))
            dq_pair, dk_pair, dv_pair = sums
            dq[slot, :, lanes] = dq_pair.astype(BF16)
            dk[slot, real_keys, lanes] = dk_pair.astype(BF16)
            dv[slot, real_keys, lanes] = dv_pair.astype(BF16)
            hs[slot, 0, :, lanes] += fold(dq_pair)
            hs[slot, 1, :, lanes] += fold(dv_pair)
        return 0

    lax.fori_loop(0, T, heads, 0)

    def load_qkv(slot, parity):
        return pltpu.make_async_copy(source_of(slot, 0), wq.at[parity], lq.at[parity])

    load_qkv(0, 0).start()
    for slot in range(T):
        load_qkv(slot, slot % 2).wait()
        if slot + 1 < T:
            load_qkv(slot + 1, (slot + 1) % 2).start()
        for n in range(D // 256):
            cols = pl.ds(n * 256, 256)
            part = dot_last(dq[slot, real, :], wq[slot % 2, 0, cols, :])
            part = part + dot_last(dk[slot, real, :], wq[slot % 2, 1, cols, :])
            part = part + dot_last(dv[slot, real, :], wq[slot % 2, 2, cols, :])
            if slot == 0:
                acc[:, cols] = part
            else:
                acc[:, cols] += part

    gain1, bias1 = full_vector(dm, spb, LN1_GAIN), full_vector(dm, spb, LN1_BIAS)

    def first_norm(r, _):
        rows = pl.ds(pl.multiple_of(r * STEP, STEP), STEP)
        hat, inv = norm_rows(block_rows(dm, xx, rows).astype(F32), D)
        grad = acc[rows, :]
        fs[4] += fold(grad * hat)
        fs[5] += fold(grad)
        whole = dh[rows, :] + norm_rows_back(grad, hat, inv, gain1, D)
        nb[rows, :] = (hat * gain1 + bias1).astype(BF16)
        low = whole.astype(BF16)
        for j in range(T):
            yb[j, rows, :] = whole[:, j * W : (j + 1) * W]
            xx[j, rows, :] = low[:, j * W : (j + 1) * W]
        return 0

    lax.fori_loop(0, RP // STEP, first_norm, 0)

    down_copy = pltpu.make_async_remote_copy(
        src_ref=xx,
        dst_ref=arr,
        send_sem=ssem.at[0],
        recv_sem=ssem.at[1],
        device_id={"section": 1 - section},
    )

    @pl.when(upper)
    def _():
        down_copy.start()

    keep_dx = pltpu.make_async_copy(yb, dxkeep, lsem.at[0])
    keep_dx.start()
    turn(n1t)

    pending = []
    for slot in range(T):
        for number, source in enumerate((dq, dk, dv)):
            turn_number = len(pending) % 2
            if len(pending) >= 2:
                pending[-2].wait()
            for n in range(D // 256):
                cols = pl.ds(n * 256, 256)
                s1[turn_number, cols, pl.ds(0, W)] = dot_plain(n1t[cols, :], source[slot])
            pending.append(
                pltpu.make_async_copy(
                    s1.at[turn_number, :, pl.ds(0, W)], dqkv.at[slot, number], lg.at[turn_number]
                )
            )
            pending[-1].start()
    for put in pending[-2:]:
        put.wait()
    pending = []
    for slot in range(T):
        if len(pending) >= 2:
            pending[-2].wait()
        s2[slot % 2, pl.ds(0, W), :] = dot_rows(o[slot], dhb[...])
        pending.append(pltpu.make_async_copy(s2.at[slot % 2, pl.ds(0, W), :], dout.at[slot], lg.at[2 + slot % 2]))
        pending[-1].start()
    for put in pending[-2:]:
        put.wait()

    @pl.when(upper)
    def _():
        feed_weights()

    keeps = []
    for number, (source, target) in enumerate(((fs, flat_sums), (hs, head_sums), (us, up_sums))):
        keeps.append(pltpu.make_async_copy(source, target, lsem.at[1 + number]))
        keeps[-1].start()
    for keep in keeps:
        keep.wait()
    keep_dx.wait()
    own_out.wait()
    for slot in range(1, T):
        output_copy(slot).wait()

    @pl.when(upper)
    def _():
        down_copy.wait_send()


def backward_call(dm, kept, own):
    T, W, D, RP, RL, C, NI, FL = dm.T, dm.W, dm.D, dm.RP, dm.RL, dm.C, dm.NI, dm.FL
    sds = jax.ShapeDtypeStruct
    gathered, rest = kept[:4], kept[4:]
    outs = (
        sds((T, 3, D, W), F32), sds((T, W, D), F32), sds((T, D, FL), F32), sds((T, FL, D), F32),
        sds((T, RP, W), BF16), sds((T, RP, W), F32), sds((6, 8, D), F32), sds((T, 2, 8, W), F32), sds((NI, 1, C), F32),
    )
    dma = pltpu.SemaphoreType.DMA
    heads = pltpu.VMEM((T, RL, W), BF16)
    scratch = [
        pltpu.VMEM((T, RP, W), BF16), pltpu.VMEM((RL, D), BF16), pltpu.VMEM((RP, D), F32), pltpu.VMEM((RP, D), F32),
        pltpu.VMEM((RP, D), F32), pltpu.VMEM((RL, D), BF16), pltpu.VMEM((NI, RL, C), BF16), pltpu.VMEM((NI, RL, C), BF16),
        pltpu.VMEM((D, RL), BF16), pltpu.VMEM((D, RL), BF16), pltpu.VMEM((RL, D), BF16),
        heads, heads, heads, heads, heads, heads, heads, heads, pltpu.VMEM((T, RP, W), BF16),
        pltpu.VMEM((2, D, C), BF16), pltpu.VMEM((2, C, D), BF16), pltpu.VMEM((2, RP, C), F32),
        pltpu.VMEM((D, D), BF16), pltpu.VMEM((2, 3, D, W), BF16), pltpu.VMEM((2, D, C), F32), pltpu.VMEM((2, C, D), F32),
        pltpu.VMEM((T, RP, W), F32), pltpu.VMEM((T, VECTOR_ROWS, W), F32),
        pltpu.VMEM((6, 8, D), F32), pltpu.VMEM((T, 2, 8, W), F32), pltpu.VMEM((NI, 1, C), F32),
        pltpu.VMEM((T, dm.HS, RL), F32),
        dma((2,)), dma((T,)), dma((T,)), dma((10,)), dma((6,)), dma((2 + T,)), dma((8,)),
    ]
    return pl.pallas_call(
        functools.partial(backward_kernel, dm),
        out_shape=outs,
        in_specs=[ANY] * 19,
        out_specs=[ANY] * len(outs),
        scratch_shapes=scratch,
        name="layer_backward",
        compiler_params=pltpu.CompilerParams(
            collective_id=1, has_side_effects=True, vmem_limit_bytes=VMEM_BYTES
        ),
    )(*rest, *own, *gathered)


def piece_list(dm):
    down, up, out, qkv = [], [], [], []
    for first in range(0, dm.FL, 128):
        down.append((3, first, 128))
    for first in range(0, dm.D, 128):
        up.append((2, first, 128))
    for first in range(0, dm.W, 128):
        out.append((1, first, 128))
    for first in range(0, 3 * dm.D, 512):
        qkv.append((0, first, 512))
    return down + up + out + qkv


def reduce_kernel(
    dm,
    dqkv, dout, dup, ddown, dxkeep, flat_sums, head_sums, up_sums,
    rqkv, rout, rup, rdown, result, fqkv, fout, fup, fdown, rsmall,
    *scratch,
):
    section, dp, tensor = lax.axis_index("section"), lax.axis_index("dp"), lax.axis_index("tensor")
    T, W, D, FL, NI, C = dm.T, dm.W, dm.D, dm.FL, dm.NI, dm.C
    line = lax.axis_size("dp")
    stages = dm.stages
    scratch = list(scratch)
    kept, come = scratch.pop(0), scratch.pop(0)
    land = [[scratch.pop(0) for _ in range(4)] for _ in range(stages)]
    inward = [scratch.pop(0) for _ in range(4)]
    outward = [scratch.pop(0) for _ in range(4)]
    parts, gathered, small_in, small_out, small_own = [scratch.pop(0) for _ in range(5)]
    lsend, lrecv, isend, irecv, osend, orecv, msem, wsem, gsend, grecv, vsem, dsend, drecv = scratch
    first_land = (fqkv, fout, fup, fdown)
    partial = (dqkv, dout, dup, ddown)
    reduced = (rqkv, rout, rup, rdown)
    pieces = piece_list(dm)
    NP = len(pieces)

    half = line // 2
    left = dp < half
    outer = jnp.logical_or(dp == 0, dp == line - 1)
    middle = jnp.logical_or(dp == half - 1, dp == half)
    toward = jnp.where(left, 1, -1)
    inner_dp = dp + toward
    outer_dp = lax.rem(dp - toward + line, line)

    barrier = pltpu.get_barrier_semaphore()
    for slot in range(1, T):
        pl.semaphore_signal(barrier, inc=1, device_id={"tensor": partner(tensor, slot)})
    pl.semaphore_signal(barrier, inc=1, device_id={"dp": lax.rem(dp + 1, line)})
    pl.semaphore_signal(barrier, inc=1, device_id={"dp": lax.rem(dp + line - 1, line)})
    pl.semaphore_wait(barrier, T + 1)

    def at(ref, piece, *lead):
        kind, first, rows = pieces[piece]
        return ref[kind].at[(*lead, pl.ds(first, rows), slice(None))]

    def lowest(slot):
        stage = 0
        while slot % 2 == 0:
            slot //= 2
            stage += 1
        return stage

    def fold_copy(piece, slot):
        stage = lowest(slot)
        bit = 1 << stage
        place = (slot - bit) >> (stage + 1)
        if stage == 0:
            source, target = at(partial, piece, slot), at(first_land, piece, place)
        else:
            source, target = at(land[0], piece, slot // 2), at(land[stage], piece, place)
        return pltpu.make_async_remote_copy(
            src_ref=source,
            dst_ref=target,
            send_sem=lsend.at[piece, slot],
            recv_sem=lrecv.at[piece, slot],
            device_id={"tensor": flip(tensor, bit)},
        )

    def inward_copy(piece, source):
        return pltpu.make_async_remote_copy(
            src_ref=source,
            dst_ref=at(inward, piece),
            send_sem=isend.at[piece],
            recv_sem=irecv.at[piece],
            device_id={"dp": inner_dp},
        )

    def meet_copy(piece, source):
        return pltpu.make_async_remote_copy(
            src_ref=source,
            dst_ref=at(outward, piece),
            send_sem=isend.at[piece],
            recv_sem=orecv.at[piece],
            device_id={"dp": inner_dp},
        )

    def outward_copy(piece):
        return pltpu.make_async_remote_copy(
            src_ref=at(outward, piece),
            dst_ref=at(outward, piece),
            send_sem=osend.at[piece],
            recv_sem=orecv.at[piece],
            device_id={"dp": outer_dp},
        )

    def loads(piece, slot):
        kind, first, rows = pieces[piece]
        wide = (W, D, FL, D)[kind]
        view = (slot // 2, piece % 2, kind)
        pair = []
        for number, (stage, ref) in enumerate(((kept, at(partial, piece, slot)), (come, at(first_land, piece, slot // 2)))):
            place = stage[view[2]].at[view[0], view[1]]
            pair.append(pltpu.make_async_copy(ref, place, msem.at[number, slot // 2, piece % 2, int(kind == 0)]))
        return pair

    def fetch(piece, slot):
        if piece < NP:
            fold_copy(piece, slot + 1).wait_recv()
            for one in loads(piece, slot):
                one.start()

    def input_grad_copy(slot):
        return pltpu.make_async_remote_copy(
            src_ref=dxkeep.at[partner(tensor, slot)],
            dst_ref=result.at[tensor],
            send_sem=dsend.at[slot],
            recv_sem=drecv.at[slot],
            device_id={"tensor": partner(tensor, slot)},
        )

    def store(piece):
        return pltpu.make_async_copy(at(outward, piece), at(reduced, piece), wsem.at[piece])

    for j in range(T):
        for row in range(6):
            parts[j, row : row + 1, :] = jnp.sum(flat_sums[row, :, j * W : (j + 1) * W], axis=0, keepdims=True)
        parts[j, 8 + FL // W : VECTOR_ROWS, :] = jnp.zeros((VECTOR_ROWS - 8 - FL // W, W), F32)
    per = C // W
    for slot in range(T):
        place = partner(tensor, slot)
        for row in range(2):
            parts[place, 6 + row : 7 + row, :] = jnp.sum(head_sums[slot, row], axis=0, keepdims=True)
        for index, (owner, c) in enumerate(dm.order):
            if owner == slot:
                for i in range(per):
                    row = 8 + c * per + i
                    parts[place, row : row + 1, :] = up_sums[index, :, i * W : (i + 1) * W]

    def small_copy(slot):
        return pltpu.make_async_remote_copy(
            src_ref=parts.at[partner(tensor, slot)],
            dst_ref=gathered.at[slot],
            send_sem=gsend.at[slot],
            recv_sem=grecv.at[slot],
            device_id={"tensor": partner(tensor, slot)},
        )

    def small_line(number, source, target, place):
        return pltpu.make_async_remote_copy(
            src_ref=source,
            dst_ref=target,
            send_sem=vsem.at[number],
            recv_sem=vsem.at[number + 1],
            device_id={"dp": place},
        )

    for piece in range(NP):
        for slot in range(1, T, 2):
            fold_copy(piece, slot).start()
    for slot in range(1, T):
        small_copy(slot).start()
    own_grad = pltpu.make_async_copy(dxkeep.at[tensor], result.at[tensor], dsend.at[0])
    own_grad.start()

    def rows_of(piece):
        kind, first, rows = pieces[piece]
        width = (W, D, FL, D)[kind]
        step = max(16, min(rows, 32768 // width))
        return kind, first, rows // step, step

    def add_into(piece, target, sources, staged=None):
        kind, first, count, step = rows_of(piece)

        def one(r, _):
            rows = pl.ds(pl.multiple_of(first + r * step, 16), step)
            near = pl.ds(pl.multiple_of(r * step, 16), step)
            total = None
            if staged is not None:
                lead = (staged // 2, piece % 2, near, slice(None))
                total = kept[kind][lead] + come[kind][lead]
            for ref, lead in sources:
                term = ref[kind][(*lead, rows, slice(None))].astype(F32)
                total = term if total is None else total + term
            target[0][kind][(*target[1], rows, slice(None))] = total.astype(BF16)
            return 0

        lax.fori_loop(0, count, one, 0)

    def pass_on(piece, stage):
        bit = 1 << stage
        for slot in range(bit, T, 2 * bit):
            for before in range(1, stage):
                fold_copy(piece, slot + (1 << before)).wait_recv()
            for one in loads(piece, slot):
                one.wait()
            add_into(
                piece,
                (land[0], (slot // 2,)),
                [(land[b], (slot >> (b + 1),)) for b in range(1, stage)],
                staged=slot,
            )
            fold_copy(piece, slot).start()
            fetch(piece + 2, slot)

    own_terms = [(land[b], (0,)) for b in range(1, stages)]

    def own_sum(piece):
        for stage in range(1, stages):
            fold_copy(piece, 1 << stage).wait_recv()

        @pl.when(outer)
        def _():
            for one in loads(piece, 0):
                one.wait()
            add_into(piece, (land[0], (0,)), own_terms, staged=0)
            inward_copy(piece, at(land[0], piece, 0)).start()
            fetch(piece + 2, 0)

    def gather_in(piece):
        @pl.when(jnp.logical_not(outer))
        def _():
            for one in loads(piece, 0):
                one.wait()
            inward_copy(piece, at(inward, piece)).wait_recv()
            add_into(piece, (inward, ()), own_terms + [(inward, ())], staged=0)

            @pl.when(middle)
            def _():
                meet_copy(piece, at(inward, piece)).start()

            @pl.when(jnp.logical_not(middle))
            def _():
                inward_copy(piece, at(inward, piece)).start()

            fetch(piece + 2, 0)

    def spread_middle(piece):
        @pl.when(middle)
        def _():
            meet_copy(piece, at(inward, piece)).wait_recv()
            add_into(piece, (outward, ()), [(outward, ()), (inward, ())])
            outward_copy(piece).start()
            store(piece).start()

    def spread_out(piece):
        @pl.when(jnp.logical_not(middle))
        def _():
            outward_copy(piece).wait_recv()

            @pl.when(jnp.logical_not(outer))
            def _():
                outward_copy(piece).start()

            store(piece).start()

    def small_chain():
        for slot in range(1, T):
            small_copy(slot).wait_recv()
        total = parts[tensor]
        for slot in range(1, T):
            total = total + gathered[slot]
        small_own[...] = total

        @pl.when(outer)
        def _():
            small_line(0, small_own, small_in, inner_dp).start()

        @pl.when(jnp.logical_not(outer))
        def _():
            small_line(0, small_own, small_in, inner_dp).wait_recv()
            small_in[...] = small_in[...] + small_own[...]

            @pl.when(jnp.logical_not(middle))
            def _():
                small_line(0, small_in, small_in, inner_dp).start()

        @pl.when(middle)
        def _():
            meeting = small_line(2, small_in, small_out, inner_dp)
            meeting.start()
            meeting.wait_recv()
            small_out[...] = small_out[...] + small_in[...]
            small_line(4, small_out, small_out, outer_dp).start()

        @pl.when(jnp.logical_not(middle))
        def _():
            small_line(4, small_out, small_out, outer_dp).wait_recv()

            @pl.when(jnp.logical_not(outer))
            def _():
                small_line(4, small_out, small_out, outer_dp).start()

        rsmall[...] = small_out[...]

    def run(action, piece, *rest):
        if 0 <= piece < NP:
            action(piece, *rest)

    for piece in range(2):
        for slot in range(0, T, 2):
            fetch(piece, slot)
    ahead = 1
    depth = stages - 1
    for stage in range(1, stages):
        for piece in range(ahead + (depth - stage)):
            run(pass_on, piece, stage)
    for step in range(NP + 4):
        for stage in range(1, stages):
            run(pass_on, step + ahead + (depth - stage), stage)
        run(own_sum, step)
        run(gather_in, step - 1)
        run(spread_middle, step - 2)
        run(spread_out, step - 3)
        if step == NP - 1:
            for slot in range(1, T):
                input_grad_copy(slot).start()
        if step == NP:
            small_chain()

    for piece in range(NP):
        store(piece).wait()
        for slot in range(1, T):
            fold_copy(piece, slot).wait_send()

        @pl.when(jnp.logical_not(middle))
        def _():
            inward_copy(piece, at(inward, piece)).wait_send()

        @pl.when(middle)
        def _():
            meet_copy(piece, at(inward, piece)).wait_send()

        @pl.when(jnp.logical_not(outer))
        def _():
            outward_copy(piece).wait_send()

    own_grad.wait()
    for slot in range(1, T):
        small_copy(slot).wait_send()
        input_grad_copy(slot).wait()

    @pl.when(jnp.logical_not(middle))
    def _():
        small_line(0, small_in, small_in, inner_dp).wait_send()

    @pl.when(middle)
    def _():
        small_line(2, small_in, small_out, inner_dp).wait_send()

    @pl.when(jnp.logical_not(outer))
    def _():
        small_line(4, small_out, small_out, outer_dp).wait_send()


def reduce_call(dm, partial, dx, sums):
    T, W, D, FL = dm.T, dm.W, dm.D, dm.FL
    dm.stages = T.bit_length() - 1
    sds = jax.ShapeDtypeStruct
    dims = ((3 * D, W), (W, D), (D, FL), (FL, D))
    partial = (partial[0].reshape(T, 3 * D, W),) + tuple(partial[1:])
    outs = tuple(sds(d, BF16) for d in dims) + (sds(dx.shape, F32),)
    outs += tuple(sds((T // 2, *d), F32) for d in dims) + (sds((VECTOR_ROWS, W), F32),)
    NP = len(piece_list(dm))
    dma = pltpu.SemaphoreType.DMA
    staged = [pltpu.VMEM((T // 2, 2, 512, W), F32)] + [pltpu.VMEM((T // 2, 2, 128, w), F32) for w in (D, FL, D)]
    scratch = [staged, staged]
    for stage in range(dm.stages):
        scratch += [pltpu.VMEM((max(T >> (stage + 1), 1), *d), BF16) for d in dims]
    scratch += [pltpu.VMEM(d, BF16) for d in dims] * 2
    scratch += [pltpu.VMEM((T, VECTOR_ROWS, W), F32)] * 2 + [pltpu.VMEM((VECTOR_ROWS, W), F32)] * 3
    scratch += [
        dma((NP, T)), dma((NP, T)), dma((NP,)), dma((NP,)), dma((NP,)), dma((NP,)),
        dma((2, T // 2, 2, 2)), dma((NP,)), dma((T,)), dma((T,)), dma((6,)), dma((T,)), dma((T,)),
    ]
    whole = pl.BlockSpec(memory_space=pltpu.VMEM)
    return pl.pallas_call(
        functools.partial(reduce_kernel, dm),
        out_shape=outs,
        in_specs=[ANY] * 5 + [whole] * 3,
        out_specs=[ANY] * 9 + [whole],
        scratch_shapes=scratch,
        name="grad_reduce",
        compiler_params=pltpu.CompilerParams(
            collective_id=2, has_side_effects=True, vmem_limit_bytes=VMEM_BYTES
        ),
    )(*partial, dx, *sums)


def shards(
    images, cotangent, ln1_gain, ln1_bias, qkv_weight, qv_bias, out_weight, out_bias,
    ln2_gain, ln2_bias, fc1_weight, fc1_bias, fc2_weight, fc2_bias,
):
    dm = sizes_of(images, fc1_weight, lax.axis_size("tensor"))
    T, W, D = dm.T, dm.W, dm.D
    section, tensor = lax.axis_index("section"), lax.axis_index("tensor")
    xin = padded_rows(dm, jnp.where(section == 0, images[:, 0], cotangent[:, 0]))
    vectors = packed_vectors(
        dm, ln1_gain[0], ln1_bias[0], qv_bias, out_bias[0], ln2_gain[0], ln2_bias[0], fc1_bias[0], fc2_bias[0]
    )
    own = (qkv_weight[0], out_weight[0], fc1_weight[0], fc2_weight[0])
    kept = forward_call(dm, xin, vectors, *own)
    dqkv, dout, dup, ddown, result, dx, flat_sums, head_sums, up_sums = backward_call(dm, kept, own)
    section_out = result[: dm.micro, : dm.tok][None, :, None]

    rqkv, rout, rup, rdown, result, _, _, _, _, small = reduce_call(
        dm, (dqkv, dout, dup, ddown), dx, (flat_sums, head_sums, up_sums)
    )
    input_grads = result[: dm.micro, : dm.tok][None, :, None]
    g2, b2, ob, db, g1, b1 = (small[i][None] for i in range(6))
    qv = small[6:8][None]
    ub = small[8 : 8 + dm.FL // W].reshape(1, -1)
    wide = lambda array: array.astype(F32)[None]
    return (
        section_out, input_grads, g1, b1, wide(rqkv.reshape(3, D, W)), qv, wide(rout), ob, g2, b2,
        wide(rup), ub, wide(rdown), db,
    )


def solution(mesh):
    vector = P("section", "tensor")
    rows = P(None, "dp", None, "tensor")
    placed_rows = P("section", None, "dp", None, "tensor")
    qkv, qv = P("section", None, None, "tensor"), P("section", None, "tensor")
    by_row, by_column = P("section", "tensor", None), P("section", None, "tensor")
    return jax.shard_map(
        shards,
        mesh=mesh,
        in_specs=(rows, rows, vector, vector, qkv, qv, by_row, vector, vector, vector, by_column, vector, by_row, vector),
        out_specs=(
            placed_rows, placed_rows, vector, vector, qkv, qv, by_row, vector, vector, vector,
            by_column, vector, by_row, vector,
        ),
        check_vma=False,
    )
```

```python
import functools
import types

import jax
import jax.numpy as jnp
from jax import lax
from jax.experimental import pallas as pl
from jax.experimental.pallas import tpu as pltpu
from jax.sharding import PartitionSpec as P

BF16, F32 = jnp.bfloat16, jnp.float32
HEAD_DIM = 64
EPSILON = 1e-06
ROOT_HALF = 0.7071067811865476
GAUSS_FACTOR = 0.3989422804014327
MASKED = -1e30
STEP = 32
ANY = pl.BlockSpec(memory_space=pl.ANY)
VMEM_BYTES = 67043328

LN1_GAIN, LN1_BIAS, Q_BIAS, V_BIAS, OUT_BIAS, LN2_GAIN, LN2_BIAS, FC2_BIAS, FC1_BIAS = range(9)
VECTOR_ROWS = 16


def flip(place, bit):
    return place + bit - 2 * bit * lax.rem(lax.div(place, bit), 2)


def partner(place, slot):
    bit = 1
    while bit <= slot:
        if slot & bit:
            place = flip(place, bit)
        bit *= 2
    return place


def sizes_of(images, fc1_weight, tensor):
    micro, _, tok, width = images.shape
    dm = types.SimpleNamespace()
    dm.T, dm.W, dm.micro, dm.tok = tensor, width, micro, tok
    dm.D = width * tensor
    dm.FL = fc1_weight.shape[2]
    dm.RP = -(-tok // STEP) * STEP
    dm.RL = -(-tok // 128) * 128
    dm.KR = -(-tok // 16) * 16
    dm.HS = width // HEAD_DIM
    dm.C = min(512, dm.FL)
    dm.NC = dm.FL // dm.C
    dm.order = [
        (2 * p + half, c) for p in range(tensor // 2) for c in range(dm.NC) for half in range(2)
    ]
    dm.NI = len(dm.order)
    dm.NCH = 2 + 2 * dm.NC
    return dm


def full_vector(dm, vectors, row):
    return jnp.concatenate([vectors[j, row : row + 1, :] for j in range(dm.T)], axis=1)


def norm_rows(rows, width):
    mean = jnp.sum(rows, axis=1, keepdims=True) * (1.0 / width)
    var = jnp.sum(rows * rows, axis=1, keepdims=True) * (1.0 / width) - mean * mean
    inv = lax.rsqrt(var + EPSILON)
    return (rows - mean) * inv, inv


def block_rows(dm, ref, rows):
    return jnp.concatenate([ref[j, rows, :] for j in range(dm.T)], axis=1)


def dot_last(left, right):
    return lax.dot_general(left, right, (((1,), (1,)), ((), ())), preferred_element_type=F32)


def dot_plain(left, right):
    return lax.dot_general(left, right, (((1,), (0,)), ((), ())), preferred_element_type=F32)


def add_masked(dm, scores):
    cut = dm.tok // 8 * 8
    if cut == dm.KR:
        return scores
    row = lax.broadcasted_iota(jnp.int32, (dm.KR - cut, 1), 0) + cut
    bias = jnp.where(row < dm.tok, 0.0, MASKED).astype(F32)
    return jnp.concatenate([scores[:cut], scores[cut:] + bias], axis=0)


def half_masks(rows):
    lane = lax.broadcasted_iota(jnp.int32, (rows, 128), 1)
    return [lane < HEAD_DIM, lane >= HEAD_DIM]


def chunk_refs(dm, index, qkv, out, up, down):
    if index == 0:
        return qkv
    if index == 1:
        return out
    c = (index - 2) // 2
    if index % 2 == 0:
        return up.at[:, pl.ds(c * dm.C, dm.C)]
    return down.at[pl.ds(c * dm.C, dm.C), :]


def meet(dm, section, tensor, dp=None):
    barrier = pltpu.get_barrier_semaphore()
    if dp is not None:
        line = lax.axis_size("dp")
        pl.semaphore_signal(barrier, inc=1, device_id={"dp": lax.rem(dp + 1, line)})
        pl.semaphore_signal(barrier, inc=1, device_id={"dp": lax.rem(dp + line - 1, line)})
    for slot in range(1, dm.T):
        pl.semaphore_signal(barrier, inc=1, device_id={"tensor": partner(tensor, slot)})
    pl.semaphore_signal(barrier, inc=1, device_id={"section": 1 - section})
    pl.semaphore_wait(barrier, dm.T if dp is None else dm.T + 2)


def forward_kernel(
    dm,
    xin, spin, wqkv, wout, wup, wdown,
    gqkv, gout, gup, gdown, xc, xkeep, qkeep, kkeep, vkeep, okeep, lkeep, hkeep, akeep, spkeep, ykeep,
    xarr, n1, wq, wob, w1b, w2b, ab, gb, acc, n2, yb, b1r, spb, q, k, v, o, lse,
    wsend, wrecv, xsend, xrecv, psend, precv, ssem, lsem, lw, la, fsend, hsend, frecv,
):
    section, tensor = lax.axis_index("section"), lax.axis_index("tensor")
    dp, line = lax.axis_index("dp"), lax.axis_size("dp")
    T, W, D, RP, RL, C, NI = dm.T, dm.W, dm.D, dm.RP, dm.RL, dm.C, dm.NI
    lower, upper = section == 0, section == 1
    own = (wqkv, wout, wup, wdown)

    def slot_refs(slot):
        return (gqkv.at[slot], gout.at[slot], gup.at[slot], gdown.at[slot])

    def weight_copy(slot, index):
        relay = slot > 1 and slot % 2 == 1
        source = chunk_refs(dm, index, *(slot_refs(slot - 1) if relay else own))
        return pltpu.make_async_remote_copy(
            src_ref=source,
            dst_ref=chunk_refs(dm, index, *slot_refs(slot)),
            send_sem=wsend.at[slot, index],
            recv_sem=wrecv.at[slot, index],
            device_id={"tensor": flip(tensor, 1) if relay else partner(tensor, slot)},
        )

    def input_copy(slot):
        return pltpu.make_async_remote_copy(
            src_ref=xin.at[lax.rem(partner(tensor, slot), dm.micro)],
            dst_ref=xc.at[tensor],
            send_sem=xsend.at[slot],
            recv_sem=xrecv.at[slot],
            device_id={"tensor": partner(tensor, slot)},
        )

    def vector_copy(slot):
        return pltpu.make_async_remote_copy(
            src_ref=spin,
            dst_ref=spb.at[tensor],
            send_sem=psend.at[slot],
            recv_sem=precv.at[slot],
            device_id={"tensor": partner(tensor, slot)},
        )

    far = list(range(2, T, 2))
    fed = dm.NCH - 2

    def part_of(refs, number, origin):
        whole = chunk_refs(dm, number + 2, *refs)
        rows = whole.shape[0] // line
        return whole.at[pl.ds(pl.multiple_of(origin * rows, rows), rows), :]

    def far_copy(slot, number):
        return pltpu.make_async_remote_copy(
            src_ref=part_of(own, number, dp),
            dst_ref=part_of(slot_refs(slot), number, dp),
            send_sem=fsend.at[slot // 2, number],
            recv_sem=frecv.at[slot // 2, number, dp],
            device_id={"tensor": partner(tensor, slot)},
        )

    def hop_copy(slot, number, origin, way):
        place = lax.rem(dp + (1 if way == 0 else line - 1), line)
        return pltpu.make_async_remote_copy(
            src_ref=part_of(slot_refs(slot), number, origin),
            dst_ref=part_of(slot_refs(slot), number, origin),
            send_sem=hsend.at[slot // 2, number, origin, way],
            recv_sem=frecv.at[slot // 2, number, origin],
            device_id={"dp": place},
        )

    def hop_ways(origin):
        return (
            jnp.logical_and(dp >= origin, dp < line - 1),
            jnp.logical_and(dp <= origin, dp > 0),
        )

    def pass_part(slot, number, origin):
        hop_copy(slot, number, origin, 0).wait_recv()
        for way, go in enumerate(hop_ways(origin)):

            @pl.when(go)
            def _():
                hop_copy(slot, number, origin, way).start()

    pump_steps = fed + line - 1

    def pump(step):
        for slot in far:
            for distance in range(line):
                number = step - distance
                if not 0 <= number < fed:
                    continue
                if distance == 0:
                    pass_part(slot, number, dp)
                    continue

                @pl.when(dp >= distance)
                def _():
                    pass_part(slot, number, dp - distance)

                @pl.when(dp + distance < line)
                def _():
                    pass_part(slot, number, dp + distance)

            if 0 <= step - (line - 1) < fed:
                weight_copy(slot + 1, step - (line - 1) + 2).start()

    stream_copy = pltpu.make_async_remote_copy(
        src_ref=yb,
        dst_ref=xarr,
        send_sem=ssem.at[0],
        recv_sem=ssem.at[1],
        device_id={"section": 1 - section},
    )

    meet(dm, section, tensor, dp)
    for slot in range(1, T):
        vector_copy(slot).start()
        input_copy(slot).start()
    own_vec = pltpu.make_async_copy(spin, spb.at[tensor], lsem.at[0])
    own_vec.start()
    own_in = pltpu.make_async_copy(xin.at[lax.rem(tensor, dm.micro)], xc.at[tensor], lsem.at[1])
    own_in.start()
    for number in range(fed):
        for slot in far:
            far_copy(slot, number).start()
    for index in range(dm.NCH):
        weight_copy(1, index).start()
    for index in range(2):
        for slot in far:
            weight_copy(slot, index).start()

    def relay(slot, index):
        weight_copy(slot, index).wait_recv()
        weight_copy(slot + 1, index).start()

    own_vec.wait()
    own_in.wait()
    for slot in range(1, T):
        vector_copy(slot).wait_recv()
        input_copy(slot).wait_recv()

    @pl.when(upper)
    def _():
        for step in range(pump_steps):
            pump(step)
        for index in range(2):
            for slot in far:
                relay(slot, index)
        stream_copy.wait_recv()

    @pl.when(lower)
    def _():
        load = pltpu.make_async_copy(xc, xarr, lsem.at[0])
        load.start()
        load.wait()

    def arrive(slot, index):
        if slot == 0:
            return
        if slot % 2 == 0:
            if index < 2:

                @pl.when(lower)
                def _():
                    relay(slot, index)

        else:
            weight_copy(slot, index).wait_recv()

    def source_of(slot, index):
        return chunk_refs(dm, index, *(own if slot == 0 else slot_refs(slot)))

    keep_x = pltpu.make_async_copy(xarr, xkeep, lsem.at[1])
    keep_x.start()
    keep_p = pltpu.make_async_copy(spb, spkeep, lsem.at[2])
    keep_p.start()

    gain, bias = full_vector(dm, spb, LN1_GAIN), full_vector(dm, spb, LN1_BIAS)

    def first_norm(r, _):
        rows = pl.ds(pl.multiple_of(r * STEP, STEP), STEP)
        hat, _inv = norm_rows(block_rows(dm, xarr, rows).astype(F32), D)
        n1[rows, :] = (hat * gain + bias).astype(BF16)
        return 0

    lax.fori_loop(0, RP // STEP, first_norm, 0)

    for index, (slot, c) in enumerate(dm.order):
        shard = spb[partner(tensor, slot)]
        per = C // W
        first = FC1_BIAS + c * per
        b1r[index] = jnp.concatenate([shard[first + i : first + i + 1, :] for i in range(per)], axis=1)

    pad = jnp.zeros((RL - RP, W), BF16)
    for slot in range(T):
        for ref in (q, k, v):
            ref[slot, pl.ds(RP, RL - RP), :] = pad

    def load_qkv(slot, parity):
        return pltpu.make_async_copy(source_of(slot, 0), wq.at[parity], lw.at[parity])

    def fetch_qkv(which):
        for slot in range(T):

            @pl.when(which == slot)
            def _():
                arrive(slot, 0)
                load_qkv(slot, slot % 2).start()

    masks = half_masks(RL)

    fetch_qkv(0)

    def pump_lower(steps):
        @pl.when(lower)
        def _():
            for step in steps:
                pump(step)

    pump_lower(range(1))

    def heads(slot, _):
        parity = lax.rem(slot, 2)
        pltpu.make_async_copy(gqkv.at[0], wq.at[parity], lw.at[parity]).wait()
        early = jnp.logical_or(upper, slot < 1)

        @pl.when(jnp.logical_and(early, slot + 1 < T))
        def _():
            fetch_qkv(slot + 1)

        shard = spb[partner_dynamic(dm, tensor, slot)]
        rows = pl.ds(0, RP)
        q[slot, rows, :] = (dot_plain(n1[...], wq[parity, 0]) + shard[Q_BIAS : Q_BIAS + 1]).astype(BF16)
        k[slot, rows, :] = dot_plain(n1[...], wq[parity, 1]).astype(BF16)
        v[slot, rows, :] = (dot_plain(n1[...], wq[parity, 2]) + shard[V_BIAS : V_BIAS + 1]).astype(BF16)

        for pair in range(W // 128):
            lanes = slice(pair * 128, pair * 128 + 128)

            keys, values = k[slot, pl.ds(0, dm.KR), lanes], v[slot, pl.ds(0, dm.KR), lanes]
            query = q[slot, :, lanes] * jnp.asarray(HEAD_DIM**-0.5, BF16)
            total = None
            for half in range(2):
                query_h = jnp.where(masks[half], query, jnp.zeros_like(query))
                values_h = jnp.where(masks[half][: dm.KR], values, jnp.zeros_like(values))
                scores = add_masked(dm, dot_last(keys, query_h))
                most = jnp.max(scores, axis=0, keepdims=True)
                e = jnp.exp(scores - most)
                norm = jnp.sum(e, axis=0, keepdims=True)
                lse[slot, pl.ds(2 * pair + half, 1), :] = most + jnp.log(norm)
                part = dot_rows((e * (1.0 / norm)).astype(BF16), values_h)
                total = part if total is None else total + part
            o[slot, :, lanes] = total.astype(BF16)

        @pl.when(jnp.logical_and(lower, slot == 0))
        def _():
            pump(1)

        @pl.when(jnp.logical_and(lower, slot == 1))
        def _():
            for step in range(2, pump_steps - 2):
                pump(step)

        @pl.when(jnp.logical_and(jnp.logical_not(early), slot + 1 < T))
        def _():
            fetch_qkv(slot + 1)

        return 0

    lax.fori_loop(0, T, heads, 0)

    keeps = []
    for number, (source, target) in enumerate(((q, qkeep), (k, kkeep), (v, vkeep), (o, okeep), (lse, lkeep))):
        keeps.append(pltpu.make_async_copy(source, target, la.at[2 + number]))
        keeps[-1].start()

    loads = []
    for slot in range(T):
        arrive(slot, 1)
        loads.append(
            pltpu.make_async_copy(source_of(slot, 1), wob.at[pl.ds(slot * W, W)], lw.at[2 + slot])
        )
        loads[-1].start()

    def arrive_ff(index):
        slot, c = dm.order[index]
        arrive(slot, 2 + 2 * c)
        arrive(slot, 3 + 2 * c)

    def load_ff(index, parity):
        slot, c = dm.order[index]
        return [
            pltpu.make_async_copy(source_of(slot, 2 + 2 * c), w1b.at[parity], lsem.at[3 + parity]),
            pltpu.make_async_copy(source_of(slot, 3 + 2 * c), w2b.at[parity], lsem.at[5 + parity]),
        ]

    def fetch_ff(which):
        for index in range(NI):

            @pl.when(which == index)
            def _():
                arrive_ff(index)
                for load in load_ff(index, index % 2):
                    load.start()

    fetch_ff(0)
    pump_lower(range(pump_steps - 2, pump_steps - 1))
    for load in loads:
        load.wait()
    attended = jnp.concatenate([o[slot, pl.ds(0, RP), :] for slot in range(T)], axis=1)
    for n in range(D // 256):
        acc[:, pl.ds(n * 256, 256)] = dot_plain(attended, wob[:, pl.ds(n * 256, 256)])

    out_bias = full_vector(dm, spb, OUT_BIAS)
    gain2, bias2 = full_vector(dm, spb, LN2_GAIN), full_vector(dm, spb, LN2_BIAS)
    down_bias = full_vector(dm, spb, FC2_BIAS)

    def second_norm(r, _):
        rows = pl.ds(pl.multiple_of(r * STEP, STEP), STEP)
        hidden = block_rows(dm, xarr, rows).astype(F32) + (acc[rows, :] + out_bias)
        hat, _inv = norm_rows(hidden, D)
        n2[rows, :] = (hat * gain2 + bias2).astype(BF16)
        acc[rows, :] = hidden
        return 0

    lax.fori_loop(0, RP // STEP, second_norm, 0)
    pump_lower(range(pump_steps - 1, pump_steps))
    keep_h = pltpu.make_async_copy(acc, hkeep, lsem.at[0])
    keep_h.start()
    keep_h.wait()

    def keep_a(index, parity):
        return pltpu.make_async_copy(ab.at[parity], akeep.at[index], la.at[parity])

    def feed(index, _):
        parity = lax.rem(index, 2)
        for load in load_ff(0, parity):
            load.wait()
        early = jnp.logical_or(upper, index + 1 < 2 * dm.NC)

        @pl.when(jnp.logical_and(early, index + 1 < NI))
        def _():
            fetch_ff(index + 1)

        @pl.when(index >= 2)
        def _():
            keep_a(index - 2, parity).wait()

        a = dot_plain(n2[...], w1b[parity]) + b1r[index]
        ab[parity] = a
        gb[...] = (0.5 * a * (1.0 + lax.erf(a * ROOT_HALF))).astype(BF16)
        keep_a(index, parity).start()
        for n in range(D // 256):
            cols = pl.ds(n * 256, 256)
            acc[:, cols] += dot_plain(gb[...], w2b[parity, :, cols])

        @pl.when(jnp.logical_and(jnp.logical_not(early), index + 1 < NI))
        def _():
            fetch_ff(index + 1)

        return 0

    lax.fori_loop(0, NI, feed, 0)

    def close(r, _):
        rows = pl.ds(pl.multiple_of(r * STEP, STEP), STEP)
        y = (acc[rows, :] + down_bias).astype(BF16)
        for j in range(T):
            yb[j, rows, :] = y[:, j * W : (j + 1) * W]
        return 0

    lax.fori_loop(0, RP // STEP, close, 0)

    @pl.when(lower)
    def _():
        stream_copy.start()

    keep_y = pltpu.make_async_copy(yb, ykeep, lsem.at[0])
    keep_y.start()
    keep_y.wait()
    keep_x.wait()
    keep_p.wait()
    for keep in keeps:
        keep.wait()
    for index in (NI - 2, NI - 1):
        keep_a(index, index % 2).wait()
    for slot in range(1, T):
        vector_copy(slot).wait_send()
        input_copy(slot).wait_send()
        for index in range(2 if slot in far else dm.NCH):
            weight_copy(slot, index).wait_send()
    for slot in far:
        for number in range(fed):
            far_copy(slot, number).wait_send()
            for origin in range(line):
                for way, go in enumerate(hop_ways(origin)):

                    @pl.when(go)
                    def _():
                        hop_copy(slot, number, origin, way).wait_send()

    @pl.when(lower)
    def _():
        stream_copy.wait_send()


def partner_dynamic(dm, place, slot):
    bit = 1
    while bit < dm.T:
        take = lax.rem(lax.div(slot, bit), 2)
        place = place + take * (bit - 2 * bit * lax.rem(lax.div(place, bit), 2))
        bit *= 2
    return place


def forward_call(dm, xin, vectors, wqkv, wout, wup, wdown):
    T, W, D, RP, RL, C, NI, FL = dm.T, dm.W, dm.D, dm.RP, dm.RL, dm.C, dm.NI, dm.FL
    sds = jax.ShapeDtypeStruct
    outs = (
        sds((T, 3, D, W), BF16), sds((T, W, D), BF16), sds((T, D, FL), BF16), sds((T, FL, D), BF16),
        sds((T, RP, W), BF16), sds((T, RP, W), BF16),
        sds((T, RL, W), BF16), sds((T, RL, W), BF16), sds((T, RL, W), BF16), sds((T, RL, W), BF16),
        sds((T, dm.HS, RL), F32), sds((RP, D), F32), sds((NI, RP, C), F32), sds((T, VECTOR_ROWS, W), F32), sds((T, RP, W), BF16),
    )
    dma = pltpu.SemaphoreType.DMA
    line, fed = lax.axis_size("dp"), dm.NCH - 2
    scratch = [
        pltpu.VMEM((T, RP, W), BF16), pltpu.VMEM((RP, D), BF16), pltpu.VMEM((2, 3, D, W), BF16),
        pltpu.VMEM((D, D), BF16), pltpu.VMEM((2, D, C), BF16), pltpu.VMEM((2, C, D), BF16),
        pltpu.VMEM((2, RP, C), F32), pltpu.VMEM((RP, C), BF16), pltpu.VMEM((RP, D), F32),
        pltpu.VMEM((RP, D), BF16), pltpu.VMEM((T, RP, W), BF16), pltpu.VMEM((NI, 1, C), F32),
        pltpu.VMEM((T, VECTOR_ROWS, W), F32),
        pltpu.VMEM((T, RL, W), BF16), pltpu.VMEM((T, RL, W), BF16), pltpu.VMEM((T, RL, W), BF16), pltpu.VMEM((T, RL, W), BF16),
        pltpu.VMEM((T, dm.HS, RL), F32),
        dma((T, dm.NCH)), dma((T, dm.NCH)), dma((T,)), dma((T,)), dma((T,)), dma((T,)),
        dma((2,)), dma((8,)), dma((2 + T,)), dma((7,)),
        dma((T // 2, fed)), dma((T // 2, fed, line, 2)), dma((T // 2, fed, line)),
    ]
    return pl.pallas_call(
        functools.partial(forward_kernel, dm),
        out_shape=outs,
        in_specs=[ANY] * 6,
        out_specs=[ANY] * len(outs),
        scratch_shapes=scratch,
        name="layer_forward",
        compiler_params=pltpu.CompilerParams(
            collective_id=0, has_side_effects=True, vmem_limit_bytes=VMEM_BYTES
        ),
    )(xin, vectors, wqkv, wout, wup, wdown)


def packed_vectors(dm, ln1_gain, ln1_bias, qv_bias, out_bias, ln2_gain, ln2_bias, fc1_bias, fc2_bias):
    rows = [ln1_gain, ln1_bias, qv_bias[0], out_bias, ln2_gain, ln2_bias, fc2_bias, fc1_bias]
    flat = jnp.concatenate([row.reshape(-1, dm.W) for row in rows], axis=0)
    return jnp.pad(flat, ((0, VECTOR_ROWS - flat.shape[0]), (0, 0)))


def padded_rows(dm, array):
    return jnp.pad(array, ((0, 0), (0, dm.RP - dm.tok), (0, 0)))


def dot_rows(left, right):
    return lax.dot_general(left, right, (((0,), (0,)), ((), ())), preferred_element_type=F32)


def fold(rows):
    total = rows[0:8, :]
    for first in range(8, rows.shape[0], 8):
        total = total + rows[first : first + 8, :]
    return total


def norm_rows_back(grad, hat, inv, gain, width):
    scaled = grad * gain
    mean = jnp.sum(scaled, axis=1, keepdims=True) * (1.0 / width)
    along = jnp.sum(scaled * hat, axis=1, keepdims=True) * (1.0 / width)
    return inv * (scaled - mean - hat * along)


def backward_kernel(
    dm,
    xc, xkeep, qkeep, kkeep, vkeep, okeep, lkeep, hkeep, akeep, spkeep, ykeep,
    wqkv, wout, wup, wdown, gqkv, gout, gup, gdown,
    dqkv, dout, dup, ddown, result, dxkeep, flat_sums, head_sums, up_sums,
    arr, dyb, acc, dh, hh, dhb, gs, das, n1t, n2t, nb, q, k, v, o, do, dq, dk, dv, xx,
    w1b, w2b, ab, wob, wq, s1, s2, yb, spb, fs, hs, us, lse,
    ssem, osend, orecv, lsem, lw, lq, lg,
):
    section, tensor = lax.axis_index("section"), lax.axis_index("tensor")
    T, W, D, RP, RL, C, NI = dm.T, dm.W, dm.D, dm.RP, dm.RL, dm.C, dm.NI
    lower, upper = section == 0, section == 1
    own = (wqkv, wout, wup, wdown)
    real = pl.ds(0, RP)

    def source_of(slot, index):
        if slot == 0:
            return chunk_refs(dm, index, *own)
        return chunk_refs(dm, index, gqkv.at[slot], gout.at[slot], gup.at[slot], gdown.at[slot])

    stream_copy = pltpu.make_async_remote_copy(
        src_ref=arr,
        dst_ref=arr,
        send_sem=ssem.at[0],
        recv_sem=ssem.at[1],
        device_id={"section": 1 - section},
    )

    def output_copy(slot):
        return pltpu.make_async_remote_copy(
            src_ref=ykeep.at[partner(tensor, slot)],
            dst_ref=result.at[tensor],
            send_sem=osend.at[slot],
            recv_sem=orecv.at[slot],
            device_id={"tensor": partner(tensor, slot)},
        )

    def load_ff(index, parity):
        slot, c = dm.order[index]
        return [
            pltpu.make_async_copy(source_of(slot, 2 + 2 * c), w1b.at[parity], lw.at[parity]),
            pltpu.make_async_copy(source_of(slot, 3 + 2 * c), w2b.at[parity], lw.at[2 + parity]),
            pltpu.make_async_copy(akeep.at[index], ab.at[parity], lw.at[4 + parity]),
        ]

    def fetch_ff(which):
        for index in range(NI):

            @pl.when(which == index)
            def _():
                for load in load_ff(index, index % 2):
                    load.start()

    fetch_ff(0)
    loads = [
        pltpu.make_async_copy(source, target, lsem.at[number])
        for number, (source, target) in enumerate(
            ((spkeep, spb), (hkeep, hh), (qkeep, q), (kkeep, k), (vkeep, v), (okeep, o), (xkeep, xx), (lkeep, lse))
        )
    ]
    for load in loads:
        load.start()
    out_loads = [
        pltpu.make_async_copy(source_of(slot, 1), wob.at[pl.ds(slot * W, W)], lq.at[2 + slot])
        for slot in range(T)
    ]
    for load in out_loads:
        load.start()

    meet(dm, section, tensor)
    for slot in range(1, T):
        output_copy(slot).start()
    own_out = pltpu.make_async_copy(ykeep.at[tensor], result.at[tensor], lsem.at[8])
    own_out.start()

    @pl.when(upper)
    def _():
        load = pltpu.make_async_copy(xc, arr, lsem.at[9])
        load.start()
        load.wait()

    tail_rows = pl.ds(RP, RL - RP)
    blank = jnp.zeros((RL - RP, D), BF16)
    dyb[tail_rows, :] = blank
    dhb[tail_rows, :] = blank
    nb[tail_rows, :] = blank
    for index in range(NI):
        gs[index, tail_rows, :] = blank[:, :C]
        das[index, tail_rows, :] = blank[:, :C]
    for slot in range(T):
        do[slot, tail_rows, :] = blank[:, :W]
        if dm.KR < RL:
            for ref in (dk, dv):
                ref[slot, pl.ds(dm.KR, RL - dm.KR), :] = jnp.zeros((RL - dm.KR, W), BF16)
    acc[...] = jnp.zeros_like(acc)
    fs[...] = jnp.zeros_like(fs)
    hs[...] = jnp.zeros_like(hs)

    @pl.when(lower)
    def _():
        stream_copy.wait_recv()

    def spread(r, _):
        rows = pl.ds(pl.multiple_of(r * STEP, STEP), STEP)
        incoming = block_rows(dm, arr, rows)
        if T > dm.micro:
            incoming = jnp.where(tensor < dm.micro, incoming, jnp.zeros_like(incoming))
        dyb[rows, :] = incoming
        return 0

    lax.fori_loop(0, RP // STEP, spread, 0)

    def feed_back(index, _):
        parity = lax.rem(index, 2)
        for load in load_ff(0, parity):
            load.wait()

        @pl.when(index + 1 < NI)
        def _():
            fetch_ff(index + 1)

        for first in range(0, C, 256):
            cols = pl.ds(first, 256)
            a = ab[parity, :, cols]
            cdf = 0.5 * (1.0 + lax.erf(a * ROOT_HALF))
            gs[index, real, cols] = (a * cdf).astype(BF16)
            slope = cdf + a * jnp.exp(-0.5 * a * a) * GAUSS_FACTOR
            da = dot_last(dyb[real, :], w2b[parity, cols, :]) * slope
            das[index, real, cols] = da.astype(BF16)
            us[index, :, cols] = jnp.sum(fold(da), axis=0, keepdims=True)
        for n in range(D // 256):
            cols = pl.ds(n * 256, 256)
            acc[:, cols] += dot_last(das[index, real, :], w1b[parity, cols, :])
        return 0

    lax.fori_loop(0, NI, feed_back, 0)

    for load in loads:
        load.wait()
    for load in out_loads:
        load.wait()
    gain2, bias2 = full_vector(dm, spb, LN2_GAIN), full_vector(dm, spb, LN2_BIAS)

    def second_norm(r, _):
        rows = pl.ds(pl.multiple_of(r * STEP, STEP), STEP)
        hat, inv = norm_rows(hh[rows, :], D)
        grad = acc[rows, :]
        dy = dyb[rows, :].astype(F32)
        fs[0] += fold(grad * hat)
        fs[1] += fold(grad)
        whole = dy + norm_rows_back(grad, hat, inv, gain2, D)
        dh[rows, :] = whole
        dhb[rows, :] = whole.astype(BF16)
        fs[2] += fold(whole)
        fs[3] += fold(dy)
        nb[rows, :] = (hat * gain2 + bias2).astype(BF16)
        return 0

    lax.fori_loop(0, RP // STEP, second_norm, 0)

    def turn(target):
        for n in range(D // 256):
            cols = pl.ds(n * 256, 256)
            target[cols, :] = nb[:, cols].T

    turn(n2t)

    def put_ff(index, parity):
        slot, c = dm.order[index]
        return [
            pltpu.make_async_copy(s1.at[parity], dup.at[slot, :, pl.ds(c * C, C)], lg.at[parity]),
            pltpu.make_async_copy(s2.at[parity], ddown.at[slot, pl.ds(c * C, C), :], lg.at[2 + parity]),
        ]

    def feed_weights():
        def one(index, _):
            parity = lax.rem(index, 2)

            @pl.when(index >= 2)
            def _():
                for put in put_ff(0, parity):
                    put.wait()

            for n in range(D // 256):
                cols = pl.ds(n * 256, 256)
                s1[parity, cols, :] = dot_plain(n2t[cols, :], das[index])
            for n in range(C // 256):
                cols = pl.ds(n * 256, 256)
                s2[parity, cols, :] = dot_rows(gs[index, :, cols], dyb[...])
            for j in range(NI):

                @pl.when(index == j)
                def _():
                    for put in put_ff(j, j % 2):
                        put.start()

            return 0

        lax.fori_loop(0, NI, one, 0)
        for parity in range(2):
            for put in put_ff(0, parity):
                put.wait()

    @pl.when(lower)
    def _():
        feed_weights()

    for slot in range(T):
        do[slot, real, :] = dot_last(dhb[real, :], wob[pl.ds(slot * W, W), :]).astype(BF16)

    masks = half_masks(RL)
    scale = jnp.asarray(HEAD_DIM**-0.5, BF16)
    real_keys = pl.ds(0, dm.KR)

    def heads(slot, _):
        for pair in range(W // 128):
            lanes = slice(pair * 128, pair * 128 + 128)
            keys, values = k[slot, real_keys, lanes], v[slot, real_keys, lanes]
            query, grad = q[slot, :, lanes] * scale, do[slot, :, lanes]
            scaled_keys = keys * scale
            sums = None
            for half in range(2):
                mask = masks[half]
                query_h = jnp.where(mask, query, jnp.zeros_like(query))
                grad_h = jnp.where(mask, grad, jnp.zeros_like(grad))
                keys_h = jnp.where(mask[: dm.KR], scaled_keys, jnp.zeros_like(keys))
                scores = add_masked(dm, dot_last(keys, query_h))
                p = jnp.exp(scores - lse[slot, pl.ds(2 * pair + half, 1), :])
                dp = dot_last(values, grad_h)
                delta = jnp.sum(p * dp, axis=0, keepdims=True)
                ds = (p * (dp - delta)).astype(BF16)
                terms = (dot_rows(ds, keys_h), dot_plain(ds, query_h), dot_plain(p.astype(BF16), grad_h))
                sums = terms if sums is None else tuple(x + y for x, y in zip(sums, terms))
            dq_pair, dk_pair, dv_pair = sums
            dq[slot, :, lanes] = dq_pair.astype(BF16)
            dk[slot, real_keys, lanes] = dk_pair.astype(BF16)
            dv[slot, real_keys, lanes] = dv_pair.astype(BF16)
            hs[slot, 0, :, lanes] += fold(dq_pair)
            hs[slot, 1, :, lanes] += fold(dv_pair)
        return 0

    lax.fori_loop(0, T, heads, 0)

    def load_qkv(slot, parity):
        return pltpu.make_async_copy(source_of(slot, 0), wq.at[parity], lq.at[parity])

    load_qkv(0, 0).start()
    for slot in range(T):
        load_qkv(slot, slot % 2).wait()
        if slot + 1 < T:
            load_qkv(slot + 1, (slot + 1) % 2).start()
        for n in range(D // 256):
            cols = pl.ds(n * 256, 256)
            part = dot_last(dq[slot, real, :], wq[slot % 2, 0, cols, :])
            part = part + dot_last(dk[slot, real, :], wq[slot % 2, 1, cols, :])
            part = part + dot_last(dv[slot, real, :], wq[slot % 2, 2, cols, :])
            if slot == 0:
                acc[:, cols] = part
            else:
                acc[:, cols] += part

    gain1, bias1 = full_vector(dm, spb, LN1_GAIN), full_vector(dm, spb, LN1_BIAS)

    def first_norm(r, _):
        rows = pl.ds(pl.multiple_of(r * STEP, STEP), STEP)
        hat, inv = norm_rows(block_rows(dm, xx, rows).astype(F32), D)
        grad = acc[rows, :]
        fs[4] += fold(grad * hat)
        fs[5] += fold(grad)
        whole = dh[rows, :] + norm_rows_back(grad, hat, inv, gain1, D)
        nb[rows, :] = (hat * gain1 + bias1).astype(BF16)
        low = whole.astype(BF16)
        for j in range(T):
            yb[j, rows, :] = whole[:, j * W : (j + 1) * W]
            xx[j, rows, :] = low[:, j * W : (j + 1) * W]
        return 0

    lax.fori_loop(0, RP // STEP, first_norm, 0)

    down_copy = pltpu.make_async_remote_copy(
        src_ref=xx,
        dst_ref=arr,
        send_sem=ssem.at[0],
        recv_sem=ssem.at[1],
        device_id={"section": 1 - section},
    )

    @pl.when(upper)
    def _():
        down_copy.start()

    keep_dx = pltpu.make_async_copy(yb, dxkeep, lsem.at[0])
    keep_dx.start()
    turn(n1t)

    pending = []
    for slot in range(T):
        for number, source in enumerate((dq, dk, dv)):
            turn_number = len(pending) % 2
            if len(pending) >= 2:
                pending[-2].wait()
            for n in range(D // 256):
                cols = pl.ds(n * 256, 256)
                s1[turn_number, cols, pl.ds(0, W)] = dot_plain(n1t[cols, :], source[slot])
            pending.append(
                pltpu.make_async_copy(
                    s1.at[turn_number, :, pl.ds(0, W)], dqkv.at[slot, number], lg.at[turn_number]
                )
            )
            pending[-1].start()
    for put in pending[-2:]:
        put.wait()
    pending = []
    for slot in range(T):
        if len(pending) >= 2:
            pending[-2].wait()
        s2[slot % 2, pl.ds(0, W), :] = dot_rows(o[slot], dhb[...])
        pending.append(pltpu.make_async_copy(s2.at[slot % 2, pl.ds(0, W), :], dout.at[slot], lg.at[2 + slot % 2]))
        pending[-1].start()
    for put in pending[-2:]:
        put.wait()

    @pl.when(upper)
    def _():
        feed_weights()

    keeps = []
    for number, (source, target) in enumerate(((fs, flat_sums), (hs, head_sums), (us, up_sums))):
        keeps.append(pltpu.make_async_copy(source, target, lsem.at[1 + number]))
        keeps[-1].start()
    for keep in keeps:
        keep.wait()
    keep_dx.wait()
    own_out.wait()
    for slot in range(1, T):
        output_copy(slot).wait()

    @pl.when(upper)
    def _():
        down_copy.wait_send()


def backward_call(dm, kept, own):
    T, W, D, RP, RL, C, NI, FL = dm.T, dm.W, dm.D, dm.RP, dm.RL, dm.C, dm.NI, dm.FL
    sds = jax.ShapeDtypeStruct
    gathered, rest = kept[:4], kept[4:]
    outs = (
        sds((T, 3, D, W), F32), sds((T, W, D), F32), sds((T, D, FL), F32), sds((T, FL, D), F32),
        sds((T, RP, W), BF16), sds((T, RP, W), F32), sds((6, 8, D), F32), sds((T, 2, 8, W), F32), sds((NI, 1, C), F32),
    )
    dma = pltpu.SemaphoreType.DMA
    heads = pltpu.VMEM((T, RL, W), BF16)
    scratch = [
        pltpu.VMEM((T, RP, W), BF16), pltpu.VMEM((RL, D), BF16), pltpu.VMEM((RP, D), F32), pltpu.VMEM((RP, D), F32),
        pltpu.VMEM((RP, D), F32), pltpu.VMEM((RL, D), BF16), pltpu.VMEM((NI, RL, C), BF16), pltpu.VMEM((NI, RL, C), BF16),
        pltpu.VMEM((D, RL), BF16), pltpu.VMEM((D, RL), BF16), pltpu.VMEM((RL, D), BF16),
        heads, heads, heads, heads, heads, heads, heads, heads, pltpu.VMEM((T, RP, W), BF16),
        pltpu.VMEM((2, D, C), BF16), pltpu.VMEM((2, C, D), BF16), pltpu.VMEM((2, RP, C), F32),
        pltpu.VMEM((D, D), BF16), pltpu.VMEM((2, 3, D, W), BF16), pltpu.VMEM((2, D, C), F32), pltpu.VMEM((2, C, D), F32),
        pltpu.VMEM((T, RP, W), F32), pltpu.VMEM((T, VECTOR_ROWS, W), F32),
        pltpu.VMEM((6, 8, D), F32), pltpu.VMEM((T, 2, 8, W), F32), pltpu.VMEM((NI, 1, C), F32),
        pltpu.VMEM((T, dm.HS, RL), F32),
        dma((2,)), dma((T,)), dma((T,)), dma((10,)), dma((6,)), dma((2 + T,)), dma((8,)),
    ]
    return pl.pallas_call(
        functools.partial(backward_kernel, dm),
        out_shape=outs,
        in_specs=[ANY] * 19,
        out_specs=[ANY] * len(outs),
        scratch_shapes=scratch,
        name="layer_backward",
        compiler_params=pltpu.CompilerParams(
            collective_id=1, has_side_effects=True, vmem_limit_bytes=VMEM_BYTES
        ),
    )(*rest, *own, *gathered)


def piece_list(dm):
    down, up, out, qkv = [], [], [], []
    for first in range(0, dm.FL, 128):
        down.append((3, first, 128))
    for first in range(0, dm.D, 128):
        up.append((2, first, 128))
    for first in range(0, dm.W, 128):
        out.append((1, first, 128))
    for first in range(0, 3 * dm.D, 512):
        qkv.append((0, first, 512))
    return down + up + out + qkv


def reduce_kernel(
    dm,
    dqkv, dout, dup, ddown, dxkeep, flat_sums, head_sums, up_sums,
    rqkv, rout, rup, rdown, result, fqkv, fout, fup, fdown, rsmall,
    *scratch,
):
    section, dp, tensor = lax.axis_index("section"), lax.axis_index("dp"), lax.axis_index("tensor")
    T, W, D, FL, NI, C = dm.T, dm.W, dm.D, dm.FL, dm.NI, dm.C
    line = lax.axis_size("dp")
    stages = dm.stages
    scratch = list(scratch)
    kept, come = scratch.pop(0), scratch.pop(0)
    land = [[scratch.pop(0) for _ in range(4)] for _ in range(stages)]
    inward = [scratch.pop(0) for _ in range(4)]
    outward = [scratch.pop(0) for _ in range(4)]
    parts, gathered, small_in, small_out, small_own = [scratch.pop(0) for _ in range(5)]
    lsend, lrecv, isend, irecv, osend, orecv, msem, wsem, gsend, grecv, vsem, dsend, drecv = scratch
    first_land = (fqkv, fout, fup, fdown)
    partial = (dqkv, dout, dup, ddown)
    reduced = (rqkv, rout, rup, rdown)
    pieces = piece_list(dm)
    NP = len(pieces)

    half = line // 2
    left = dp < half
    outer = jnp.logical_or(dp == 0, dp == line - 1)
    middle = jnp.logical_or(dp == half - 1, dp == half)
    toward = jnp.where(left, 1, -1)
    inner_dp = dp + toward
    outer_dp = lax.rem(dp - toward + line, line)

    barrier = pltpu.get_barrier_semaphore()
    for slot in range(1, T):
        pl.semaphore_signal(barrier, inc=1, device_id={"tensor": partner(tensor, slot)})
    pl.semaphore_signal(barrier, inc=1, device_id={"dp": lax.rem(dp + 1, line)})
    pl.semaphore_signal(barrier, inc=1, device_id={"dp": lax.rem(dp + line - 1, line)})
    pl.semaphore_wait(barrier, T + 1)

    def at(ref, piece, *lead):
        kind, first, rows = pieces[piece]
        return ref[kind].at[(*lead, pl.ds(first, rows), slice(None))]

    def lowest(slot):
        stage = 0
        while slot % 2 == 0:
            slot //= 2
            stage += 1
        return stage

    def fold_copy(piece, slot):
        stage = lowest(slot)
        bit = 1 << stage
        place = (slot - bit) >> (stage + 1)
        if stage == 0:
            source, target = at(partial, piece, slot), at(first_land, piece, place)
        else:
            source, target = at(land[0], piece, slot // 2), at(land[stage], piece, place)
        return pltpu.make_async_remote_copy(
            src_ref=source,
            dst_ref=target,
            send_sem=lsend.at[piece, slot],
            recv_sem=lrecv.at[piece, slot],
            device_id={"tensor": flip(tensor, bit)},
        )

    def inward_copy(piece, source):
        return pltpu.make_async_remote_copy(
            src_ref=source,
            dst_ref=at(inward, piece),
            send_sem=isend.at[piece],
            recv_sem=irecv.at[piece],
            device_id={"dp": inner_dp},
        )

    def meet_copy(piece, source):
        return pltpu.make_async_remote_copy(
            src_ref=source,
            dst_ref=at(outward, piece),
            send_sem=isend.at[piece],
            recv_sem=orecv.at[piece],
            device_id={"dp": inner_dp},
        )

    def outward_copy(piece):
        return pltpu.make_async_remote_copy(
            src_ref=at(outward, piece),
            dst_ref=at(outward, piece),
            send_sem=osend.at[piece],
            recv_sem=orecv.at[piece],
            device_id={"dp": outer_dp},
        )

    def loads(piece, slot):
        kind, first, rows = pieces[piece]
        wide = (W, D, FL, D)[kind]
        view = (slot // 2, piece % 2, kind)
        pair = []
        for number, (stage, ref) in enumerate(((kept, at(partial, piece, slot)), (come, at(first_land, piece, slot // 2)))):
            place = stage[view[2]].at[view[0], view[1]]
            pair.append(pltpu.make_async_copy(ref, place, msem.at[number, slot // 2, piece % 2, int(kind == 0)]))
        return pair

    def fetch(piece, slot):
        if piece < NP:
            fold_copy(piece, slot + 1).wait_recv()
            for one in loads(piece, slot):
                one.start()

    def input_grad_copy(slot):
        return pltpu.make_async_remote_copy(
            src_ref=dxkeep.at[partner(tensor, slot)],
            dst_ref=result.at[tensor],
            send_sem=dsend.at[slot],
            recv_sem=drecv.at[slot],
            device_id={"tensor": partner(tensor, slot)},
        )

    def store(piece):
        return pltpu.make_async_copy(at(outward, piece), at(reduced, piece), wsem.at[piece])

    for j in range(T):
        for row in range(6):
            parts[j, row : row + 1, :] = jnp.sum(flat_sums[row, :, j * W : (j + 1) * W], axis=0, keepdims=True)
        parts[j, 8 + FL // W : VECTOR_ROWS, :] = jnp.zeros((VECTOR_ROWS - 8 - FL // W, W), F32)
    per = C // W
    for slot in range(T):
        place = partner(tensor, slot)
        for row in range(2):
            parts[place, 6 + row : 7 + row, :] = jnp.sum(head_sums[slot, row], axis=0, keepdims=True)
        for index, (owner, c) in enumerate(dm.order):
            if owner == slot:
                for i in range(per):
                    row = 8 + c * per + i
                    parts[place, row : row + 1, :] = up_sums[index, :, i * W : (i + 1) * W]

    def small_copy(slot):
        return pltpu.make_async_remote_copy(
            src_ref=parts.at[partner(tensor, slot)],
            dst_ref=gathered.at[slot],
            send_sem=gsend.at[slot],
            recv_sem=grecv.at[slot],
            device_id={"tensor": partner(tensor, slot)},
        )

    def small_line(number, source, target, place):
        return pltpu.make_async_remote_copy(
            src_ref=source,
            dst_ref=target,
            send_sem=vsem.at[number],
            recv_sem=vsem.at[number + 1],
            device_id={"dp": place},
        )

    for piece in range(NP):
        for slot in range(1, T, 2):
            fold_copy(piece, slot).start()
    for slot in range(1, T):
        small_copy(slot).start()
    own_grad = pltpu.make_async_copy(dxkeep.at[tensor], result.at[tensor], dsend.at[0])
    own_grad.start()

    def rows_of(piece):
        kind, first, rows = pieces[piece]
        width = (W, D, FL, D)[kind]
        step = max(16, min(rows, 32768 // width))
        return kind, first, rows // step, step

    def add_into(piece, target, sources, staged=None):
        kind, first, count, step = rows_of(piece)

        def one(r, _):
            rows = pl.ds(pl.multiple_of(first + r * step, 16), step)
            near = pl.ds(pl.multiple_of(r * step, 16), step)
            total = None
            if staged is not None:
                lead = (staged // 2, piece % 2, near, slice(None))
                total = kept[kind][lead] + come[kind][lead]
            for ref, lead in sources:
                term = ref[kind][(*lead, rows, slice(None))].astype(F32)
                total = term if total is None else total + term
            target[0][kind][(*target[1], rows, slice(None))] = total.astype(BF16)
            return 0

        lax.fori_loop(0, count, one, 0)

    def pass_on(piece, stage):
        bit = 1 << stage
        for slot in range(bit, T, 2 * bit):
            for before in range(1, stage):
                fold_copy(piece, slot + (1 << before)).wait_recv()
            for one in loads(piece, slot):
                one.wait()
            add_into(
                piece,
                (land[0], (slot // 2,)),
                [(land[b], (slot >> (b + 1),)) for b in range(1, stage)],
                staged=slot,
            )
            fold_copy(piece, slot).start()
            fetch(piece + 2, slot)

    own_terms = [(land[b], (0,)) for b in range(1, stages)]

    def own_sum(piece):
        for stage in range(1, stages):
            fold_copy(piece, 1 << stage).wait_recv()

        @pl.when(outer)
        def _():
            for one in loads(piece, 0):
                one.wait()
            add_into(piece, (land[0], (0,)), own_terms, staged=0)
            inward_copy(piece, at(land[0], piece, 0)).start()
            fetch(piece + 2, 0)

    def gather_in(piece):
        @pl.when(jnp.logical_not(outer))
        def _():
            for one in loads(piece, 0):
                one.wait()
            inward_copy(piece, at(inward, piece)).wait_recv()
            add_into(piece, (inward, ()), own_terms + [(inward, ())], staged=0)

            @pl.when(middle)
            def _():
                meet_copy(piece, at(inward, piece)).start()

            @pl.when(jnp.logical_not(middle))
            def _():
                inward_copy(piece, at(inward, piece)).start()

            fetch(piece + 2, 0)

    def spread_middle(piece):
        @pl.when(middle)
        def _():
            meet_copy(piece, at(inward, piece)).wait_recv()
            add_into(piece, (outward, ()), [(outward, ()), (inward, ())])
            outward_copy(piece).start()
            store(piece).start()

    def spread_out(piece):
        @pl.when(jnp.logical_not(middle))
        def _():
            outward_copy(piece).wait_recv()

            @pl.when(jnp.logical_not(outer))
            def _():
                outward_copy(piece).start()

            store(piece).start()

    def small_chain():
        for slot in range(1, T):
            small_copy(slot).wait_recv()
        total = parts[tensor]
        for slot in range(1, T):
            total = total + gathered[slot]
        small_own[...] = total

        @pl.when(outer)
        def _():
            small_line(0, small_own, small_in, inner_dp).start()

        @pl.when(jnp.logical_not(outer))
        def _():
            small_line(0, small_own, small_in, inner_dp).wait_recv()
            small_in[...] = small_in[...] + small_own[...]

            @pl.when(jnp.logical_not(middle))
            def _():
                small_line(0, small_in, small_in, inner_dp).start()

        @pl.when(middle)
        def _():
            meeting = small_line(2, small_in, small_out, inner_dp)
            meeting.start()
            meeting.wait_recv()
            small_out[...] = small_out[...] + small_in[...]
            small_line(4, small_out, small_out, outer_dp).start()

        @pl.when(jnp.logical_not(middle))
        def _():
            small_line(4, small_out, small_out, outer_dp).wait_recv()

            @pl.when(jnp.logical_not(outer))
            def _():
                small_line(4, small_out, small_out, outer_dp).start()

        rsmall[...] = small_out[...]

    def run(action, piece, *rest):
        if 0 <= piece < NP:
            action(piece, *rest)

    for piece in range(2):
        for slot in range(0, T, 2):
            fetch(piece, slot)
    ahead = 1
    depth = stages - 1
    for stage in range(1, stages):
        for piece in range(ahead + (depth - stage)):
            run(pass_on, piece, stage)
    for step in range(NP + 4):
        for stage in range(1, stages):
            run(pass_on, step + ahead + (depth - stage), stage)
        run(own_sum, step)
        run(gather_in, step - 1)
        run(spread_middle, step - 2)
        run(spread_out, step - 3)
        if step == NP - 1:
            for slot in range(1, T):
                input_grad_copy(slot).start()
        if step == NP:
            small_chain()

    for piece in range(NP):
        store(piece).wait()
        for slot in range(1, T):
            fold_copy(piece, slot).wait_send()

        @pl.when(jnp.logical_not(middle))
        def _():
            inward_copy(piece, at(inward, piece)).wait_send()

        @pl.when(middle)
        def _():
            meet_copy(piece, at(inward, piece)).wait_send()

        @pl.when(jnp.logical_not(outer))
        def _():
            outward_copy(piece).wait_send()

    own_grad.wait()
    for slot in range(1, T):
        small_copy(slot).wait_send()
        input_grad_copy(slot).wait()

    @pl.when(jnp.logical_not(middle))
    def _():
        small_line(0, small_in, small_in, inner_dp).wait_send()

    @pl.when(middle)
    def _():
        small_line(2, small_in, small_out, inner_dp).wait_send()

    @pl.when(jnp.logical_not(outer))
    def _():
        small_line(4, small_out, small_out, outer_dp).wait_send()


def reduce_call(dm, partial, dx, sums):
    T, W, D, FL = dm.T, dm.W, dm.D, dm.FL
    dm.stages = T.bit_length() - 1
    sds = jax.ShapeDtypeStruct
    dims = ((3 * D, W), (W, D), (D, FL), (FL, D))
    partial = (partial[0].reshape(T, 3 * D, W),) + tuple(partial[1:])
    outs = tuple(sds(d, BF16) for d in dims) + (sds(dx.shape, F32),)
    outs += tuple(sds((T // 2, *d), F32) for d in dims) + (sds((VECTOR_ROWS, W), F32),)
    NP = len(piece_list(dm))
    dma = pltpu.SemaphoreType.DMA
    staged = [pltpu.VMEM((T // 2, 2, 512, W), F32)] + [pltpu.VMEM((T // 2, 2, 128, w), F32) for w in (D, FL, D)]
    scratch = [staged, staged]
    for stage in range(dm.stages):
        scratch += [pltpu.VMEM((max(T >> (stage + 1), 1), *d), BF16) for d in dims]
    scratch += [pltpu.VMEM(d, BF16) for d in dims] * 2
    scratch += [pltpu.VMEM((T, VECTOR_ROWS, W), F32)] * 2 + [pltpu.VMEM((VECTOR_ROWS, W), F32)] * 3
    scratch += [
        dma((NP, T)), dma((NP, T)), dma((NP,)), dma((NP,)), dma((NP,)), dma((NP,)),
        dma((2, T // 2, 2, 2)), dma((NP,)), dma((T,)), dma((T,)), dma((6,)), dma((T,)), dma((T,)),
    ]
    whole = pl.BlockSpec(memory_space=pltpu.VMEM)
    return pl.pallas_call(
        functools.partial(reduce_kernel, dm),
        out_shape=outs,
        in_specs=[ANY] * 5 + [whole] * 3,
        out_specs=[ANY] * 9 + [whole],
        scratch_shapes=scratch,
        name="grad_reduce",
        compiler_params=pltpu.CompilerParams(
            collective_id=2, has_side_effects=True, vmem_limit_bytes=VMEM_BYTES
        ),
    )(*partial, dx, *sums)


def shards(
    images, cotangent, ln1_gain, ln1_bias, qkv_weight, qv_bias, out_weight, out_bias,
    ln2_gain, ln2_bias, fc1_weight, fc1_bias, fc2_weight, fc2_bias,
):
    dm = sizes_of(images, fc1_weight, lax.axis_size("tensor"))
    T, W, D = dm.T, dm.W, dm.D
    section, tensor = lax.axis_index("section"), lax.axis_index("tensor")
    xin = padded_rows(dm, jnp.where(section == 0, images[:, 0], cotangent[:, 0]))
    vectors = packed_vectors(
        dm, ln1_gain[0], ln1_bias[0], qv_bias, out_bias[0], ln2_gain[0], ln2_bias[0], fc1_bias[0], fc2_bias[0]
    )
    own = (qkv_weight[0], out_weight[0], fc1_weight[0], fc2_weight[0])
    kept = forward_call(dm, xin, vectors, *own)
    dqkv, dout, dup, ddown, result, dx, flat_sums, head_sums, up_sums = backward_call(dm, kept, own)
    section_out = result[: dm.micro, : dm.tok][None, :, None]

    rqkv, rout, rup, rdown, result, _, _, _, _, small = reduce_call(
        dm, (dqkv, dout, dup, ddown), dx, (flat_sums, head_sums, up_sums)
    )
    input_grads = result[: dm.micro, : dm.tok][None, :, None]
    g2, b2, ob, db, g1, b1 = (small[i][None] for i in range(6))
    qv = small[6:8][None]
    ub = small[8 : 8 + dm.FL // W].reshape(1, -1)
    wide = lambda array: array.astype(F32)[None]
    return (
        section_out, input_grads, g1, b1, wide(rqkv.reshape(3, D, W)), qv, wide(rout), ob, g2, b2,
        wide(rup), ub, wide(rdown), db,
    )


def solution(mesh):
    vector = P("section", "tensor")
    rows = P(None, "dp", None, "tensor")
    placed_rows = P("section", None, "dp", None, "tensor")
    qkv, qv = P("section", None, None, "tensor"), P("section", None, "tensor")
    by_row, by_column = P("section", "tensor", None), P("section", None, "tensor")
    return jax.shard_map(
        shards,
        mesh=mesh,
        in_specs=(rows, rows, vector, vector, qkv, qv, by_row, vector, vector, vector, by_column, vector, by_row, vector),
        out_specs=(
            placed_rows, placed_rows, vector, vector, qkv, qv, by_row, vector, vector, vector,
            by_column, vector, by_row, vector,
        ),
        check_vma=False,
    )
```
